8 devices in a mesh: dp: 2 (over z, y), tp: 4 (over x, core).
Axes of the slice: x: 2, y: 2, z: 1, core: 2. Of those that a mesh axis runs over, the one named last changes fastest.
Arguments:
- x: bfloat16 [32, 1536], P('dp'), parts along dimension 0
- k_cache: bfloat16 [32, 4096, 12, 128], P('dp', None, 'tp'), parts along dimension 0
- v_cache: bfloat16 [32, 4096, 12, 128], P('dp', None, 'tp'), parts along dimension 0
- seq_lens: int32 [32], P('dp'), parts along dimension 0
- nbr_enc: bfloat16 [32, 256, 896], P('dp', 'tp'), parts along dimension 0
- ln1_gain: float32 [1536], replicated
- ln1_bias: float32 [1536], replicated
- w_q: bfloat16 [1536, 1536], P(None, 'tp')
- w_k: bfloat16 [1536, 1536], P(None, 'tp')
- w_v: bfloat16 [1536, 1536], P(None, 'tp')
- w_o: bfloat16 [1536, 1536], P('tp')
- ln2_gain: float32 [1536], replicated
- ln2_bias: float32 [1536], replicated
- wq_c: bfloat16 [1536, 1536], P(None, 'tp')
- wk_c: bfloat16 [896, 1536], P(None, 'tp')
- wv_c: bfloat16 [896, 1536], P(None, 'tp')
- wo_c: bfloat16 [1536, 1536], P('tp')
- ln3_gain: float32 [1536], replicated
- ln3_bias: float32 [1536], replicated
- w_up: bfloat16 [1536, 6144], P(None, 'tp')
- w_down: bfloat16 [6144, 1536], P('tp')
Outputs:
- output 1: bfloat16 [32, 1536], P('dp'), parts along dimension 0
- output 2: bfloat16 [32, 12, 128], P('dp', 'tp'), parts along dimension 0
- output 3: bfloat16 [32, 12, 128], P('dp', 'tp'), parts along dimension 0
There are 2 independent parts. The reference program is written for one: setup_inputs(seed, part) draws one part's arguments, and reference() takes and returns one part's arrays. A program takes and returns all parts, laid end to end along the dimension named above; an argument that names none is the same for every part.
All inputs are finite; a program needn't handle non-finite values.
Results may differ from the reference program's by a relative error of at most 0.0147339.
Values are sent between devices in bfloat16 or wider.
A program may use at most 1 GiB of HBM per device.

```python
import jax
import jax.numpy as jnp
from jax import lax

D = 1536
HEADS = 12
HEAD = 128
ENC_DIM = 896
NEIGHBOURS = 2
RET_LEN = 128
SEGMENT = 64
BATCH = 16
CTX_LEN = 4096

FF_DIM = 4 * D
WIDTH = HEADS * HEAD
NBR_TOKENS = NEIGHBOURS * RET_LEN
LN_EPS = 1e-5


def draw_lens(key):
    key_len, key_pick = jax.random.split(key)
    top_seg = CTX_LEN // SEGMENT - 1
    seg_count = jax.random.randint(key_len, (BATCH,), 1, top_seg + 1)
    pick_row = jax.random.randint(key_pick, (), 0, BATCH)
    seg_count = jnp.where(jnp.arange(BATCH) == pick_row, top_seg, seg_count)
    return (seg_count * SEGMENT).astype(jnp.int32)


def draw_weight(key, fan_in, fan_out, gain):
    return (jax.random.normal(key, (fan_in, fan_out), jnp.float32) * (gain * fan_in ** -0.5)).astype(jnp.bfloat16)


def setup_inputs(seed: int = 0, part: int = 0) -> dict:
    own_keys = jax.random.split(jax.random.fold_in(jax.random.key(seed), part), 8)
    shared_keys = jax.random.split(jax.random.key(seed + 1), 12)
    ramp = (2.0 * jnp.arange(CTX_LEN, dtype=jnp.float32) / CTX_LEN - 1.0)[None, :, None, None]
    cache_shape = (BATCH, CTX_LEN, HEADS, HEAD)
    head_shape = (BATCH, 1, HEADS, HEAD)
    k_dir = jax.random.normal(own_keys[1], head_shape, jnp.float32)
    k_cache = 3.0 * ramp * k_dir + jax.random.normal(own_keys[2], cache_shape, jnp.float32)
    v_base = jax.random.normal(own_keys[3], head_shape, jnp.float32)
    v_dir = jax.random.normal(own_keys[4], head_shape, jnp.float32)
    v_cache = v_base + ramp * v_dir + 0.5 * jax.random.normal(own_keys[5], cache_shape, jnp.float32)
    nbr_enc = jax.random.normal(own_keys[7], (BATCH, NBR_TOKENS, ENC_DIM), jnp.float32)
    ln_gains = 1.0 + 0.4 * jax.random.normal(shared_keys[0], (3, D), jnp.float32)
    ln_biases = 0.4 * jax.random.normal(shared_keys[1], (3, D), jnp.float32)
    return {
        'x': jax.random.normal(own_keys[0], (BATCH, D), jnp.float32).astype(jnp.bfloat16),
        'k_cache': k_cache.astype(jnp.bfloat16),
        'v_cache': v_cache.astype(jnp.bfloat16),
        'seq_lens': draw_lens(own_keys[6]),
        'nbr_enc': nbr_enc.astype(jnp.bfloat16),
        'ln1_gain': ln_gains[0],
        'ln1_bias': ln_biases[0],
        'w_q': draw_weight(shared_keys[2], D, WIDTH, 1.0),
        'w_k': draw_weight(shared_keys[3], D, WIDTH, 1.0),
        'w_v': draw_weight(shared_keys[4], D, WIDTH, 1.0),
        'w_o': draw_weight(shared_keys[5], WIDTH, D, 1.0),
        'ln2_gain': ln_gains[1],
        'ln2_bias': ln_biases[1],
        'wq_c': draw_weight(shared_keys[6], D, WIDTH, 1.0),
        'wk_c': draw_weight(shared_keys[7], ENC_DIM, WIDTH, 2.5),
        'wv_c': draw_weight(shared_keys[8], ENC_DIM, WIDTH, 1.0),
        'wo_c': draw_weight(shared_keys[9], WIDTH, D, 1.0),
        'ln3_gain': ln_gains[2],
        'ln3_bias': ln_biases[2],
        'w_up': draw_weight(shared_keys[10], D, FF_DIM, 1.0),
        'w_down': draw_weight(shared_keys[11], FF_DIM, D, 1.5),
    }


def layer_norm(values, ln_gain, ln_bias):
    row_mean = jnp.mean(values, axis=-1, keepdims=True)
    centred = values - row_mean
    row_var = jnp.mean(jnp.square(centred), axis=-1, keepdims=True)
    return (centred * lax.rsqrt(row_var + LN_EPS) * ln_gain + ln_bias).astype(jnp.bfloat16)


def project(operand, weight):
    return jnp.dot(operand, weight, preferred_element_type=jnp.float32).astype(jnp.bfloat16)


def reference(x, k_cache, v_cache, seq_lens, nbr_enc, ln1_gain, ln1_bias, w_q, w_k, w_v, w_o, ln2_gain, ln2_bias, wq_c, wk_c, wv_c, wo_c, ln3_gain, ln3_bias, w_up, w_down):
    q_scale = HEAD ** -0.5
    positions = jnp.arange(CTX_LEN)
    residual = x.astype(jnp.float32)
    a_norm = layer_norm(residual, ln1_gain, ln1_bias)
    q_new = project(a_norm, w_q).reshape(BATCH, HEADS, HEAD)
    k_new = project(a_norm, w_k).reshape(BATCH, HEADS, HEAD)
    v_new = project(a_norm, w_v).reshape(BATCH, HEADS, HEAD)

    def self_row(row_args):
        q_row, k_rows, v_rows, k_one, v_one, length = row_args
        q_f = q_row.astype(jnp.float32)
        s_old = jnp.einsum('hd,thd->ht', q_f, k_rows.astype(jnp.float32)) * q_scale
        s_old = jnp.where(positions[None, :] < length, s_old, -1e30)
        s_new = jnp.sum(q_f * k_one.astype(jnp.float32), axis=-1) * q_scale
        row_max = jnp.maximum(jnp.max(s_old, axis=-1), s_new)
        e_old = jnp.exp(s_old - row_max[:, None])
        e_new = jnp.exp(s_new - row_max)
        row_sum = jnp.sum(e_old, axis=-1) + e_new
        p_old = (e_old / row_sum[:, None]).astype(jnp.bfloat16).astype(jnp.float32)
        p_new = (e_new / row_sum).astype(jnp.bfloat16).astype(jnp.float32)
        head_out = jnp.einsum('ht,thd->hd', p_old, v_rows.astype(jnp.float32)) + p_new[:, None] * v_one.astype(jnp.float32)
        return head_out.astype(jnp.bfloat16)

    def cross_row(row_args):
        q_row, enc_row = row_args
        k_nbr = project(enc_row, wk_c).reshape(NBR_TOKENS, HEADS, HEAD).astype(jnp.float32)
        v_nbr = project(enc_row, wv_c).reshape(NBR_TOKENS, HEADS, HEAD).astype(jnp.float32)
        scores = jnp.einsum('hd,nhd->hn', q_row.astype(jnp.float32), k_nbr) * q_scale
        probs = jax.nn.softmax(scores, axis=-1).astype(jnp.bfloat16).astype(jnp.float32)
        return jnp.einsum('hn,nhd->hd', probs, v_nbr).astype(jnp.bfloat16)

    self_out = lax.map(self_row, (q_new, k_cache, v_cache, k_new, v_new, seq_lens))
    residual = residual + project(self_out.reshape(BATCH, WIDTH), w_o).astype(jnp.float32)
    c_norm = layer_norm(residual, ln2_gain, ln2_bias)
    q_cross = project(c_norm, wq_c).reshape(BATCH, HEADS, HEAD)
    cross_out = lax.map(cross_row, (q_cross, nbr_enc))
    residual = residual + project(cross_out.reshape(BATCH, WIDTH), wo_c).astype(jnp.float32)
    m_norm = layer_norm(residual, ln3_gain, ln3_bias)
    hidden = jax.nn.gelu(jnp.dot(m_norm, w_up, preferred_element_type=jnp.float32), approximate=False).astype(jnp.bfloat16)
    layer_out = (residual + project(hidden, w_down).astype(jnp.float32)).astype(jnp.bfloat16)
    return layer_out, k_new, v_new
```

```python
import functools

import jax
import jax.numpy as jnp
from jax import lax
from jax.experimental import pallas as pl
from jax.experimental.pallas import tpu as pltpu
from jax.sharding import PartitionSpec as P

LN_EPS = 1e-5
NEG = -1e30
F32 = jnp.float32
BF16 = jnp.bfloat16
CHUNK = 512
UNROLL = 4
GROUPS = 6


def layer_norm(values, ln_gain, ln_bias):
    row_mean = jnp.mean(values, axis=-1, keepdims=True)
    centred = values - row_mean
    row_var = jnp.mean(jnp.square(centred), axis=-1, keepdims=True)
    return (centred * lax.rsqrt(row_var + LN_EPS) * ln_gain + ln_bias).astype(BF16)


def dot(lhs, rhs):
    return jnp.dot(lhs, rhs, preferred_element_type=F32)


def dot_t(lhs, rhs):
    return lax.dot_general(lhs, rhs, (((1,), (1,)), ((), ())), preferred_element_type=F32)


def self_kernel(batch, heads, dim, lens, x_ref, g_ref, b_ref, kc, vc, wq_h, wk_h, wv_h, wo_h,
                part_ref, knew_ref, vnew_ref,
                wq, wk, wv, wo, kbuf, vbuf, q_s, o_s, m_s, l_s, acc_s, wsem, ksem, vsem):
    width = heads * dim
    scale = dim ** -0.5
    loads = [pltpu.make_async_copy(s, d, wsem.at[i]) for i, (s, d) in enumerate(((wq_h, wq), (wk_h, wk), (wv_h, wv), (wo_h, wo)))]
    for copy in loads[:3]:
        copy.start()

    def len_of(seq):
        return jnp.where(seq < batch, lens[jnp.minimum(seq, batch - 1)], 0)

    def following(seq, blk):
        more = (blk + 1) * CHUNK < len_of(seq)
        return jnp.where(more, seq, seq + 1), jnp.where(more, blk + 1, 0)

    def copies(seq, blk, slot):
        rows = pl.ds(pl.multiple_of(blk * CHUNK, CHUNK), CHUNK)
        return (pltpu.make_async_copy(kc.at[seq, :, rows, :], kbuf.at[slot], ksem.at[slot]),
                pltpu.make_async_copy(vc.at[seq, :, rows, :], vbuf.at[slot], vsem.at[slot]))

    def fetch_group(group, ptr):
        for u in range(UNROLL):
            seq, blk = ptr

            @pl.when(seq < batch)
            def _():
                for copy in copies(seq, blk, group * UNROLL + u):
                    copy.start()
            ptr = following(seq, blk)
        return ptr

    ptr = (jnp.int32(0), jnp.int32(0))
    for group in range(GROUPS - 1):
        ptr = fetch_group(group, ptr)
    loads[3].start()

    n_items = jnp.int32(0)
    for seq in range(batch):
        n_items = n_items + lax.div(lens[seq] + (CHUNK - 1), CHUNK)
    n_steps = lax.div(n_items + (UNROLL - 1), UNROLL)

    a_norm = layer_norm(x_ref[...].astype(F32), g_ref[...].reshape(1, -1), b_ref[...].reshape(1, -1))
    loads[0].wait()
    q_new = dot(a_norm, wq[...]).astype(BF16).astype(F32)
    loads[1].wait()
    k_new = dot(a_norm, wk[...]).astype(BF16)
    loads[2].wait()
    v_new = dot(a_norm, wv[...]).astype(BF16)
    for h in range(heads):
        knew_ref[h] = k_new[:, h * dim:(h + 1) * dim]
        vnew_ref[h] = v_new[:, h * dim:(h + 1) * dim]
    q_s[0:batch, :] = q_new
    q_s[batch:, :] = jnp.zeros((q_s.shape[0] - batch, width), F32)
    head_mask = (lax.broadcasted_iota(jnp.int32, (8, width), 0) == lax.broadcasted_iota(jnp.int32, (8, width), 1) // dim).astype(F32)
    qk = q_new * k_new.astype(F32)
    v_f = v_new.astype(F32)
    for seq in range(batch):
        s_new = jnp.sum(qk[seq:seq + 1, :] * head_mask, axis=1, keepdims=True) * scale
        m_s[seq] = jnp.broadcast_to(s_new, (8, dim))
        acc_s[seq] = jnp.broadcast_to(v_f[seq:seq + 1, :], (8, width))
    l_s[...] = jnp.ones_like(l_s)
    m_s[batch] = jnp.zeros((8, dim), F32)
    acc_s[batch] = jnp.zeros((8, width), F32)
    lane = lax.broadcasted_iota(jnp.int32, (8, CHUNK), 1)

    def step(i, carry):
        ptr, cur = carry[:2], carry[2:]
        group = lax.rem(i, GROUPS)
        ptr = fetch_group(lax.rem(i + GROUPS - 1, GROUPS), ptr)
        items = []
        for u in range(UNROLL):
            items.append(cur)
            cur = following(*cur)
        for u, (seq, blk) in enumerate(items):

            @pl.when(seq < batch)
            def _():
                for copy in copies(seq, blk, group * UNROLL + u):
                    copy.wait()
        done = []
        for u, (seq, blk) in enumerate(items):
            slot = group * UNROLL + u
            row = jnp.minimum(seq, batch)
            q_blk = (q_s[pl.ds(row, 1), :] * head_mask).astype(BF16)
            k_cat = jnp.concatenate([kbuf[slot, h] for h in range(heads)], axis=1)
            s = dot_t(q_blk, k_cat) * scale
            s = jnp.where(lane < len_of(seq) - blk * CHUNK, s, NEG)
            m_i = jnp.max(s, axis=1, keepdims=True)
            p = jnp.exp(s - m_i)
            l_i = jnp.sum(p, axis=1, keepdims=True)
            v_cat = jnp.concatenate([vbuf[slot, h] for h in range(heads)], axis=1)
            done.append((row, m_i, l_i, dot(p.astype(BF16), v_cat)))
        for row, m_i, l_i, pv in done:
            m_old = m_s[row]
            m_new = jnp.maximum(m_old, m_i)
            keep = jnp.exp(m_old - m_new)
            add = jnp.exp(m_i - m_new)
            m_s[row] = m_new
            l_s[row] = l_s[row] * keep + l_i * add
            acc_s[row] = acc_s[row] * jnp.concatenate([keep] * heads, axis=1) + pv * jnp.concatenate([add] * heads, axis=1)
        return (*ptr, *cur)

    lax.fori_loop(0, n_steps, step, (*ptr, jnp.int32(0), jnp.int32(0)))
    for seq in range(batch):
        o = acc_s[seq] / jnp.concatenate([l_s[seq]] * heads, axis=1)
        o_s[seq:seq + 1, :] = jnp.sum(o * head_mask, axis=0, keepdims=True)
    loads[3].wait()
    part_ref[...] = dot(o_s[...].astype(BF16), wo[...]).astype(BF16)


def rest_kernel(batch, heads, dim, tp, dp_name, part_ref, x_ref, g2, b2, g3, b3, wqc_h, e_own_h, e_par_h, wk_h, wv_h, wkr_h, wvr_h, woc_h, wup_h, wdn_h,
                out_ref,
                wqc, enc, wkv, wkvr, woc, wup, wdn, kv_own, kv_rem, recv, send2, send3, qc_s, qc_r, o_snd, o_rcv, st_snd, st_rcv,
                lsem, ssem, rsem, xs, xr):
    width = heads * dim
    scale = dim ** -0.5
    me = lax.axis_index('tp')
    far = lax.rem(me + 2, tp)
    half = enc.shape[0] // 2

    def load(i, src, dst):
        copy = pltpu.make_async_copy(src, dst, lsem.at[i])
        copy.start()
        return copy

    ld_e0 = load(0, e_own_h, enc.at[pl.ds(0, half), :])
    ld_wk = load(1, wk_h, wkv.at[:, pl.ds(0, width)])
    ld_wv = load(2, wv_h, wkv.at[:, pl.ds(width, width)])
    ld_e1 = load(3, e_par_h, enc.at[pl.ds(half, half), :])
    ld_wqc = load(4, wqc_h, wqc)
    ld_wkr = load(5, wkr_h, wkvr.at[:, pl.ds(0, width)])
    ld_wvr = load(6, wvr_h, wkvr.at[:, pl.ds(width, width)])
    ld_woc = load(7, woc_h, woc)
    ld_up = load(8, wup_h, wup)
    ld_dn = load(9, wdn_h, wdn)

    barrier = pltpu.get_barrier_semaphore()
    for d in range(1, tp):
        pl.semaphore_signal(barrier, inc=1, device_id={'tp': lax.rem(me + d, tp)}, device_id_type=pl.DeviceIdType.MESH)
    pl.semaphore_wait(barrier, tp - 1)

    def exchange(n, src):
        for d in range(1, tp):
            pltpu.make_async_remote_copy(src_ref=src, dst_ref=recv.at[n, me], send_sem=ssem.at[n, d - 1], recv_sem=rsem.at[n, me],
                                         device_id={'tp': lax.rem(me + d, tp)}, device_id_type=pl.DeviceIdType.MESH).start()
        recv[n, me] = src[...]

    def collect(n, src):
        for d in range(1, tp):
            other = lax.rem(me + d, tp)
            pltpu.make_async_remote_copy(src_ref=src, dst_ref=recv.at[n, other], send_sem=ssem.at[n, d - 1], recv_sem=rsem.at[n, other],
                                         device_id={'tp': other}, device_id_type=pl.DeviceIdType.MESH).wait()
        total = recv[n, 0].astype(F32)
        for t in range(1, tp):
            total = total + recv[n, t].astype(F32)
        return total

    def to_far(i, src, dst):
        return pltpu.make_async_remote_copy(src_ref=src, dst_ref=dst, send_sem=xs.at[i], recv_sem=xr.at[i],
                                            device_id={'tp': far}, device_id_type=pl.DeviceIdType.MESH)

    def project(weights, out, tile=256):
        def body(i, c):
            rows = pl.ds(pl.multiple_of(i * tile, tile), tile)
            out[rows, :] = dot(enc[rows, :], weights[...]).astype(BF16)
            return c
        lax.fori_loop(0, enc.shape[0] // tile, body, 0)

    exchange(0, part_ref)
    for copy in (ld_e0, ld_wk, ld_wv, ld_e1):
        copy.wait()
    project(wkv, kv_own)

    h1 = x_ref[...].astype(F32) + collect(0, part_ref)
    c_norm = layer_norm(h1, g2[...].reshape(1, -1), b2[...].reshape(1, -1))
    ld_wqc.wait()
    qc_s[...] = dot(c_norm, wqc[...]).astype(BF16)
    send_q = to_far(0, qc_s, qc_r)
    send_q.start()
    for copy in (ld_wkr, ld_wvr):
        copy.wait()
    project(wkvr, kv_rem)

    rows = heads * batch
    row_b = lax.rem(lax.broadcasted_iota(jnp.int32, (rows, 128), 0), batch)
    lane = lax.broadcasted_iota(jnp.int32, (rows, 128), 1)
    per = half // batch
    pack = 128 // per
    blocks = half // 128
    mine = lax.rem(row_b, pack) == lane // per
    row_blk = row_b // pack
    lane_head = lax.broadcasted_iota(jnp.int32, (batch, width), 1) // dim

    def attend(q, kv):
        qf = q.astype(F32)
        q_rows = jnp.concatenate([jnp.where(lane_head == h, qf, 0.0) for h in range(heads)], axis=0).astype(BF16)
        parts = []
        for part in range(2):
            s_all = dot_t(q_rows, kv[part * half:(part + 1) * half, 0:width])
            s = s_all[:, 0:128]
            for k in range(1, blocks):
                s = jnp.where(row_blk == k, s_all[:, k * 128:(k + 1) * 128], s)
            parts.append(jnp.where(mine, s * scale, NEG))
        m = jnp.maximum(jnp.max(parts[0], axis=1, keepdims=True), jnp.max(parts[1], axis=1, keepdims=True))
        p = [jnp.exp(s - m) for s in parts]
        l = jnp.sum(p[0], axis=1, keepdims=True) + jnp.sum(p[1], axis=1, keepdims=True)
        o = None
        for part in range(2):
            p_wide = jnp.concatenate([jnp.where(row_blk == k, p[part], 0.0) for k in range(blocks)], axis=1).astype(BF16)
            o_part = dot(p_wide, kv[part * half:(part + 1) * half, width:2 * width])
            o = o_part if o is None else o + o_part
        o = jnp.concatenate([o[h * batch:(h + 1) * batch, h * dim:(h + 1) * dim] for h in range(heads)], axis=0)
        return m, l, o

    send_q.wait()
    m_r, l_r, o_r = attend(qc_r[...], kv_rem)
    o_snd[...] = o_r
    st_snd[...] = jnp.where(lane < 64, m_r, l_r)
    send_o = to_far(1, o_snd, o_rcv)
    send_st = to_far(2, st_snd, st_rcv)
    send_o.start()
    send_st.start()
    m_a, l_a, o_a = attend(qc_s[...], kv_own)
    send_o.wait()
    send_st.wait()
    stats = st_rcv[...]
    m_b, l_b = stats[:, 0:1], stats[:, 64:65]
    m = jnp.maximum(m_a, m_b)
    w_a, w_b = jnp.exp(m_a - m), jnp.exp(m_b - m)
    o = (o_a * w_a + o_rcv[...] * w_b) / (l_a * w_a + l_b * w_b)
    oc = jnp.concatenate([o[h * batch:(h + 1) * batch, :] for h in range(heads)], axis=1).astype(BF16)
    ld_woc.wait()
    send2[...] = dot(oc, woc[...]).astype(BF16)
    exchange(1, send2)
    h2 = h1 + collect(1, send2)
    m_norm = layer_norm(h2, g3[...].reshape(1, -1), b3[...].reshape(1, -1))
    ld_up.wait()
    up = dot(m_norm, wup[...])
    hidden = (0.5 * up * (1.0 + lax.erf(up * (0.5 ** 0.5)))).astype(BF16)
    ld_dn.wait()
    send3[...] = dot(hidden, wdn[...]).astype(BF16)
    exchange(2, send3)
    out_ref[...] = (h2 + collect(2, send3)).astype(BF16)


def local_step(x, k_cache, v_cache, seq_lens, nbr_enc, ln1_gain, ln1_bias, w_q, w_k, w_v, w_o, ln2_gain, ln2_bias, wq_c, wk_c, wv_c, wo_c, ln3_gain, ln3_bias, w_up, w_down):
    batch, d_model = x.shape
    heads, dim = k_cache.shape[2:]
    width = heads * dim
    tp = lax.axis_size('tp')
    far = [(i, (i + 2) % tp) for i in range(tp)]
    near = [(i, i ^ 1) for i in range(tp)]
    enc = nbr_enc.reshape(-1, nbr_enc.shape[-1])
    enc_near = lax.ppermute(enc, 'tp', near)
    wk_far = lax.ppermute(wk_c, 'tp', far)
    wv_far = lax.ppermute(wv_c, 'tp', far)

    any_spec = pl.BlockSpec(memory_space=pltpu.HBM)
    vmem = pl.BlockSpec(memory_space=pltpu.VMEM)
    smem = pl.BlockSpec(memory_space=pltpu.SMEM)
    slots = GROUPS * UNROLL
    part, k_new, v_new = pl.pallas_call(
        functools.partial(self_kernel, batch, heads, dim),
        out_shape=(jax.ShapeDtypeStruct((batch, d_model), BF16), jax.ShapeDtypeStruct((heads, batch, dim), BF16), jax.ShapeDtypeStruct((heads, batch, dim), BF16)),
        in_specs=[smem, vmem, vmem, vmem] + [any_spec] * 6,
        out_specs=(vmem, vmem, vmem),
        scratch_shapes=[
            pltpu.VMEM((d_model, width), BF16), pltpu.VMEM((d_model, width), BF16), pltpu.VMEM((d_model, width), BF16), pltpu.VMEM((width, d_model), BF16),
            pltpu.VMEM((slots, heads, CHUNK, dim), BF16), pltpu.VMEM((slots, heads, CHUNK, dim), BF16),
            pltpu.VMEM((batch + 8, width), F32), pltpu.VMEM((batch, width), F32),
            pltpu.VMEM((batch + 1, 8, dim), F32), pltpu.VMEM((batch + 1, 8, dim), F32), pltpu.VMEM((batch + 1, 8, width), F32),
            pltpu.SemaphoreType.DMA((4,)), pltpu.SemaphoreType.DMA((slots,)), pltpu.SemaphoreType.DMA((slots,)),
        ],
        compiler_params=pltpu.CompilerParams(vmem_limit_bytes=63 * 2**20),
        cost_estimate=pl.CostEstimate(flops=40_000_000_000, bytes_accessed=60_000_000, transcendentals=0),
        name='self_attention',
    )(seq_lens, x, ln1_gain, ln1_bias, jnp.transpose(k_cache, (0, 2, 1, 3)), jnp.transpose(v_cache, (0, 2, 1, 3)), w_q, w_k, w_v, w_o)

    n_enc, enc_dim = enc.shape
    ff = w_up.shape[1]
    out = pl.pallas_call(
        functools.partial(rest_kernel, batch, heads, dim, tp, 'dp'),
        out_shape=jax.ShapeDtypeStruct((batch, d_model), BF16),
        in_specs=[vmem] * 6 + [any_spec] * 10,
        out_specs=vmem,
        scratch_shapes=[
            pltpu.VMEM((d_model, width), BF16), pltpu.VMEM((2 * n_enc, enc_dim), BF16),
            pltpu.VMEM((enc_dim, 2 * width), BF16), pltpu.VMEM((enc_dim, 2 * width), BF16),
            pltpu.VMEM((width, d_model), BF16), pltpu.VMEM((d_model, ff), BF16), pltpu.VMEM((ff, d_model), BF16),
            pltpu.VMEM((2 * n_enc, 2 * width), BF16), pltpu.VMEM((2 * n_enc, 2 * width), BF16),
            pltpu.VMEM((3, tp, batch, d_model), BF16), pltpu.VMEM((batch, d_model), BF16), pltpu.VMEM((batch, d_model), BF16),
            pltpu.VMEM((batch, width), BF16), pltpu.VMEM((batch, width), BF16),
            pltpu.VMEM((heads * batch, dim), F32), pltpu.VMEM((heads * batch, dim), F32), pltpu.VMEM((heads * batch, 128), F32), pltpu.VMEM((heads * batch, 128), F32),
            pltpu.SemaphoreType.DMA((10,)), pltpu.SemaphoreType.DMA((3, tp - 1)), pltpu.SemaphoreType.DMA((3, tp)),
            pltpu.SemaphoreType.DMA((3,)), pltpu.SemaphoreType.DMA((3,)),
        ],
        compiler_params=pltpu.CompilerParams(collective_id=0, has_side_effects=True, vmem_limit_bytes=63 * 2**20),
        cost_estimate=pl.CostEstimate(flops=20_000_000_000, bytes_accessed=30_000_000, transcendentals=0),
        name='rest_of_layer',
    )(part, x, ln2_gain, ln2_bias, ln3_gain, ln3_bias, wq_c, enc, enc_near, wk_c, wv_c, wk_far, wv_far, wo_c, w_up, w_down)
    return out, jnp.transpose(k_new, (1, 0, 2)), jnp.transpose(v_new, (1, 0, 2))


def solution(mesh):
    row_spec = P('dp', None)
    cache_spec = P('dp', None, 'tp', None)
    head_spec = P('dp', 'tp', None)
    vec_spec = P(None)
    col_split = P(None, 'tp')
    row_split = P('tp', None)
    in_specs = (row_spec, cache_spec, cache_spec, P('dp'), P('dp', 'tp', None), vec_spec, vec_spec, col_split, col_split, col_split, row_split, vec_spec, vec_spec, col_split, col_split, col_split, row_split, vec_spec, vec_spec, col_split, row_split)
    out_specs = (row_spec, head_spec, head_spec)
    return jax.shard_map(local_step, mesh=mesh, in_specs=in_specs, out_specs=out_specs, check_vma=False)
```

```python
import functools

import jax
import jax.numpy as jnp
from jax import lax
from jax.experimental import pallas as pl
from jax.experimental.pallas import tpu as pltpu
from jax.sharding import PartitionSpec as P

LN_EPS = 1e-5
NEG = -1e30
F32 = jnp.float32
BF16 = jnp.bfloat16
CHUNK = 1024
UNROLL = 2
GROUPS = 6


def layer_norm(values, ln_gain, ln_bias):
    row_mean = jnp.mean(values, axis=-1, keepdims=True)
    centred = values - row_mean
    row_var = jnp.mean(jnp.square(centred), axis=-1, keepdims=True)
    return (centred * lax.rsqrt(row_var + LN_EPS) * ln_gain + ln_bias).astype(BF16)


def dot(lhs, rhs):
    return jnp.dot(lhs, rhs, preferred_element_type=F32)


def dot_t(lhs, rhs):
    return lax.dot_general(lhs, rhs, (((1,), (1,)), ((), ())), preferred_element_type=F32)


def self_kernel(batch, heads, dim, lens, x_ref, g_ref, b_ref, kc, vc, wq_h, wk_h, wv_h, wo_h,
                part_ref, knew_ref, vnew_ref,
                wq, wk, wv, wo, kbuf, vbuf, q_s, o_s, m_s, l_s, acc_s, wsem, ksem, vsem):
    width = heads * dim
    scale = dim ** -0.5
    loads = [pltpu.make_async_copy(s, d, wsem.at[i]) for i, (s, d) in enumerate(((wq_h, wq), (wk_h, wk), (wv_h, wv), (wo_h, wo)))]
    for copy in loads[:3]:
        copy.start()

    def len_of(seq):
        return jnp.where(seq < batch, lens[jnp.minimum(seq, batch - 1)], 0)

    def following(seq, blk):
        more = (blk + 1) * CHUNK < len_of(seq)
        return jnp.where(more, seq, seq + 1), jnp.where(more, blk + 1, 0)

    def copies(seq, blk, slot):
        rows = pl.ds(pl.multiple_of(blk * CHUNK, CHUNK), CHUNK)
        return (pltpu.make_async_copy(kc.at[seq, :, rows, :], kbuf.at[slot], ksem.at[slot]),
                pltpu.make_async_copy(vc.at[seq, :, rows, :], vbuf.at[slot], vsem.at[slot]))

    def fetch_group(group, ptr):
        for u in range(UNROLL):
            seq, blk = ptr

            @pl.when(seq < batch)
            def _():
                for copy in copies(seq, blk, group * UNROLL + u):
                    copy.start()
            ptr = following(seq, blk)
        return ptr

    ptr = (jnp.int32(0), jnp.int32(0))
    for group in range(GROUPS - 1):
        ptr = fetch_group(group, ptr)
    loads[3].start()

    n_items = jnp.int32(0)
    for seq in range(batch):
        n_items = n_items + lax.div(lens[seq] + (CHUNK - 1), CHUNK)
    n_steps = lax.div(n_items + (UNROLL - 1), UNROLL)

    a_norm = layer_norm(x_ref[...].astype(F32), g_ref[...].reshape(1, -1), b_ref[...].reshape(1, -1))
    loads[0].wait()
    q_new = dot(a_norm, wq[...]).astype(BF16).astype(F32)
    loads[1].wait()
    k_new = dot(a_norm, wk[...]).astype(BF16)
    loads[2].wait()
    v_new = dot(a_norm, wv[...]).astype(BF16)
    for h in range(heads):
        knew_ref[h] = k_new[:, h * dim:(h + 1) * dim]
        vnew_ref[h] = v_new[:, h * dim:(h + 1) * dim]
    q_s[0:batch, :] = q_new
    q_s[batch:, :] = jnp.zeros((q_s.shape[0] - batch, width), F32)
    head_mask = (lax.broadcasted_iota(jnp.int32, (8, width), 0) == lax.broadcasted_iota(jnp.int32, (8, width), 1) // dim).astype(F32)
    qk = q_new * k_new.astype(F32)
    v_f = v_new.astype(F32)
    for seq in range(batch):
        s_new = jnp.sum(qk[seq:seq + 1, :] * head_mask, axis=1, keepdims=True) * scale
        m_s[seq] = jnp.broadcast_to(s_new, (8, dim))
        acc_s[seq] = jnp.broadcast_to(v_f[seq:seq + 1, :], (8, width))
    l_s[...] = jnp.ones_like(l_s)
    m_s[batch] = jnp.zeros((8, dim), F32)
    acc_s[batch] = jnp.zeros((8, width), F32)
    lane = lax.broadcasted_iota(jnp.int32, (8, CHUNK), 1)

    def step(i, carry):
        ptr, cur = carry[:2], carry[2:]
        group = lax.rem(i, GROUPS)
        ptr = fetch_group(lax.rem(i + GROUPS - 1, GROUPS), ptr)
        items = []
        for u in range(UNROLL):
            items.append(cur)
            cur = following(*cur)
        for u, (seq, blk) in enumerate(items):

            @pl.when(seq < batch)
            def _():
                for copy in copies(seq, blk, group * UNROLL + u):
                    copy.wait()
        done = []
        for u, (seq, blk) in enumerate(items):
            slot = group * UNROLL + u
            row = jnp.minimum(seq, batch)
            q_blk = (q_s[pl.ds(row, 1), :] * head_mask).astype(BF16)
            k_cat = jnp.concatenate([kbuf[slot, h] for h in range(heads)], axis=1)
            s = dot_t(q_blk, k_cat) * scale
            s = jnp.where(lane < len_of(seq) - blk * CHUNK, s, NEG)
            m_i = jnp.max(s, axis=1, keepdims=True)
            p = jnp.exp(s - m_i)
            l_i = jnp.sum(p, axis=1, keepdims=True)
            v_cat = jnp.concatenate([vbuf[slot, h] for h in range(heads)], axis=1)
            done.append((row, m_i, l_i, dot(p.astype(BF16), v_cat)))
        for row, m_i, l_i, pv in done:
            m_old = m_s[row]
            m_new = jnp.maximum(m_old, m_i)
            keep = jnp.exp(m_old - m_new)
            add = jnp.exp(m_i - m_new)
            m_s[row] = m_new
            l_s[row] = l_s[row] * keep + l_i * add
            acc_s[row] = acc_s[row] * jnp.concatenate([keep] * heads, axis=1) + pv * jnp.concatenate([add] * heads, axis=1)
        return (*ptr, *cur)

    lax.fori_loop(0, n_steps, step, (*ptr, jnp.int32(0), jnp.int32(0)))
    for seq in range(batch):
        o = acc_s[seq] / jnp.concatenate([l_s[seq]] * heads, axis=1)
        o_s[seq:seq + 1, :] = jnp.sum(o * head_mask, axis=0, keepdims=True)
    loads[3].wait()
    part_ref[...] = dot(o_s[...].astype(BF16), wo[...]).astype(BF16)


def rest_kernel(batch, heads, dim, tp, dp_name, part_ref, x_ref, g2, b2, g3, b3, wqc_h, e_own_h, e_par_h, wk_h, wv_h, wkr_h, wvr_h, woc_h, wup_h, wdn_h,
                out_ref,
                wqc, enc, wkv, wkvr, woc, wup, wdn, kv_own, kv_rem, recv, send2, send3, qc_s, qc_r, o_snd, o_rcv, st_snd, st_rcv,
                lsem, ssem, rsem, xs, xr):
    width = heads * dim
    scale = dim ** -0.5
    me = lax.axis_index('tp')
    far = lax.rem(me + 2, tp)
    half = enc.shape[0] // 2

    def load(i, src, dst):
        copy = pltpu.make_async_copy(src, dst, lsem.at[i])
        copy.start()
        return copy

    ld_e0 = load(0, e_own_h, enc.at[pl.ds(0, half), :])
    ld_wk = load(1, wk_h, wkv.at[:, pl.ds(0, width)])
    ld_wv = load(2, wv_h, wkv.at[:, pl.ds(width, width)])
    ld_e1 = load(3, e_par_h, enc.at[pl.ds(half, half), :])
    ld_wqc = load(4, wqc_h, wqc)
    ld_wkr = load(5, wkr_h, wkvr.at[:, pl.ds(0, width)])
    ld_wvr = load(6, wvr_h, wkvr.at[:, pl.ds(width, width)])
    ld_woc = load(7, woc_h, woc)
    ld_up = load(8, wup_h, wup)
    ld_dn = load(9, wdn_h, wdn)

    barrier = pltpu.get_barrier_semaphore()
    for d in range(1, tp):
        pl.semaphore_signal(barrier, inc=1, device_id={'tp': lax.rem(me + d, tp)}, device_id_type=pl.DeviceIdType.MESH)
    pl.semaphore_wait(barrier, tp - 1)

    def exchange(n, src):
        for d in range(1, tp):
            pltpu.make_async_remote_copy(src_ref=src, dst_ref=recv.at[n, me], send_sem=ssem.at[n, d - 1], recv_sem=rsem.at[n, me],
                                         device_id={'tp': lax.rem(me + d, tp)}, device_id_type=pl.DeviceIdType.MESH).start()
        recv[n, me] = src[...]

    def collect(n, src):
        for d in range(1, tp):
            other = lax.rem(me + d, tp)
            pltpu.make_async_remote_copy(src_ref=src, dst_ref=recv.at[n, other], send_sem=ssem.at[n, d - 1], recv_sem=rsem.at[n, other],
                                         device_id={'tp': other}, device_id_type=pl.DeviceIdType.MESH).wait()
        total = recv[n, 0].astype(F32)
        for t in range(1, tp):
            total = total + recv[n, t].astype(F32)
        return total

    def to_far(i, src, dst):
        return pltpu.make_async_remote_copy(src_ref=src, dst_ref=dst, send_sem=xs.at[i], recv_sem=xr.at[i],
                                            device_id={'tp': far}, device_id_type=pl.DeviceIdType.MESH)

    def project(weights, out, tile=256):
        def body(i, c):
            rows = pl.ds(pl.multiple_of(i * tile, tile), tile)
            out[rows, :] = dot(enc[rows, :], weights[...]).astype(BF16)
            return c
        lax.fori_loop(0, enc.shape[0] // tile, body, 0)

    exchange(0, part_ref)
    for copy in (ld_e0, ld_wk, ld_wv, ld_e1):
        copy.wait()
    project(wkv, kv_own)

    h1 = x_ref[...].astype(F32) + collect(0, part_ref)
    c_norm = layer_norm(h1, g2[...].reshape(1, -1), b2[...].reshape(1, -1))
    ld_wqc.wait()
    qc_s[...] = dot(c_norm, wqc[...]).astype(BF16)
    send_q = to_far(0, qc_s, qc_r)
    send_q.start()
    for copy in (ld_wkr, ld_wvr):
        copy.wait()
    project(wkvr, kv_rem)

    rows = heads * batch
    row_b = lax.rem(lax.broadcasted_iota(jnp.int32, (rows, 128), 0), batch)
    lane = lax.broadcasted_iota(jnp.int32, (rows, 128), 1)
    per = half // batch
    pack = 128 // per
    blocks = half // 128
    mine = lax.rem(row_b, pack) == lane // per
    row_blk = row_b // pack
    lane_head = lax.broadcasted_iota(jnp.int32, (batch, width), 1) // dim

    def attend(q, kv):
        qf = q.astype(F32)
        q_rows = jnp.concatenate([jnp.where(lane_head == h, qf, 0.0) for h in range(heads)], axis=0).astype(BF16)
        parts = []
        for part in range(2):
            s_all = dot_t(q_rows, kv[part * half:(part + 1) * half, 0:width])
            s = s_all[:, 0:128]
            for k in range(1, blocks):
                s = jnp.where(row_blk == k, s_all[:, k * 128:(k + 1) * 128], s)
            parts.append(jnp.where(mine, s * scale, NEG))
        m = jnp.maximum(jnp.max(parts[0], axis=1, keepdims=True), jnp.max(parts[1], axis=1, keepdims=True))
        p = [jnp.exp(s - m) for s in parts]
        l = jnp.sum(p[0], axis=1, keepdims=True) + jnp.sum(p[1], axis=1, keepdims=True)
        o = None
        for part in range(2):
            p_wide = jnp.concatenate([jnp.where(row_blk == k, p[part], 0.0) for k in range(blocks)], axis=1).astype(BF16)
            o_part = dot(p_wide, kv[part * half:(part + 1) * half, width:2 * width])
            o = o_part if o is None else o + o_part
        o = jnp.concatenate([o[h * batch:(h + 1) * batch, h * dim:(h + 1) * dim] for h in range(heads)], axis=0)
        return m, l, o

    send_q.wait()
    m_r, l_r, o_r = attend(qc_r[...], kv_rem)
    o_snd[...] = o_r
    st_snd[...] = jnp.where(lane < 64, m_r, l_r)
    send_o = to_far(1, o_snd, o_rcv)
    send_st = to_far(2, st_snd, st_rcv)
    send_o.start()
    send_st.start()
    m_a, l_a, o_a = attend(qc_s[...], kv_own)
    send_o.wait()
    send_st.wait()
    stats = st_rcv[...]
    m_b, l_b = stats[:, 0:1], stats[:, 64:65]
    m = jnp.maximum(m_a, m_b)
    w_a, w_b = jnp.exp(m_a - m), jnp.exp(m_b - m)
    o = (o_a * w_a + o_rcv[...] * w_b) / (l_a * w_a + l_b * w_b)
    oc = jnp.concatenate([o[h * batch:(h + 1) * batch, :] for h in range(heads)], axis=1).astype(BF16)
    ld_woc.wait()
    send2[...] = dot(oc, woc[...]).astype(BF16)
    exchange(1, send2)
    h2 = h1 + collect(1, send2)
    m_norm = layer_norm(h2, g3[...].reshape(1, -1), b3[...].reshape(1, -1))
    ld_up.wait()
    up = dot(m_norm, wup[...])
    hidden = (0.5 * up * (1.0 + lax.erf(up * (0.5 ** 0.5)))).astype(BF16)
    ld_dn.wait()
    send3[...] = dot(hidden, wdn[...]).astype(BF16)
    exchange(2, send3)
    out_ref[...] = (h2 + collect(2, send3)).astype(BF16)


def local_step(x, k_cache, v_cache, seq_lens, nbr_enc, ln1_gain, ln1_bias, w_q, w_k, w_v, w_o, ln2_gain, ln2_bias, wq_c, wk_c, wv_c, wo_c, ln3_gain, ln3_bias, w_up, w_down):
    batch, d_model = x.shape
    heads, dim = k_cache.shape[2:]
    width = heads * dim
    tp = lax.axis_size('tp')
    far = [(i, (i + 2) % tp) for i in range(tp)]
    near = [(i, i ^ 1) for i in range(tp)]
    enc = nbr_enc.reshape(-1, nbr_enc.shape[-1])
    enc_near = lax.ppermute(enc, 'tp', near)
    wk_far = lax.ppermute(wk_c, 'tp', far)
    wv_far = lax.ppermute(wv_c, 'tp', far)

    any_spec = pl.BlockSpec(memory_space=pltpu.HBM)
    vmem = pl.BlockSpec(memory_space=pltpu.VMEM)
    smem = pl.BlockSpec(memory_space=pltpu.SMEM)
    slots = GROUPS * UNROLL
    part, k_new, v_new = pl.pallas_call(
        functools.partial(self_kernel, batch, heads, dim),
        out_shape=(jax.ShapeDtypeStruct((batch, d_model), BF16), jax.ShapeDtypeStruct((heads, batch, dim), BF16), jax.ShapeDtypeStruct((heads, batch, dim), BF16)),
        in_specs=[smem, vmem, vmem, vmem] + [any_spec] * 6,
        out_specs=(vmem, vmem, vmem),
        scratch_shapes=[
            pltpu.VMEM((d_model, width), BF16), pltpu.VMEM((d_model, width), BF16), pltpu.VMEM((d_model, width), BF16), pltpu.VMEM((width, d_model), BF16),
            pltpu.VMEM((slots, heads, CHUNK, dim), BF16), pltpu.VMEM((slots, heads, CHUNK, dim), BF16),
            pltpu.VMEM((batch + 8, width), F32), pltpu.VMEM((batch, width), F32),
            pltpu.VMEM((batch + 1, 8, dim), F32), pltpu.VMEM((batch + 1, 8, dim), F32), pltpu.VMEM((batch + 1, 8, width), F32),
            pltpu.SemaphoreType.DMA((4,)), pltpu.SemaphoreType.DMA((slots,)), pltpu.SemaphoreType.DMA((slots,)),
        ],
        compiler_params=pltpu.CompilerParams(vmem_limit_bytes=63 * 2**20),
        cost_estimate=pl.CostEstimate(flops=40_000_000_000, bytes_accessed=60_000_000, transcendentals=0),
        name='self_attention',
    )(seq_lens, x, ln1_gain, ln1_bias, jnp.transpose(k_cache, (0, 2, 1, 3)), jnp.transpose(v_cache, (0, 2, 1, 3)), w_q, w_k, w_v, w_o)

    n_enc, enc_dim = enc.shape
    ff = w_up.shape[1]
    out = pl.pallas_call(
        functools.partial(rest_kernel, batch, heads, dim, tp, 'dp'),
        out_shape=jax.ShapeDtypeStruct((batch, d_model), BF16),
        in_specs=[vmem] * 6 + [any_spec] * 10,
        out_specs=vmem,
        scratch_shapes=[
            pltpu.VMEM((d_model, width), BF16), pltpu.VMEM((2 * n_enc, enc_dim), BF16),
            pltpu.VMEM((enc_dim, 2 * width), BF16), pltpu.VMEM((enc_dim, 2 * width), BF16),
            pltpu.VMEM((width, d_model), BF16), pltpu.VMEM((d_model, ff), BF16), pltpu.VMEM((ff, d_model), BF16),
            pltpu.VMEM((2 * n_enc, 2 * width), BF16), pltpu.VMEM((2 * n_enc, 2 * width), BF16),
            pltpu.VMEM((3, tp, batch, d_model), BF16), pltpu.VMEM((batch, d_model), BF16), pltpu.VMEM((batch, d_model), BF16),
            pltpu.VMEM((batch, width), BF16), pltpu.VMEM((batch, width), BF16),
            pltpu.VMEM((heads * batch, dim), F32), pltpu.VMEM((heads * batch, dim), F32), pltpu.VMEM((heads * batch, 128), F32), pltpu.VMEM((heads * batch, 128), F32),
            pltpu.SemaphoreType.DMA((10,)), pltpu.SemaphoreType.DMA((3, tp - 1)), pltpu.SemaphoreType.DMA((3, tp)),
            pltpu.SemaphoreType.DMA((3,)), pltpu.SemaphoreType.DMA((3,)),
        ],
        compiler_params=pltpu.CompilerParams(collective_id=0, has_side_effects=True, vmem_limit_bytes=63 * 2**20),
        cost_estimate=pl.CostEstimate(flops=20_000_000_000, bytes_accessed=30_000_000, transcendentals=0),
        name='rest_of_layer',
    )(part, x, ln2_gain, ln2_bias, ln3_gain, ln3_bias, wq_c, enc, enc_near, wk_c, wv_c, wk_far, wv_far, wo_c, w_up, w_down)
    return out, jnp.transpose(k_new, (1, 0, 2)), jnp.transpose(v_new, (1, 0, 2))


def solution(mesh):
    row_spec = P('dp', None)
    cache_spec = P('dp', None, 'tp', None)
    head_spec = P('dp', 'tp', None)
    vec_spec = P(None)
    col_split = P(None, 'tp')
    row_split = P('tp', None)
    in_specs = (row_spec, cache_spec, cache_spec, P('dp'), P('dp', 'tp', None), vec_spec, vec_spec, col_split, col_split, col_split, row_split, vec_spec, vec_spec, col_split, col_split, col_split, row_split, vec_spec, vec_spec, col_split, row_split)
    out_specs = (row_spec, head_spec, head_spec)
    return jax.shard_map(local_step, mesh=mesh, in_specs=in_specs, out_specs=out_specs, check_vma=False)
```

```python
import functools

import jax
import jax.numpy as jnp
from jax import lax
from jax.experimental import pallas as pl
from jax.experimental.pallas import tpu as pltpu
from jax.sharding import PartitionSpec as P

LN_EPS = 1e-5
NEG = -1e30
F32 = jnp.float32
BF16 = jnp.bfloat16
CHUNK = 1024
UNROLL = 2
GROUPS = 6


def layer_norm(values, ln_gain, ln_bias):
    row_mean = jnp.mean(values, axis=-1, keepdims=True)
    centred = values - row_mean
    row_var = jnp.mean(jnp.square(centred), axis=-1, keepdims=True)
    return (centred * lax.rsqrt(row_var + LN_EPS) * ln_gain + ln_bias).astype(BF16)


def dot(lhs, rhs):
    return jnp.dot(lhs, rhs, preferred_element_type=F32)


def dot_t(lhs, rhs):
    return lax.dot_general(lhs, rhs, (((1,), (1,)), ((), ())), preferred_element_type=F32)


def self_kernel(batch, heads, dim, lens, x_ref, g_ref, b_ref, kc, vc, wq_h, wk_h, wv_h, wo_h,
                part_ref, knew_ref, vnew_ref,
                wq, wk, wv, wo, kbuf, vbuf, q_s, o_s, m_s, l_s, acc_s, wsem, ksem, vsem):
    width = heads * dim
    scale = dim ** -0.5
    loads = [pltpu.make_async_copy(s, d, wsem.at[i]) for i, (s, d) in enumerate(((wq_h, wq), (wk_h, wk), (wv_h, wv), (wo_h, wo)))]
    for copy in loads[:3]:
        copy.start()

    def len_of(seq):
        return jnp.where(seq < batch, lens[jnp.minimum(seq, batch - 1)], 0)

    def following(seq, blk):
        more = (blk + 1) * CHUNK < len_of(seq)
        return jnp.where(more, seq, seq + 1), jnp.where(more, blk + 1, 0)

    def copies(seq, blk, slot):
        rows = pl.ds(pl.multiple_of(blk * CHUNK, CHUNK), CHUNK)
        return (pltpu.make_async_copy(kc.at[seq, :, rows, :], kbuf.at[slot], ksem.at[slot]),
                pltpu.make_async_copy(vc.at[seq, :, rows, :], vbuf.at[slot], vsem.at[slot]))

    def fetch_group(group, ptr):
        for u in range(UNROLL):
            seq, blk = ptr

            @pl.when(seq < batch)
            def _():
                for copy in copies(seq, blk, group * UNROLL + u):
                    copy.start()
            ptr = following(seq, blk)
        return ptr

    ptr = (jnp.int32(0), jnp.int32(0))
    for group in range(GROUPS - 1):
        ptr = fetch_group(group, ptr)
    loads[3].start()

    n_items = jnp.int32(0)
    for seq in range(batch):
        n_items = n_items + lax.div(lens[seq] + (CHUNK - 1), CHUNK)
    n_steps = lax.div(n_items + (UNROLL - 1), UNROLL)

    a_norm = layer_norm(x_ref[...].astype(F32), g_ref[...].reshape(1, -1), b_ref[...].reshape(1, -1))
    loads[0].wait()
    q_new = dot(a_norm, wq[...]).astype(BF16).astype(F32)
    loads[1].wait()
    k_new = dot(a_norm, wk[...]).astype(BF16)
    loads[2].wait()
    v_new = dot(a_norm, wv[...]).astype(BF16)
    for h in range(heads):
        knew_ref[h] = k_new[:, h * dim:(h + 1) * dim]
        vnew_ref[h] = v_new[:, h * dim:(h + 1) * dim]
    q_s[0:batch, :] = q_new
    q_s[batch:, :] = jnp.zeros((q_s.shape[0] - batch, width), F32)
    pair = 2 * dim
    part_rows = CHUNK // 2
    row8 = lax.broadcasted_iota(jnp.int32, (8, 1), 0)
    pair_row = lax.broadcasted_iota(jnp.int32, (8, pair), 0)
    pair_side = lax.broadcasted_iota(jnp.int32, (8, pair), 1) // dim
    sel01 = (pair_row == pair_side).astype(F32)
    sel2 = (pair_row == pair_side + 2).astype(F32)
    qk = q_new * k_new.astype(F32)
    v_f = v_new.astype(F32)
    for seq in range(batch):
        prod = qk[seq:seq + 1, :]
        tail = jnp.concatenate([prod[:, pair:width], jnp.zeros((1, pair - dim), F32)], axis=1)
        s_new = jnp.sum(prod[:, 0:pair] * sel01 + tail * sel2, axis=1, keepdims=True) * scale
        m_s[seq] = jnp.broadcast_to(jnp.where(row8 == 3, NEG, s_new), (8, dim))
        tail_v = jnp.concatenate([v_f[seq:seq + 1, pair:width]] * 2, axis=1)
        acc_s[seq] = jnp.where(pair_row < 2, jnp.broadcast_to(v_f[seq:seq + 1, 0:pair], (8, pair)), jnp.where(pair_row == 2, jnp.broadcast_to(tail_v, (8, pair)), 0.0))
        l_s[seq] = jnp.broadcast_to(jnp.where(row8 == 3, 0.0, 1.0), (8, dim))
    m_s[batch] = jnp.zeros((8, dim), F32)
    l_s[batch] = jnp.ones((8, dim), F32)
    acc_s[batch] = jnp.zeros((8, pair), F32)
    lane = lax.broadcasted_iota(jnp.int32, (8, CHUNK), 1)
    lane2 = lax.broadcasted_iota(jnp.int32, (8, part_rows), 1)

    def step(i, carry):
        ptr, cur = carry[:2], carry[2:]
        group = lax.rem(i, GROUPS)
        ptr = fetch_group(lax.rem(i + GROUPS - 1, GROUPS), ptr)
        items = []
        for u in range(UNROLL):
            items.append((*cur, group * UNROLL + u))
            cur = following(*cur)
        for seq, blk, slot in items:

            @pl.when(seq < batch)
            def _():
                for copy in copies(seq, blk, slot):
                    copy.wait()
        scores = []
        for seq, blk, slot in items:
            q_row = q_s[pl.ds(jnp.minimum(seq, batch), 1), :]
            q01 = (q_row[:, 0:pair] * sel01).astype(BF16)
            q2 = (jnp.concatenate([q_row[:, pair:width]] * 2, axis=1) * sel2).astype(BF16)
            k01 = jnp.concatenate([kbuf[slot, 0], kbuf[slot, 1]], axis=1)
            k2 = jnp.concatenate([kbuf[slot, 2, 0:part_rows, :], kbuf[slot, 2, part_rows:CHUNK, :]], axis=1)
            scores.append((dot_t(q01, k01), dot_t(q2, k2)))
        weights = []
        for (seq, blk, slot), (s01, s2) in zip(items, scores):
            live = len_of(seq) - blk * CHUNK
            s01 = jnp.where(lane < jnp.where(row8 < 2, live, 0), s01 * scale, NEG)
            s2 = jnp.where(lane2 < jnp.where(row8 == 2, live, jnp.where(row8 == 3, live - part_rows, 0)), s2 * scale, NEG)
            m_i = jnp.maximum(jnp.max(s01, axis=1, keepdims=True), jnp.max(s2, axis=1, keepdims=True))
            p01 = jnp.where(row8 < 2, jnp.exp(s01 - m_i), 0.0)
            p2 = jnp.where(row8 < 2, 0.0, jnp.exp(s2 - m_i))
            l_i = jnp.sum(p01, axis=1, keepdims=True) + jnp.sum(p2, axis=1, keepdims=True)
            weights.append((m_i, l_i, p01.astype(BF16), p2.astype(BF16)))
        values = []
        for (seq, blk, slot), (m_i, l_i, p01, p2) in zip(items, weights):
            v01 = jnp.concatenate([vbuf[slot, 0], vbuf[slot, 1]], axis=1)
            v2 = jnp.concatenate([vbuf[slot, 2, 0:part_rows, :], vbuf[slot, 2, part_rows:CHUNK, :]], axis=1)
            values.append(dot(p01, v01) + dot(p2, v2))
        for (seq, blk, slot), (m_i, l_i, p01, p2), pv in zip(items, weights, values):
            row = jnp.minimum(seq, batch)
            m_old = m_s[row]
            m_new = jnp.maximum(m_old, m_i)
            keep = jnp.exp(m_old - m_new)
            add = jnp.exp(m_i - m_new)
            m_s[row] = m_new
            l_s[row] = l_s[row] * keep + l_i * add
            acc_s[row] = acc_s[row] * jnp.concatenate([keep] * 2, axis=1) + pv * jnp.concatenate([add] * 2, axis=1)
        return (*ptr, *cur)

    lax.fori_loop(0, n_steps, step, (*ptr, jnp.int32(0), jnp.int32(0)))
    for seq in range(batch):
        m, l, acc = m_s[seq], l_s[seq], acc_s[seq]
        top = jnp.maximum(m[2:3], m[3:4])
        w_a, w_b = jnp.exp(m[2:3] - top), jnp.exp(m[3:4] - top)
        o2 = (acc[2:3, 0:dim] * w_a + acc[3:4, dim:pair] * w_b) / (l[2:3] * w_a + l[3:4] * w_b)
        o_s[seq:seq + 1, :] = jnp.concatenate([acc[0:1, 0:dim] / l[0:1], acc[1:2, dim:pair] / l[1:2], o2], axis=1)
    loads[3].wait()
    part_ref[...] = dot(o_s[...].astype(BF16), wo[...]).astype(BF16)


def rest_kernel(batch, heads, dim, tp, dp_name, part_ref, x_ref, g2, b2, g3, b3, wqc_h, e_own_h, e_par_h, wk_h, wv_h, wkr_h, wvr_h, woc_h, wup_h, wdn_h,
                out_ref,
                wqc, enc, wkv, wkvr, woc, wup, wdn, kv_own, kv_rem, recv, send2, send3, qc_s, qc_r, o_snd, o_rcv, st_snd, st_rcv,
                lsem, ssem, rsem, xs, xr):
    width = heads * dim
    scale = dim ** -0.5
    me = lax.axis_index('tp')
    far = lax.rem(me + 2, tp)
    half = enc.shape[0] // 2

    def load(i, src, dst):
        copy = pltpu.make_async_copy(src, dst, lsem.at[i])
        copy.start()
        return copy

    ld_e0 = load(0, e_own_h, enc.at[pl.ds(0, half), :])
    ld_wk = load(1, wk_h, wkv.at[:, pl.ds(0, width)])
    ld_wv = load(2, wv_h, wkv.at[:, pl.ds(width, width)])
    ld_e1 = load(3, e_par_h, enc.at[pl.ds(half, half), :])
    ld_wqc = load(4, wqc_h, wqc)
    ld_wkr = load(5, wkr_h, wkvr.at[:, pl.ds(0, width)])
    ld_wvr = load(6, wvr_h, wkvr.at[:, pl.ds(width, width)])
    ld_woc = load(7, woc_h, woc)
    ld_up = load(8, wup_h, wup)
    ld_dn = load(9, wdn_h, wdn)

    barrier = pltpu.get_barrier_semaphore()
    for d in range(1, tp):
        pl.semaphore_signal(barrier, inc=1, device_id={'tp': lax.rem(me + d, tp)}, device_id_type=pl.DeviceIdType.MESH)
    pl.semaphore_wait(barrier, tp - 1)

    def exchange(n, src):
        for d in range(1, tp):
            pltpu.make_async_remote_copy(src_ref=src, dst_ref=recv.at[n, me], send_sem=ssem.at[n, d - 1], recv_sem=rsem.at[n, me],
                                         device_id={'tp': lax.rem(me + d, tp)}, device_id_type=pl.DeviceIdType.MESH).start()
        recv[n, me] = src[...]

    def collect(n, src):
        for d in range(1, tp):
            other = lax.rem(me + d, tp)
            pltpu.make_async_remote_copy(src_ref=src, dst_ref=recv.at[n, other], send_sem=ssem.at[n, d - 1], recv_sem=rsem.at[n, other],
                                         device_id={'tp': other}, device_id_type=pl.DeviceIdType.MESH).wait()
        total = recv[n, 0].astype(F32)
        for t in range(1, tp):
            total = total + recv[n, t].astype(F32)
        return total

    def to_far(i, src, dst):
        return pltpu.make_async_remote_copy(src_ref=src, dst_ref=dst, send_sem=xs.at[i], recv_sem=xr.at[i],
                                            device_id={'tp': far}, device_id_type=pl.DeviceIdType.MESH)

    def project(weights, out, tile=256):
        def body(i, c):
            rows = pl.ds(pl.multiple_of(i * tile, tile), tile)
            out[rows, :] = dot(enc[rows, :], weights[...]).astype(BF16)
            return c
        lax.fori_loop(0, enc.shape[0] // tile, body, 0)

    exchange(0, part_ref)
    for copy in (ld_e0, ld_wk, ld_wv, ld_e1):
        copy.wait()
    project(wkv, kv_own)

    h1 = x_ref[...].astype(F32) + collect(0, part_ref)
    c_norm = layer_norm(h1, g2[...].reshape(1, -1), b2[...].reshape(1, -1))
    ld_wqc.wait()
    qc_s[...] = dot(c_norm, wqc[...]).astype(BF16)
    send_q = to_far(0, qc_s, qc_r)
    send_q.start()
    for copy in (ld_wkr, ld_wvr):
        copy.wait()
    project(wkvr, kv_rem)

    rows = heads * batch
    row_b = lax.rem(lax.broadcasted_iota(jnp.int32, (rows, 128), 0), batch)
    lane = lax.broadcasted_iota(jnp.int32, (rows, 128), 1)
    per = half // batch
    pack = 128 // per
    blocks = half // 128
    mine = lax.rem(row_b, pack) == lane // per
    row_blk = row_b // pack
    lane_head = lax.broadcasted_iota(jnp.int32, (batch, width), 1) // dim

    def attend(q, kv):
        qf = q.astype(F32)
        q_rows = jnp.concatenate([jnp.where(lane_head == h, qf, 0.0) for h in range(heads)], axis=0).astype(BF16)
        parts = []
        for part in range(2):
            s_all = dot_t(q_rows, kv[part * half:(part + 1) * half, 0:width])
            s = s_all[:, 0:128]
            for k in range(1, blocks):
                s = jnp.where(row_blk == k, s_all[:, k * 128:(k + 1) * 128], s)
            parts.append(jnp.where(mine, s * scale, NEG))
        m = jnp.maximum(jnp.max(parts[0], axis=1, keepdims=True), jnp.max(parts[1], axis=1, keepdims=True))
        p = [jnp.exp(s - m) for s in parts]
        l = jnp.sum(p[0], axis=1, keepdims=True) + jnp.sum(p[1], axis=1, keepdims=True)
        o = None
        for part in range(2):
            p_wide = jnp.concatenate([jnp.where(row_blk == k, p[part], 0.0) for k in range(blocks)], axis=1).astype(BF16)
            o_part = dot(p_wide, kv[part * half:(part + 1) * half, width:2 * width])
            o = o_part if o is None else o + o_part
        o = jnp.concatenate([o[h * batch:(h + 1) * batch, h * dim:(h + 1) * dim] for h in range(heads)], axis=0)
        return m, l, o

    send_q.wait()
    m_r, l_r, o_r = attend(qc_r[...], kv_rem)
    o_snd[...] = o_r
    st_snd[...] = jnp.where(lane < 64, m_r, l_r)
    send_o = to_far(1, o_snd, o_rcv)
    send_st = to_far(2, st_snd, st_rcv)
    send_o.start()
    send_st.start()
    m_a, l_a, o_a = attend(qc_s[...], kv_own)
    send_o.wait()
    send_st.wait()
    stats = st_rcv[...]
    m_b, l_b = stats[:, 0:1], stats[:, 64:65]
    m = jnp.maximum(m_a, m_b)
    w_a, w_b = jnp.exp(m_a - m), jnp.exp(m_b - m)
    o = (o_a * w_a + o_rcv[...] * w_b) / (l_a * w_a + l_b * w_b)
    oc = jnp.concatenate([o[h * batch:(h + 1) * batch, :] for h in range(heads)], axis=1).astype(BF16)
    ld_woc.wait()
    send2[...] = dot(oc, woc[...]).astype(BF16)
    exchange(1, send2)
    h2 = h1 + collect(1, send2)
    m_norm = layer_norm(h2, g3[...].reshape(1, -1), b3[...].reshape(1, -1))
    ld_up.wait()
    up = dot(m_norm, wup[...])
    hidden = (0.5 * up * (1.0 + lax.erf(up * (0.5 ** 0.5)))).astype(BF16)
    ld_dn.wait()
    send3[...] = dot(hidden, wdn[...]).astype(BF16)
    exchange(2, send3)
    out_ref[...] = (h2 + collect(2, send3)).astype(BF16)


def local_step(x, k_cache, v_cache, seq_lens, nbr_enc, ln1_gain, ln1_bias, w_q, w_k, w_v, w_o, ln2_gain, ln2_bias, wq_c, wk_c, wv_c, wo_c, ln3_gain, ln3_bias, w_up, w_down):
    batch, d_model = x.shape
    heads, dim = k_cache.shape[2:]
    width = heads * dim
    tp = lax.axis_size('tp')
    far = [(i, (i + 2) % tp) for i in range(tp)]
    near = [(i, i ^ 1) for i in range(tp)]
    enc = nbr_enc.reshape(-1, nbr_enc.shape[-1])
    enc_near = lax.ppermute(enc, 'tp', near)
    wk_far = lax.ppermute(wk_c, 'tp', far)
    wv_far = lax.ppermute(wv_c, 'tp', far)

    any_spec = pl.BlockSpec(memory_space=pltpu.HBM)
    vmem = pl.BlockSpec(memory_space=pltpu.VMEM)
    smem = pl.BlockSpec(memory_space=pltpu.SMEM)
    slots = GROUPS * UNROLL
    part, k_new, v_new = pl.pallas_call(
        functools.partial(self_kernel, batch, heads, dim),
        out_shape=(jax.ShapeDtypeStruct((batch, d_model), BF16), jax.ShapeDtypeStruct((heads, batch, dim), BF16), jax.ShapeDtypeStruct((heads, batch, dim), BF16)),
        in_specs=[smem, vmem, vmem, vmem] + [any_spec] * 6,
        out_specs=(vmem, vmem, vmem),
        scratch_shapes=[
            pltpu.VMEM((d_model, width), BF16), pltpu.VMEM((d_model, width), BF16), pltpu.VMEM((d_model, width), BF16), pltpu.VMEM((width, d_model), BF16),
            pltpu.VMEM((slots, heads, CHUNK, dim), BF16), pltpu.VMEM((slots, heads, CHUNK, dim), BF16),
            pltpu.VMEM((batch + 8, width), F32), pltpu.VMEM((batch, width), F32),
            pltpu.VMEM((batch + 1, 8, dim), F32), pltpu.VMEM((batch + 1, 8, dim), F32), pltpu.VMEM((batch + 1, 8, 2 * dim), F32),
            pltpu.SemaphoreType.DMA((4,)), pltpu.SemaphoreType.DMA((slots,)), pltpu.SemaphoreType.DMA((slots,)),
        ],
        compiler_params=pltpu.CompilerParams(vmem_limit_bytes=63 * 2**20),
        cost_estimate=pl.CostEstimate(flops=40_000_000_000, bytes_accessed=60_000_000, transcendentals=0),
        name='self_attention',
    )(seq_lens, x, ln1_gain, ln1_bias, jnp.transpose(k_cache, (0, 2, 1, 3)), jnp.transpose(v_cache, (0, 2, 1, 3)), w_q, w_k, w_v, w_o)

    n_enc, enc_dim = enc.shape
    ff = w_up.shape[1]
    out = pl.pallas_call(
        functools.partial(rest_kernel, batch, heads, dim, tp, 'dp'),
        out_shape=jax.ShapeDtypeStruct((batch, d_model), BF16),
        in_specs=[vmem] * 6 + [any_spec] * 10,
        out_specs=vmem,
        scratch_shapes=[
            pltpu.VMEM((d_model, width), BF16), pltpu.VMEM((2 * n_enc, enc_dim), BF16),
            pltpu.VMEM((enc_dim, 2 * width), BF16), pltpu.VMEM((enc_dim, 2 * width), BF16),
            pltpu.VMEM((width, d_model), BF16), pltpu.VMEM((d_model, ff), BF16), pltpu.VMEM((ff, d_model), BF16),
            pltpu.VMEM((2 * n_enc, 2 * width), BF16), pltpu.VMEM((2 * n_enc, 2 * width), BF16),
            pltpu.VMEM((3, tp, batch, d_model), BF16), pltpu.VMEM((batch, d_model), BF16), pltpu.VMEM((batch, d_model), BF16),
            pltpu.VMEM((batch, width), BF16), pltpu.VMEM((batch, width), BF16),
            pltpu.VMEM((heads * batch, dim), F32), pltpu.VMEM((heads * batch, dim), F32), pltpu.VMEM((heads * batch, 128), F32), pltpu.VMEM((heads * batch, 128), F32),
            pltpu.SemaphoreType.DMA((10,)), pltpu.SemaphoreType.DMA((3, tp - 1)), pltpu.SemaphoreType.DMA((3, tp)),
            pltpu.SemaphoreType.DMA((3,)), pltpu.SemaphoreType.DMA((3,)),
        ],
        compiler_params=pltpu.CompilerParams(collective_id=0, has_side_effects=True, vmem_limit_bytes=63 * 2**20),
        cost_estimate=pl.CostEstimate(flops=20_000_000_000, bytes_accessed=30_000_000, transcendentals=0),
        name='rest_of_layer',
    )(part, x, ln2_gain, ln2_bias, ln3_gain, ln3_bias, wq_c, enc, enc_near, wk_c, wv_c, wk_far, wv_far, wo_c, w_up, w_down)
    return out, jnp.transpose(k_new, (1, 0, 2)), jnp.transpose(v_new, (1, 0, 2))


def solution(mesh):
    row_spec = P('dp', None)
    cache_spec = P('dp', None, 'tp', None)
    head_spec = P('dp', 'tp', None)
    vec_spec = P(None)
    col_split = P(None, 'tp')
    row_split = P('tp', None)
    in_specs = (row_spec, cache_spec, cache_spec, P('dp'), P('dp', 'tp', None), vec_spec, vec_spec, col_split, col_split, col_split, row_split, vec_spec, vec_spec, col_split, col_split, col_split, row_split, vec_spec, vec_spec, col_split, row_split)
    out_specs = (row_spec, head_spec, head_spec)
    return jax.shard_map(local_step, mesh=mesh, in_specs=in_specs, out_specs=out_specs, check_vma=False)
```

```python
import functools

import jax
import jax.numpy as jnp
from jax import lax
from jax.experimental import pallas as pl
from jax.experimental.pallas import tpu as pltpu
from jax.sharding import PartitionSpec as P

LN_EPS = 1e-5
NEG = -1e30
F32 = jnp.float32
BF16 = jnp.bfloat16
CHUNK = 512
UNROLL = 4
GRAIN = 64
GROUPS = 6


def layer_norm(values, ln_gain, ln_bias):
    row_mean = jnp.mean(values, axis=-1, keepdims=True)
    centred = values - row_mean
    row_var = jnp.mean(jnp.square(centred), axis=-1, keepdims=True)
    return (centred * lax.rsqrt(row_var + LN_EPS) * ln_gain + ln_bias).astype(BF16)


def dot(lhs, rhs):
    return jnp.dot(lhs, rhs, preferred_element_type=F32)


def dot_t(lhs, rhs):
    return lax.dot_general(lhs, rhs, (((1,), (1,)), ((), ())), preferred_element_type=F32)


def self_kernel(batch, heads, dim, lens, x_ref, g_ref, b_ref, kc, vc, wq_h, wk_h, wv_h, wo_h,
                part_ref, knew_ref, vnew_ref,
                wq, wk, wv, wo, kbuf, vbuf, q_s, o_s, m_s, l_s, acc_s, wsem, ksem, vsem):
    width = heads * dim
    scale = dim ** -0.5
    loads = [pltpu.make_async_copy(s, d, wsem.at[i]) for i, (s, d) in enumerate(((wq_h, wq), (wk_h, wk), (wv_h, wv), (wo_h, wo)))]
    for copy in loads[:3]:
        copy.start()

    def len_of(seq):
        return jnp.where(seq < batch, lens[jnp.minimum(seq, batch - 1)], 0)

    def following(seq, blk):
        more = (blk + 1) * CHUNK < len_of(seq)
        return jnp.where(more, seq, seq + 1), jnp.where(more, blk + 1, 0)

    def copies(seq, blk, slot, whole):
        live = CHUNK if whole else pl.multiple_of(jnp.minimum(len_of(seq) - blk * CHUNK, CHUNK), GRAIN)
        src = pl.ds(pl.multiple_of(blk * CHUNK, CHUNK), live)
        dst = pl.ds(0, live)
        return (pltpu.make_async_copy(kc.at[seq, :, src, :], kbuf.at[slot, :, dst, :], ksem.at[slot]),
                pltpu.make_async_copy(vc.at[seq, :, src, :], vbuf.at[slot, :, dst, :], vsem.at[slot]))

    def fetch_group(group, ptr, whole):
        for u in range(UNROLL):
            seq, blk = ptr

            @pl.when(seq < batch)
            def _():
                for copy in copies(seq, blk, group * UNROLL + u, whole):
                    copy.start()
            ptr = following(seq, blk)
        return ptr

    ptr = (jnp.int32(0), jnp.int32(0))
    for group in range(GROUPS):
        ptr = fetch_group(group, ptr, True)
    loads[3].start()

    n_items = jnp.int32(0)
    for seq in range(batch):
        n_items = n_items + lax.div(lens[seq] + (CHUNK - 1), CHUNK)
    n_steps = lax.div(n_items + (UNROLL - 1), UNROLL)

    a_norm = layer_norm(x_ref[...].astype(F32), g_ref[...].reshape(1, -1), b_ref[...].reshape(1, -1))
    loads[0].wait()
    q_new = dot(a_norm, wq[...]).astype(BF16).astype(F32)
    loads[1].wait()
    k_new = dot(a_norm, wk[...]).astype(BF16)
    loads[2].wait()
    v_new = dot(a_norm, wv[...]).astype(BF16)
    for h in range(heads):
        knew_ref[h] = k_new[:, h * dim:(h + 1) * dim]
        vnew_ref[h] = v_new[:, h * dim:(h + 1) * dim]
    q_s[0:batch, :] = q_new
    q_s[batch:, :] = jnp.zeros((q_s.shape[0] - batch, width), F32)
    pair = 2 * dim
    part_rows = CHUNK // 2
    row8 = lax.broadcasted_iota(jnp.int32, (8, 1), 0)
    pair_row = lax.broadcasted_iota(jnp.int32, (8, pair), 0)
    pair_side = lax.broadcasted_iota(jnp.int32, (8, pair), 1) // dim
    sel01 = (pair_row == pair_side).astype(F32)
    sel2 = (pair_row == pair_side + 2).astype(F32)
    qk = q_new * k_new.astype(F32)
    v_f = v_new.astype(F32)
    for seq in range(batch):
        prod = qk[seq:seq + 1, :]
        tail = jnp.concatenate([prod[:, pair:width], jnp.zeros((1, pair - dim), F32)], axis=1)
        s_new = jnp.sum(prod[:, 0:pair] * sel01 + tail * sel2, axis=1, keepdims=True) * scale
        m_s[seq] = jnp.broadcast_to(jnp.where(row8 == 3, NEG, s_new), (8, dim))
        tail_v = jnp.concatenate([v_f[seq:seq + 1, pair:width]] * 2, axis=1)
        acc_s[seq] = jnp.where(pair_row < 2, jnp.broadcast_to(v_f[seq:seq + 1, 0:pair], (8, pair)), jnp.where(pair_row == 2, jnp.broadcast_to(tail_v, (8, pair)), 0.0))
        l_s[seq] = jnp.broadcast_to(jnp.where(row8 == 3, 0.0, 1.0), (8, dim))
    m_s[batch] = jnp.zeros((8, dim), F32)
    l_s[batch] = jnp.ones((8, dim), F32)
    acc_s[batch] = jnp.zeros((8, pair), F32)
    lane = lax.broadcasted_iota(jnp.int32, (8, CHUNK), 1)
    lane2 = lax.broadcasted_iota(jnp.int32, (8, part_rows), 1)

    def step(i, carry):
        ptr, cur = carry[:2], carry[2:]
        group = lax.rem(i, GROUPS)
        items = []
        for u in range(UNROLL):
            items.append((*cur, group * UNROLL + u))
            cur = following(*cur)
        for seq, blk, slot in items:

            @pl.when((seq < batch) & (i < GROUPS))
            def _():
                for copy in copies(seq, blk, slot, True):
                    copy.wait()

            @pl.when((seq < batch) & (i >= GROUPS))
            def _():
                for copy in copies(seq, blk, slot, False):
                    copy.wait()
        scores = []
        for seq, blk, slot in items:
            q_row = q_s[pl.ds(jnp.minimum(seq, batch), 1), :]
            q01 = (q_row[:, 0:pair] * sel01).astype(BF16)
            q2 = (jnp.concatenate([q_row[:, pair:width]] * 2, axis=1) * sel2).astype(BF16)
            k01 = jnp.concatenate([kbuf[slot, 0], kbuf[slot, 1]], axis=1)
            k2 = jnp.concatenate([kbuf[slot, 2, 0:part_rows, :], kbuf[slot, 2, part_rows:CHUNK, :]], axis=1)
            scores.append((dot_t(q01, k01), dot_t(q2, k2)))
        weights = []
        for (seq, blk, slot), (s01, s2) in zip(items, scores):
            live = len_of(seq) - blk * CHUNK
            s01 = jnp.where(lane < jnp.where(row8 < 2, live, 0), s01 * scale, NEG)
            s2 = jnp.where(lane2 < jnp.where(row8 == 2, live, jnp.where(row8 == 3, live - part_rows, 0)), s2 * scale, NEG)
            m_i = jnp.maximum(jnp.max(s01, axis=1, keepdims=True), jnp.max(s2, axis=1, keepdims=True))
            p01 = jnp.where(row8 < 2, jnp.exp(s01 - m_i), 0.0)
            p2 = jnp.where(row8 < 2, 0.0, jnp.exp(s2 - m_i))
            l_i = jnp.sum(p01, axis=1, keepdims=True) + jnp.sum(p2, axis=1, keepdims=True)
            weights.append((m_i, l_i, p01.astype(BF16), p2.astype(BF16)))
        values = []
        for (seq, blk, slot), (m_i, l_i, p01, p2) in zip(items, weights):
            v01 = jnp.concatenate([vbuf[slot, 0], vbuf[slot, 1]], axis=1)
            v2 = jnp.concatenate([vbuf[slot, 2, 0:part_rows, :], vbuf[slot, 2, part_rows:CHUNK, :]], axis=1)
            values.append(dot(p01, v01) + dot(p2, v2))
        for (seq, blk, slot), (m_i, l_i, p01, p2), pv in zip(items, weights, values):
            row = jnp.minimum(seq, batch)
            m_old = m_s[row]
            m_new = jnp.maximum(m_old, m_i)
            keep = jnp.exp(m_old - m_new)
            add = jnp.exp(m_i - m_new)
            m_s[row] = m_new
            l_s[row] = l_s[row] * keep + l_i * add
            acc_s[row] = acc_s[row] * jnp.concatenate([keep] * 2, axis=1) + pv * jnp.concatenate([add] * 2, axis=1)
        ptr = fetch_group(group, ptr, False)
        return (*ptr, *cur)

    lax.fori_loop(0, n_steps, step, (*ptr, jnp.int32(0), jnp.int32(0)))
    for seq in range(batch):
        m, l, acc = m_s[seq], l_s[seq], acc_s[seq]
        top = jnp.maximum(m[2:3], m[3:4])
        w_a, w_b = jnp.exp(m[2:3] - top), jnp.exp(m[3:4] - top)
        o2 = (acc[2:3, 0:dim] * w_a + acc[3:4, dim:pair] * w_b) / (l[2:3] * w_a + l[3:4] * w_b)
        o_s[seq:seq + 1, :] = jnp.concatenate([acc[0:1, 0:dim] / l[0:1], acc[1:2, dim:pair] / l[1:2], o2], axis=1)
    loads[3].wait()
    part_ref[...] = dot(o_s[...].astype(BF16), wo[...]).astype(BF16)


def rest_kernel(batch, heads, dim, tp, dp_name, part_ref, x_ref, g2, b2, g3, b3, wqc_h, e_own_h, e_par_h, wk_h, wv_h, wkr_h, wvr_h, woc_h, wup_h, wdn_h,
                out_ref,
                wqc, enc, wkv, wkvr, woc, wup, wdn, kv_own, kv_rem, recv, send2, send3, qc_s, qc_r, o_snd, o_rcv, st_snd, st_rcv,
                lsem, ssem, rsem, xs, xr):
    width = heads * dim
    scale = dim ** -0.5
    me = lax.axis_index('tp')
    far = lax.rem(me + 2, tp)
    half = enc.shape[0] // 2

    def load(i, src, dst):
        copy = pltpu.make_async_copy(src, dst, lsem.at[i])
        copy.start()
        return copy

    ld_e0 = load(0, e_own_h, enc.at[pl.ds(0, half), :])
    ld_wk = load(1, wk_h, wkv.at[:, pl.ds(0, width)])
    ld_wv = load(2, wv_h, wkv.at[:, pl.ds(width, width)])
    ld_e1 = load(3, e_par_h, enc.at[pl.ds(half, half), :])
    ld_wqc = load(4, wqc_h, wqc)
    ld_wkr = load(5, wkr_h, wkvr.at[:, pl.ds(0, width)])
    ld_wvr = load(6, wvr_h, wkvr.at[:, pl.ds(width, width)])
    ld_woc = load(7, woc_h, woc)
    ld_up = load(8, wup_h, wup)
    ld_dn = load(9, wdn_h, wdn)

    barrier = pltpu.get_barrier_semaphore()
    for d in range(1, tp):
        pl.semaphore_signal(barrier, inc=1, device_id={'tp': lax.rem(me + d, tp)}, device_id_type=pl.DeviceIdType.MESH)
    pl.semaphore_wait(barrier, tp - 1)

    def exchange(n, src):
        for d in range(1, tp):
            pltpu.make_async_remote_copy(src_ref=src, dst_ref=recv.at[n, me], send_sem=ssem.at[n, d - 1], recv_sem=rsem.at[n, me],
                                         device_id={'tp': lax.rem(me + d, tp)}, device_id_type=pl.DeviceIdType.MESH).start()
        recv[n, me] = src[...]

    def collect(n, src):
        for d in range(1, tp):
            other = lax.rem(me + d, tp)
            pltpu.make_async_remote_copy(src_ref=src, dst_ref=recv.at[n, other], send_sem=ssem.at[n, d - 1], recv_sem=rsem.at[n, other],
                                         device_id={'tp': other}, device_id_type=pl.DeviceIdType.MESH).wait()
        total = recv[n, 0].astype(F32)
        for t in range(1, tp):
            total = total + recv[n, t].astype(F32)
        return total

    def to_far(i, src, dst):
        return pltpu.make_async_remote_copy(src_ref=src, dst_ref=dst, send_sem=xs.at[i], recv_sem=xr.at[i],
                                            device_id={'tp': far}, device_id_type=pl.DeviceIdType.MESH)

    def project(weights, out, tile=256):
        def body(i, c):
            rows = pl.ds(pl.multiple_of(i * tile, tile), tile)
            out[rows, :] = dot(enc[rows, :], weights[...]).astype(BF16)
            return c
        lax.fori_loop(0, enc.shape[0] // tile, body, 0)

    exchange(0, part_ref)
    for copy in (ld_e0, ld_wk, ld_wv, ld_e1):
        copy.wait()
    project(wkv, kv_own)

    h1 = x_ref[...].astype(F32) + collect(0, part_ref)
    c_norm = layer_norm(h1, g2[...].reshape(1, -1), b2[...].reshape(1, -1))
    ld_wqc.wait()
    qc_s[...] = dot(c_norm, wqc[...]).astype(BF16)
    send_q = to_far(0, qc_s, qc_r)
    send_q.start()
    for copy in (ld_wkr, ld_wvr):
        copy.wait()
    project(wkvr, kv_rem)

    rows = heads * batch
    row_b = lax.rem(lax.broadcasted_iota(jnp.int32, (rows, 128), 0), batch)
    lane = lax.broadcasted_iota(jnp.int32, (rows, 128), 1)
    per = half // batch
    pack = 128 // per
    blocks = half // 128
    mine = lax.rem(row_b, pack) == lane // per
    row_blk = row_b // pack
    lane_head = lax.broadcasted_iota(jnp.int32, (batch, width), 1) // dim

    def attend(q, kv):
        qf = q.astype(F32)
        q_rows = jnp.concatenate([jnp.where(lane_head == h, qf, 0.0) for h in range(heads)], axis=0).astype(BF16)
        parts = []
        for part in range(2):
            s_all = dot_t(q_rows, kv[part * half:(part + 1) * half, 0:width])
            s = s_all[:, 0:128]
            for k in range(1, blocks):
                s = jnp.where(row_blk == k, s_all[:, k * 128:(k + 1) * 128], s)
            parts.append(jnp.where(mine, s * scale, NEG))
        m = jnp.maximum(jnp.max(parts[0], axis=1, keepdims=True), jnp.max(parts[1], axis=1, keepdims=True))
        p = [jnp.exp(s - m) for s in parts]
        l = jnp.sum(p[0], axis=1, keepdims=True) + jnp.sum(p[1], axis=1, keepdims=True)
        o = None
        for part in range(2):
            p_wide = jnp.concatenate([jnp.where(row_blk == k, p[part], 0.0) for k in range(blocks)], axis=1).astype(BF16)
            o_part = dot(p_wide, kv[part * half:(part + 1) * half, width:2 * width])
            o = o_part if o is None else o + o_part
        o = jnp.concatenate([o[h * batch:(h + 1) * batch, h * dim:(h + 1) * dim] for h in range(heads)], axis=0)
        return m, l, o

    send_q.wait()
    m_r, l_r, o_r = attend(qc_r[...], kv_rem)
    o_snd[...] = o_r
    st_snd[...] = jnp.where(lane < 64, m_r, l_r)
    send_o = to_far(1, o_snd, o_rcv)
    send_st = to_far(2, st_snd, st_rcv)
    send_o.start()
    send_st.start()
    m_a, l_a, o_a = attend(qc_s[...], kv_own)
    send_o.wait()
    send_st.wait()
    stats = st_rcv[...]
    m_b, l_b = stats[:, 0:1], stats[:, 64:65]
    m = jnp.maximum(m_a, m_b)
    w_a, w_b = jnp.exp(m_a - m), jnp.exp(m_b - m)
    o = (o_a * w_a + o_rcv[...] * w_b) / (l_a * w_a + l_b * w_b)
    oc = jnp.concatenate([o[h * batch:(h + 1) * batch, :] for h in range(heads)], axis=1).astype(BF16)
    ld_woc.wait()
    send2[...] = dot(oc, woc[...]).astype(BF16)
    exchange(1, send2)
    h2 = h1 + collect(1, send2)
    m_norm = layer_norm(h2, g3[...].reshape(1, -1), b3[...].reshape(1, -1))
    ld_up.wait()
    up = dot(m_norm, wup[...])
    hidden = (0.5 * up * (1.0 + lax.erf(up * (0.5 ** 0.5)))).astype(BF16)
    ld_dn.wait()
    send3[...] = dot(hidden, wdn[...]).astype(BF16)
    exchange(2, send3)
    out_ref[...] = h2 + collect(2, send3)


def local_step(x, k_cache, v_cache, seq_lens, nbr_enc, ln1_gain, ln1_bias, w_q, w_k, w_v, w_o, ln2_gain, ln2_bias, wq_c, wk_c, wv_c, wo_c, ln3_gain, ln3_bias, w_up, w_down):
    batch, d_model = x.shape
    heads, dim = k_cache.shape[2:]
    width = heads * dim
    tp = lax.axis_size('tp')
    far = [(i, (i + 2) % tp) for i in range(tp)]
    near = [(i, i ^ 1) for i in range(tp)]
    enc = nbr_enc.reshape(-1, nbr_enc.shape[-1])
    enc_near = lax.ppermute(enc, 'tp', near)
    wk_far = lax.ppermute(wk_c, 'tp', far)
    wv_far = lax.ppermute(wv_c, 'tp', far)

    any_spec = pl.BlockSpec(memory_space=pl.ANY)
    hbm = pl.BlockSpec(memory_space=pltpu.HBM)
    vmem = pl.BlockSpec(memory_space=pltpu.VMEM)
    smem = pl.BlockSpec(memory_space=pltpu.SMEM)
    slots = GROUPS * UNROLL
    part, k_new, v_new = pl.pallas_call(
        functools.partial(self_kernel, batch, heads, dim),
        out_shape=(jax.ShapeDtypeStruct((batch, d_model), BF16), jax.ShapeDtypeStruct((heads, batch, dim), BF16), jax.ShapeDtypeStruct((heads, batch, dim), BF16)),
        in_specs=[smem, vmem, vmem, vmem] + [hbm] * 6,
        out_specs=(vmem, vmem, vmem),
        scratch_shapes=[
            pltpu.VMEM((d_model, width), BF16), pltpu.VMEM((d_model, width), BF16), pltpu.VMEM((d_model, width), BF16), pltpu.VMEM((width, d_model), BF16),
            pltpu.VMEM((slots, heads, CHUNK, dim), BF16), pltpu.VMEM((slots, heads, CHUNK, dim), BF16),
            pltpu.VMEM((batch + 8, width), F32), pltpu.VMEM((batch, width), F32),
            pltpu.VMEM((batch + 1, 8, dim), F32), pltpu.VMEM((batch + 1, 8, dim), F32), pltpu.VMEM((batch + 1, 8, 2 * dim), F32),
            pltpu.SemaphoreType.DMA((4,)), pltpu.SemaphoreType.DMA((slots,)), pltpu.SemaphoreType.DMA((slots,)),
        ],
        compiler_params=pltpu.CompilerParams(vmem_limit_bytes=63*2**20),
        cost_estimate=pl.CostEstimate(flops=40_000_000_000, bytes_accessed=60_000_000, transcendentals=0),
        name='self_attention',
    )(seq_lens, x, ln1_gain, ln1_bias, jnp.transpose(k_cache, (0, 2, 1, 3)), jnp.transpose(v_cache, (0, 2, 1, 3)), w_q, w_k, w_v, w_o)

    n_enc, enc_dim = enc.shape
    ff = w_up.shape[1]
    out = pl.pallas_call(
        functools.partial(rest_kernel, batch, heads, dim, tp, 'dp'),
        out_shape=jax.ShapeDtypeStruct((batch, d_model), F32),
        in_specs=[vmem] * 6 + [hbm, hbm, any_spec, hbm, hbm, any_spec, any_spec, hbm, hbm, hbm],
        out_specs=vmem,
        scratch_shapes=[
            pltpu.VMEM((d_model, width), BF16), pltpu.VMEM((2 * n_enc, enc_dim), BF16),
            pltpu.VMEM((enc_dim, 2 * width), BF16), pltpu.VMEM((enc_dim, 2 * width), BF16),
            pltpu.VMEM((width, d_model), BF16), pltpu.VMEM((d_model, ff), BF16), pltpu.VMEM((ff, d_model), BF16),
            pltpu.VMEM((2 * n_enc, 2 * width), BF16), pltpu.VMEM((2 * n_enc, 2 * width), BF16),
            pltpu.VMEM((3, tp, batch, d_model), BF16), pltpu.VMEM((batch, d_model), BF16), pltpu.VMEM((batch, d_model), BF16),
            pltpu.VMEM((batch, width), BF16), pltpu.VMEM((batch, width), BF16),
            pltpu.VMEM((heads * batch, dim), F32), pltpu.VMEM((heads * batch, dim), F32), pltpu.VMEM((heads * batch, 128), F32), pltpu.VMEM((heads * batch, 128), F32),
            pltpu.SemaphoreType.DMA((10,)), pltpu.SemaphoreType.DMA((3, tp - 1)), pltpu.SemaphoreType.DMA((3, tp)),
            pltpu.SemaphoreType.DMA((3,)), pltpu.SemaphoreType.DMA((3,)),
        ],
        compiler_params=pltpu.CompilerParams(collective_id=0, has_side_effects=True, vmem_limit_bytes=63*2**20),
        cost_estimate=pl.CostEstimate(flops=20_000_000_000, bytes_accessed=30_000_000, transcendentals=0),
        name='rest_of_layer',
    )(part, x, ln2_gain, ln2_bias, ln3_gain, ln3_bias, wq_c, enc, enc_near, wk_c, wv_c, wk_far, wv_far, wo_c, w_up, w_down)
    return out.astype(BF16), jnp.transpose(k_new, (1, 0, 2)), jnp.transpose(v_new, (1, 0, 2))


def solution(mesh):
    row_spec = P('dp', None)
    cache_spec = P('dp', None, 'tp', None)
    head_spec = P('dp', 'tp', None)
    vec_spec = P(None)
    col_split = P(None, 'tp')
    row_split = P('tp', None)
    in_specs = (row_spec, cache_spec, cache_spec, P('dp'), P('dp', 'tp', None), vec_spec, vec_spec, col_split, col_split, col_split, row_split, vec_spec, vec_spec, col_split, col_split, col_split, row_split, vec_spec, vec_spec, col_split, row_split)
    out_specs = (row_spec, head_spec, head_spec)
    return jax.shard_map(local_step, mesh=mesh, in_specs=in_specs, out_specs=out_specs, check_vma=False)
```

```python
import functools

import jax
import jax.numpy as jnp
from jax import lax
from jax.experimental import pallas as pl
from jax.experimental.pallas import tpu as pltpu
from jax.sharding import PartitionSpec as P

LN_EPS = 1e-5
NEG = -1e30
F32 = jnp.float32
BF16 = jnp.bfloat16
CHUNK = 512
UNROLL = 4
GRAIN = 64
GROUPS = 6


def layer_norm(values, ln_gain, ln_bias):
    row_mean = jnp.mean(values, axis=-1, keepdims=True)
    centred = values - row_mean
    row_var = jnp.mean(jnp.square(centred), axis=-1, keepdims=True)
    return (centred * lax.rsqrt(row_var + LN_EPS) * ln_gain + ln_bias).astype(BF16)


def dot(lhs, rhs):
    return jnp.dot(lhs, rhs, preferred_element_type=F32)


def dot_t(lhs, rhs):
    return lax.dot_general(lhs, rhs, (((1,), (1,)), ((), ())), preferred_element_type=F32)


def self_kernel(batch, heads, dim, lens, x_ref, g_ref, b_ref, kc, vc, wq_h, wk_h, wv_h, wo_h,
                part_ref, knew_ref, vnew_ref,
                wq, wk, wv, wo, kbuf, vbuf, q_s, o_s, m_s, l_s, acc_s, wsem, ksem, vsem):
    width = heads * dim
    scale = dim ** -0.5
    loads = [pltpu.make_async_copy(s, d, wsem.at[i]) for i, (s, d) in enumerate(((wq_h, wq), (wk_h, wk), (wv_h, wv), (wo_h, wo)))]
    for copy in loads[:3]:
        copy.start()

    def len_of(seq):
        return jnp.where(seq < batch, lens[jnp.minimum(seq, batch - 1)], 0)

    def following(seq, blk):
        more = (blk + 1) * CHUNK < len_of(seq)
        return jnp.where(more, seq, seq + 1), jnp.where(more, blk + 1, 0)

    def copies(seq, blk, slot, whole):
        live = CHUNK if whole else pl.multiple_of(jnp.minimum(len_of(seq) - blk * CHUNK, CHUNK), GRAIN)
        src = pl.ds(pl.multiple_of(blk * CHUNK, CHUNK), live)
        dst = pl.ds(0, live)
        return (pltpu.make_async_copy(kc.at[seq, :, src, :], kbuf.at[slot, :, dst, :], ksem.at[slot]),
                pltpu.make_async_copy(vc.at[seq, :, src, :], vbuf.at[slot, :, dst, :], vsem.at[slot]))

    def fetch_group(group, ptr, whole):
        for u in range(UNROLL):
            seq, blk = ptr

            @pl.when(seq < batch)
            def _():
                for copy in copies(seq, blk, group * UNROLL + u, whole):
                    copy.start()
            ptr = following(seq, blk)
        return ptr

    ptr = (jnp.int32(0), jnp.int32(0))
    for group in range(GROUPS):
        ptr = fetch_group(group, ptr, True)
    loads[3].start()

    n_items = jnp.int32(0)
    for seq in range(batch):
        n_items = n_items + lax.div(lens[seq] + (CHUNK - 1), CHUNK)
    n_steps = lax.div(n_items + (UNROLL - 1), UNROLL)

    a_norm = layer_norm(x_ref[...].astype(F32), g_ref[...].reshape(1, -1), b_ref[...].reshape(1, -1))
    loads[0].wait()
    q_new = dot(a_norm, wq[...]).astype(BF16).astype(F32)
    loads[1].wait()
    k_new = dot(a_norm, wk[...]).astype(BF16)
    loads[2].wait()
    v_new = dot(a_norm, wv[...]).astype(BF16)
    for h in range(heads):
        knew_ref[h] = k_new[:, h * dim:(h + 1) * dim]
        vnew_ref[h] = v_new[:, h * dim:(h + 1) * dim]
    q_s[0:batch, :] = q_new
    q_s[batch:, :] = jnp.zeros((q_s.shape[0] - batch, width), F32)
    pair = 2 * dim
    part_rows = CHUNK // 2
    row8 = lax.broadcasted_iota(jnp.int32, (8, 1), 0)
    pair_row = lax.broadcasted_iota(jnp.int32, (8, pair), 0)
    pair_side = lax.broadcasted_iota(jnp.int32, (8, pair), 1) // dim
    sel01 = (pair_row == pair_side).astype(F32)
    sel2 = (pair_row == pair_side + 2).astype(F32)
    qk = q_new * k_new.astype(F32)
    v_f = v_new.astype(F32)
    for seq in range(batch):
        prod = qk[seq:seq + 1, :]
        tail = jnp.concatenate([prod[:, pair:width], jnp.zeros((1, pair - dim), F32)], axis=1)
        s_new = jnp.sum(prod[:, 0:pair] * sel01 + tail * sel2, axis=1, keepdims=True) * scale
        m_s[seq] = jnp.broadcast_to(jnp.where(row8 == 3, NEG, s_new), (8, dim))
        tail_v = jnp.concatenate([v_f[seq:seq + 1, pair:width]] * 2, axis=1)
        acc_s[seq] = jnp.where(pair_row < 2, jnp.broadcast_to(v_f[seq:seq + 1, 0:pair], (8, pair)), jnp.where(pair_row == 2, jnp.broadcast_to(tail_v, (8, pair)), 0.0))
        l_s[seq] = jnp.broadcast_to(jnp.where(row8 == 3, 0.0, 1.0), (8, dim))
    m_s[batch] = jnp.zeros((8, dim), F32)
    l_s[batch] = jnp.ones((8, dim), F32)
    acc_s[batch] = jnp.zeros((8, pair), F32)
    lane = lax.broadcasted_iota(jnp.int32, (8, CHUNK), 1)
    lane2 = lax.broadcasted_iota(jnp.int32, (8, part_rows), 1)

    def step(i, carry):
        ptr, cur = carry[:2], carry[2:]
        group = lax.rem(i, GROUPS)
        items = []
        for u in range(UNROLL):
            items.append((*cur, group * UNROLL + u))
            cur = following(*cur)
        for seq, blk, slot in items:

            @pl.when((seq < batch) & (i < GROUPS))
            def _():
                for copy in copies(seq, blk, slot, True):
                    copy.wait()

            @pl.when((seq < batch) & (i >= GROUPS))
            def _():
                for copy in copies(seq, blk, slot, False):
                    copy.wait()
        scores = []
        for seq, blk, slot in items:
            q_row = q_s[pl.ds(jnp.minimum(seq, batch), 1), :]
            q01 = (q_row[:, 0:pair] * sel01).astype(BF16)
            q2 = (jnp.concatenate([q_row[:, pair:width]] * 2, axis=1) * sel2).astype(BF16)
            k01 = jnp.concatenate([kbuf[slot, 0], kbuf[slot, 1]], axis=1)
            k2 = jnp.concatenate([kbuf[slot, 2, 0:part_rows, :], kbuf[slot, 2, part_rows:CHUNK, :]], axis=1)
            scores.append((dot_t(q01, k01), dot_t(q2, k2)))
        weights = []
        for (seq, blk, slot), (s01, s2) in zip(items, scores):
            live = len_of(seq) - blk * CHUNK
            s01 = jnp.where(lane < jnp.where(row8 < 2, live, 0), s01 * scale, NEG)
            s2 = jnp.where(lane2 < jnp.where(row8 == 2, live, jnp.where(row8 == 3, live - part_rows, 0)), s2 * scale, NEG)
            m_i = jnp.maximum(jnp.max(s01, axis=1, keepdims=True), jnp.max(s2, axis=1, keepdims=True))
            p01 = jnp.where(row8 < 2, jnp.exp(s01 - m_i), 0.0)
            p2 = jnp.where(row8 < 2, 0.0, jnp.exp(s2 - m_i))
            l_i = jnp.sum(p01, axis=1, keepdims=True) + jnp.sum(p2, axis=1, keepdims=True)
            weights.append((m_i, l_i, p01.astype(BF16), p2.astype(BF16)))
        values = []
        for (seq, blk, slot), (m_i, l_i, p01, p2) in zip(items, weights):
            v01 = jnp.concatenate([vbuf[slot, 0], vbuf[slot, 1]], axis=1)
            v2 = jnp.concatenate([vbuf[slot, 2, 0:part_rows, :], vbuf[slot, 2, part_rows:CHUNK, :]], axis=1)
            values.append(dot(p01, v01) + dot(p2, v2))
        for (seq, blk, slot), (m_i, l_i, p01, p2), pv in zip(items, weights, values):
            row = jnp.minimum(seq, batch)
            m_old = m_s[row]
            m_new = jnp.maximum(m_old, m_i)
            keep = jnp.exp(m_old - m_new)
            add = jnp.exp(m_i - m_new)
            m_s[row] = m_new
            l_s[row] = l_s[row] * keep + l_i * add
            acc_s[row] = acc_s[row] * jnp.concatenate([keep] * 2, axis=1) + pv * jnp.concatenate([add] * 2, axis=1)
        ptr = fetch_group(group, ptr, False)
        return (*ptr, *cur)

    lax.fori_loop(0, n_steps, step, (*ptr, jnp.int32(0), jnp.int32(0)))
    for seq in range(batch):
        m, l, acc = m_s[seq], l_s[seq], acc_s[seq]
        top = jnp.maximum(m[2:3], m[3:4])
        w_a, w_b = jnp.exp(m[2:3] - top), jnp.exp(m[3:4] - top)
        o2 = (acc[2:3, 0:dim] * w_a + acc[3:4, dim:pair] * w_b) / (l[2:3] * w_a + l[3:4] * w_b)
        o_s[seq:seq + 1, :] = jnp.concatenate([acc[0:1, 0:dim] / l[0:1], acc[1:2, dim:pair] / l[1:2], o2], axis=1)
    loads[3].wait()
    part_ref[...] = dot(o_s[...].astype(BF16), wo[...]).astype(BF16)


def rest_kernel(batch, heads, dim, tp, part_ref, x_ref, g2, b2, g3, b3, wqc_h, e_own_h, wk_h, wv_h, wkr_h, wvr_h, woc_h, wup_h, wdn_h,
                out_ref,
                wqc, enc, wkv, wkvr, woc, wup, wdn, kv_own, kv_rem, recv, send2, send3, qc_s, qc_r, o_snd, o_rcv, st_snd, st_rcv,
                lsem, ssem, rsem, xs, xr, ns, nr):
    width = heads * dim
    scale = dim ** -0.5
    me = lax.axis_index('tp')
    far = lax.rem(me + 2, tp)
    near = me + 1 - 2 * lax.rem(me, 2)
    half = enc.shape[0] // 2
    early = wvr_h.shape[1]

    def load(i, src, dst):
        copy = pltpu.make_async_copy(src, dst, lsem.at[i])
        copy.start()
        return copy

    ld_e0 = load(0, e_own_h, enc.at[pl.ds(0, half), :])
    ld_wk = load(1, wk_h, wkv.at[:, pl.ds(0, width)])
    ld_wv = load(2, wv_h, wkv.at[:, pl.ds(width, width)])
    ld_wkr = load(3, wkr_h, wkvr.at[:, pl.ds(0, width)])
    ld_wvr = load(4, wvr_h, wkvr.at[:, pl.ds(width, early)])
    ld_wqc = load(5, wqc_h, wqc)
    ld_woc = load(6, woc_h, woc)
    ld_up = load(7, wup_h, wup)
    ld_dn = load(8, wdn_h, wdn)

    barrier = pltpu.get_barrier_semaphore()
    for d in range(1, tp):
        pl.semaphore_signal(barrier, inc=1, device_id={'tp': lax.rem(me + d, tp)}, device_id_type=pl.DeviceIdType.MESH)
    pl.semaphore_wait(barrier, tp - 1)

    def exchange(n, src):
        for d in range(1, tp):
            pltpu.make_async_remote_copy(src_ref=src, dst_ref=recv.at[n, me], send_sem=ssem.at[n, d - 1], recv_sem=rsem.at[n, me],
                                         device_id={'tp': lax.rem(me + d, tp)}, device_id_type=pl.DeviceIdType.MESH).start()
        recv[n, me] = src[...]

    def collect(n, src):
        for d in range(1, tp):
            other = lax.rem(me + d, tp)
            pltpu.make_async_remote_copy(src_ref=src, dst_ref=recv.at[n, other], send_sem=ssem.at[n, d - 1], recv_sem=rsem.at[n, other],
                                         device_id={'tp': other}, device_id_type=pl.DeviceIdType.MESH).wait()
        total = recv[n, 0].astype(F32)
        for t in range(1, tp):
            total = total + recv[n, t].astype(F32)
        return total

    def to_far(i, src, dst):
        return pltpu.make_async_remote_copy(src_ref=src, dst_ref=dst, send_sem=xs.at[i], recv_sem=xr.at[i],
                                            device_id={'tp': far}, device_id_type=pl.DeviceIdType.MESH)

    def project(first, count, jobs, tile=256):
        def body(i, c):
            rows = pl.ds(pl.multiple_of(i * tile, tile), tile)
            for weights, out, lo, hi in jobs:
                out[rows, lo:hi] = dot(enc[rows, :], weights[:, lo:hi]).astype(BF16)
            return c
        lax.fori_loop(first // tile, (first + count) // tile, body, 0)

    late_rows = (0, 640, wv_h.shape[0])

    def late(i):
        rows, cols = pl.ds(late_rows[i], late_rows[i + 1] - late_rows[i]), width - early
        return to_far(3 + i, wv_h.at[rows, pl.ds(early, cols)], wkvr.at[rows, pl.ds(width + early, cols)])

    exchange(0, part_ref)
    near_e = pltpu.make_async_remote_copy(src_ref=e_own_h, dst_ref=enc.at[pl.ds(half, half), :], send_sem=ns.at[0], recv_sem=nr.at[0],
                                          device_id={'tp': near}, device_id_type=pl.DeviceIdType.MESH)
    near_e.start()
    late(0).start()
    jobs = ((wkv, kv_own, 0, 2 * width), (wkvr, kv_rem, 0, width + early))
    for copy in (ld_e0, ld_wk, ld_wv, ld_wkr, ld_wvr):
        copy.wait()
    project(0, half, jobs)

    h1 = x_ref[...].astype(F32) + collect(0, part_ref)
    c_norm = layer_norm(h1, g2[...].reshape(1, -1), b2[...].reshape(1, -1))
    ld_wqc.wait()
    qc_s[...] = dot(c_norm, wqc[...]).astype(BF16)
    send_q = to_far(0, qc_s, qc_r)
    send_q.start()
    late(1).start()
    near_e.wait()
    project(half, half, jobs)
    for i in range(2):
        late(i).wait()
    project(0, 2 * half, ((wkvr, kv_rem, width + early, 2 * width),))

    rows = heads * batch
    row_b = lax.rem(lax.broadcasted_iota(jnp.int32, (rows, 128), 0), batch)
    lane = lax.broadcasted_iota(jnp.int32, (rows, 128), 1)
    per = half // batch
    pack = 128 // per
    blocks = half // 128
    mine = lax.rem(row_b, pack) == lane // per
    row_blk = row_b // pack
    lane_head = lax.broadcasted_iota(jnp.int32, (batch, width), 1) // dim

    def attend(q, kv):
        qf = q.astype(F32)
        q_rows = jnp.concatenate([jnp.where(lane_head == h, qf, 0.0) for h in range(heads)], axis=0).astype(BF16)
        parts = []
        for part in range(2):
            s_all = dot_t(q_rows, kv[part * half:(part + 1) * half, 0:width])
            s = s_all[:, 0:128]
            for k in range(1, blocks):
                s = jnp.where(row_blk == k, s_all[:, k * 128:(k + 1) * 128], s)
            parts.append(jnp.where(mine, s * scale, NEG))
        m = jnp.maximum(jnp.max(parts[0], axis=1, keepdims=True), jnp.max(parts[1], axis=1, keepdims=True))
        p = [jnp.exp(s - m) for s in parts]
        l = jnp.sum(p[0], axis=1, keepdims=True) + jnp.sum(p[1], axis=1, keepdims=True)
        o = None
        for part in range(2):
            p_wide = jnp.concatenate([jnp.where(row_blk == k, p[part], 0.0) for k in range(blocks)], axis=1).astype(BF16)
            o_part = dot(p_wide, kv[part * half:(part + 1) * half, width:2 * width])
            o = o_part if o is None else o + o_part
        o = jnp.concatenate([o[h * batch:(h + 1) * batch, h * dim:(h + 1) * dim] for h in range(heads)], axis=0)
        return m, l, o

    send_q.wait()
    m_r, l_r, o_r = attend(qc_r[...], kv_rem)
    o_snd[...] = o_r
    st_snd[...] = jnp.where(lane < 64, m_r, l_r)
    send_o = to_far(1, o_snd, o_rcv)
    send_st = to_far(2, st_snd, st_rcv)
    send_o.start()
    send_st.start()
    m_a, l_a, o_a = attend(qc_s[...], kv_own)
    send_o.wait()
    send_st.wait()
    stats = st_rcv[...]
    m_b, l_b = stats[:, 0:1], stats[:, 64:65]
    m = jnp.maximum(m_a, m_b)
    w_a, w_b = jnp.exp(m_a - m), jnp.exp(m_b - m)
    o = (o_a * w_a + o_rcv[...] * w_b) / (l_a * w_a + l_b * w_b)
    oc = jnp.concatenate([o[h * batch:(h + 1) * batch, :] for h in range(heads)], axis=1).astype(BF16)
    ld_woc.wait()
    send2[...] = dot(oc, woc[...]).astype(BF16)
    exchange(1, send2)
    h2 = h1 + collect(1, send2)
    m_norm = layer_norm(h2, g3[...].reshape(1, -1), b3[...].reshape(1, -1))
    ld_up.wait()
    up = dot(m_norm, wup[...])
    hidden = (0.5 * up * (1.0 + lax.erf(up * (0.5 ** 0.5)))).astype(BF16)
    ld_dn.wait()
    send3[...] = dot(hidden, wdn[...]).astype(BF16)
    exchange(2, send3)
    out_ref[...] = h2 + collect(2, send3)


def local_step(x, k_cache, v_cache, seq_lens, nbr_enc, ln1_gain, ln1_bias, w_q, w_k, w_v, w_o, ln2_gain, ln2_bias, wq_c, wk_c, wv_c, wo_c, ln3_gain, ln3_bias, w_up, w_down):
    batch, d_model = x.shape
    heads, dim = k_cache.shape[2:]
    width = heads * dim
    tp = lax.axis_size('tp')
    far = [(i, (i + 2) % tp) for i in range(tp)]
    enc = nbr_enc.reshape(-1, nbr_enc.shape[-1])
    wk_far = lax.ppermute(wk_c, 'tp', far)
    wv_far = lax.ppermute(wv_c[:, :2 * dim], 'tp', far)

    any_spec = pl.BlockSpec(memory_space=pl.ANY)
    hbm = pl.BlockSpec(memory_space=pltpu.HBM)
    vmem = pl.BlockSpec(memory_space=pltpu.VMEM)
    smem = pl.BlockSpec(memory_space=pltpu.SMEM)
    slots = GROUPS * UNROLL
    part, k_new, v_new = pl.pallas_call(
        functools.partial(self_kernel, batch, heads, dim),
        out_shape=(jax.ShapeDtypeStruct((batch, d_model), BF16), jax.ShapeDtypeStruct((heads, batch, dim), BF16), jax.ShapeDtypeStruct((heads, batch, dim), BF16)),
        in_specs=[smem, vmem, vmem, vmem] + [hbm] * 6,
        out_specs=(vmem, vmem, vmem),
        scratch_shapes=[
            pltpu.VMEM((d_model, width), BF16), pltpu.VMEM((d_model, width), BF16), pltpu.VMEM((d_model, width), BF16), pltpu.VMEM((width, d_model), BF16),
            pltpu.VMEM((slots, heads, CHUNK, dim), BF16), pltpu.VMEM((slots, heads, CHUNK, dim), BF16),
            pltpu.VMEM((batch + 8, width), F32), pltpu.VMEM((batch, width), F32),
            pltpu.VMEM((batch + 1, 8, dim), F32), pltpu.VMEM((batch + 1, 8, dim), F32), pltpu.VMEM((batch + 1, 8, 2 * dim), F32),
            pltpu.SemaphoreType.DMA((4,)), pltpu.SemaphoreType.DMA((slots,)), pltpu.SemaphoreType.DMA((slots,)),
        ],
        compiler_params=pltpu.CompilerParams(vmem_limit_bytes=67043328),
        cost_estimate=pl.CostEstimate(flops=40_000_000_000, bytes_accessed=60_000_000, transcendentals=0),
        name='self_attention',
    )(seq_lens, x, ln1_gain, ln1_bias, jnp.transpose(k_cache, (0, 2, 1, 3)), jnp.transpose(v_cache, (0, 2, 1, 3)), w_q, w_k, w_v, w_o)

    n_enc, enc_dim = enc.shape
    ff = w_up.shape[1]
    out = pl.pallas_call(
        functools.partial(rest_kernel, batch, heads, dim, tp),
        out_shape=jax.ShapeDtypeStruct((batch, d_model), F32),
        in_specs=[vmem] * 6 + [hbm] * 9,
        out_specs=vmem,
        scratch_shapes=[
            pltpu.VMEM((d_model, width), BF16), pltpu.VMEM((2 * n_enc, enc_dim), BF16),
            pltpu.VMEM((enc_dim, 2 * width), BF16), pltpu.VMEM((enc_dim, 2 * width), BF16),
            pltpu.VMEM((width, d_model), BF16), pltpu.VMEM((d_model, ff), BF16), pltpu.VMEM((ff, d_model), BF16),
            pltpu.VMEM((2 * n_enc, 2 * width), BF16), pltpu.VMEM((2 * n_enc, 2 * width), BF16),
            pltpu.VMEM((3, tp, batch, d_model), BF16), pltpu.VMEM((batch, d_model), BF16), pltpu.VMEM((batch, d_model), BF16),
            pltpu.VMEM((batch, width), BF16), pltpu.VMEM((batch, width), BF16),
            pltpu.VMEM((heads * batch, dim), F32), pltpu.VMEM((heads * batch, dim), F32), pltpu.VMEM((heads * batch, 128), F32), pltpu.VMEM((heads * batch, 128), F32),
            pltpu.SemaphoreType.DMA((9,)), pltpu.SemaphoreType.DMA((3, tp - 1)), pltpu.SemaphoreType.DMA((3, tp)),
            pltpu.SemaphoreType.DMA((5,)), pltpu.SemaphoreType.DMA((5,)), pltpu.SemaphoreType.DMA((1,)), pltpu.SemaphoreType.DMA((1,)),
        ],
        compiler_params=pltpu.CompilerParams(collective_id=0, has_side_effects=True, vmem_limit_bytes=67043328),
        cost_estimate=pl.CostEstimate(flops=20_000_000_000, bytes_accessed=30_000_000, transcendentals=0),
        name='rest_of_layer',
    )(part, x, ln2_gain, ln2_bias, ln3_gain, ln3_bias, wq_c, enc, wk_c, wv_c, wk_far, wv_far, wo_c, w_up, w_down)
    return out.astype(BF16), jnp.transpose(k_new, (1, 0, 2)), jnp.transpose(v_new, (1, 0, 2))


def solution(mesh):
    row_spec = P('dp', None)
    cache_spec = P('dp', None, 'tp', None)
    head_spec = P('dp', 'tp', None)
    vec_spec = P(None)
    col_split = P(None, 'tp')
    row_split = P('tp', None)
    in_specs = (row_spec, cache_spec, cache_spec, P('dp'), P('dp', 'tp', None), vec_spec, vec_spec, col_split, col_split, col_split, row_split, vec_spec, vec_spec, col_split, col_split, col_split, row_split, vec_spec, vec_spec, col_split, row_split)
    out_specs = (row_spec, head_spec, head_spec)
    return jax.shard_map(local_step, mesh=mesh, in_specs=in_specs, out_specs=out_specs, check_vma=False)
```

```python
import functools

import jax
import jax.numpy as jnp
from jax import lax
from jax.experimental import pallas as pl
from jax.experimental.pallas import tpu as pltpu
from jax.sharding import PartitionSpec as P

LN_EPS = 1e-5
NEG = -1e30
F32 = jnp.float32
BF16 = jnp.bfloat16
CHUNK = 512
UNROLL = 8
GRAIN = 64
GROUPS = 3


def layer_norm(values, ln_gain, ln_bias):
    row_mean = jnp.mean(values, axis=-1, keepdims=True)
    centred = values - row_mean
    row_var = jnp.mean(jnp.square(centred), axis=-1, keepdims=True)
    return (centred * lax.rsqrt(row_var + LN_EPS) * ln_gain + ln_bias).astype(BF16)


def dot(lhs, rhs):
    return jnp.dot(lhs, rhs, preferred_element_type=F32)


def dot_t(lhs, rhs):
    return lax.dot_general(lhs, rhs, (((1,), (1,)), ((), ())), preferred_element_type=F32)


def in_hbm(*arrays):
    return [pltpu.with_memory_space_constraint(a, pltpu.HBM) for a in arrays]


def self_kernel(batch, heads, dim, lens, x_ref, g_ref, b_ref, kc, vc, wq_h, wk_h, wv_h, wo_h,
                part_ref, knew_ref, vnew_ref,
                wq, wk, wv, wo, kbuf, vbuf, q_s, o_s, m_s, l_s, acc_s, wsem, ksem, vsem):
    width = heads * dim
    scale = dim ** -0.5
    loads = [pltpu.make_async_copy(s, d, wsem.at[i]) for i, (s, d) in enumerate(((wq_h, wq), (wk_h, wk), (wv_h, wv), (wo_h, wo)))]
    for copy in loads[:3]:
        copy.start()

    def len_of(seq):
        return jnp.where(seq < batch, lens[jnp.minimum(seq, batch - 1)], 0)

    def following(seq, blk):
        more = (blk + 1) * CHUNK < len_of(seq)
        return jnp.where(more, seq, seq + 1), jnp.where(more, blk + 1, 0)

    def copies(seq, blk, slot, whole):
        live = CHUNK if whole else pl.multiple_of(jnp.minimum(len_of(seq) - blk * CHUNK, CHUNK), GRAIN)
        src = pl.ds(pl.multiple_of(blk * CHUNK, CHUNK), live)
        dst = pl.ds(0, live)
        return (pltpu.make_async_copy(kc.at[seq, :, src, :], kbuf.at[slot, :, dst, :], ksem.at[slot]),
                pltpu.make_async_copy(vc.at[seq, :, src, :], vbuf.at[slot, :, dst, :], vsem.at[slot]))

    def fetch_group(group, ptr, whole):
        for u in range(UNROLL):
            seq, blk = ptr

            @pl.when(seq < batch)
            def _():
                for copy in copies(seq, blk, group * UNROLL + u, whole):
                    copy.start()
            ptr = following(seq, blk)
        return ptr

    ptr = (jnp.int32(0), jnp.int32(0))
    for group in range(GROUPS):
        ptr = fetch_group(group, ptr, True)
    loads[3].start()

    n_items = jnp.int32(0)
    for seq in range(batch):
        n_items = n_items + lax.div(lens[seq] + (CHUNK - 1), CHUNK)
    n_steps = lax.div(n_items + (UNROLL - 1), UNROLL)

    a_norm = layer_norm(x_ref[...].astype(F32), g_ref[...].reshape(1, -1), b_ref[...].reshape(1, -1))
    loads[0].wait()
    q_new = dot(a_norm, wq[...]).astype(BF16).astype(F32)
    loads[1].wait()
    k_new = dot(a_norm, wk[...]).astype(BF16)
    loads[2].wait()
    v_new = dot(a_norm, wv[...]).astype(BF16)
    for h in range(heads):
        knew_ref[h] = k_new[:, h * dim:(h + 1) * dim]
        vnew_ref[h] = v_new[:, h * dim:(h + 1) * dim]
    q_s[0:batch, :] = q_new
    q_s[batch:, :] = jnp.zeros((q_s.shape[0] - batch, width), F32)
    pair = 2 * dim
    part_rows = CHUNK // 2
    row8 = lax.broadcasted_iota(jnp.int32, (8, 1), 0)
    pair_row = lax.broadcasted_iota(jnp.int32, (8, pair), 0)
    pair_side = lax.broadcasted_iota(jnp.int32, (8, pair), 1) // dim
    sel01 = (pair_row == pair_side).astype(F32)
    sel2 = (pair_row == pair_side + 2).astype(F32)
    qk = q_new * k_new.astype(F32)
    v_f = v_new.astype(F32)
    for seq in range(batch):
        prod = qk[seq:seq + 1, :]
        tail = jnp.concatenate([prod[:, pair:width], jnp.zeros((1, pair - dim), F32)], axis=1)
        s_new = jnp.sum(prod[:, 0:pair] * sel01 + tail * sel2, axis=1, keepdims=True) * scale
        m_s[seq] = jnp.broadcast_to(jnp.where(row8 == 3, NEG, s_new), (8, dim))
        tail_v = jnp.concatenate([v_f[seq:seq + 1, pair:width]] * 2, axis=1)
        acc_s[seq] = jnp.where(pair_row < 2, jnp.broadcast_to(v_f[seq:seq + 1, 0:pair], (8, pair)), jnp.where(pair_row == 2, jnp.broadcast_to(tail_v, (8, pair)), 0.0))
        l_s[seq] = jnp.broadcast_to(jnp.where(row8 == 3, 0.0, 1.0), (8, dim))
    m_s[batch] = jnp.zeros((8, dim), F32)
    l_s[batch] = jnp.ones((8, dim), F32)
    acc_s[batch] = jnp.zeros((8, pair), F32)
    lane = lax.broadcasted_iota(jnp.int32, (8, CHUNK), 1)
    lane2 = lax.broadcasted_iota(jnp.int32, (8, part_rows), 1)

    def step(i, carry):
        ptr, cur = carry[:2], carry[2:]
        group = lax.rem(i, GROUPS)
        items = []
        for u in range(UNROLL):
            items.append((*cur, group * UNROLL + u))
            cur = following(*cur)
        for seq, blk, slot in items:

            @pl.when((seq < batch) & (i < GROUPS))
            def _():
                for copy in copies(seq, blk, slot, True):
                    copy.wait()

            @pl.when((seq < batch) & (i >= GROUPS))
            def _():
                for copy in copies(seq, blk, slot, False):
                    copy.wait()
        scores = []
        for seq, blk, slot in items:
            q_row = q_s[pl.ds(jnp.minimum(seq, batch), 1), :]
            q01 = (q_row[:, 0:pair] * sel01).astype(BF16)
            q2 = (jnp.concatenate([q_row[:, pair:width]] * 2, axis=1) * sel2).astype(BF16)
            k01 = jnp.concatenate([kbuf[slot, 0], kbuf[slot, 1]], axis=1)
            k2 = jnp.concatenate([kbuf[slot, 2, 0:part_rows, :], kbuf[slot, 2, part_rows:CHUNK, :]], axis=1)
            scores.append((dot_t(q01, k01), dot_t(q2, k2)))
        weights = []
        for (seq, blk, slot), (s01, s2) in zip(items, scores):
            live = len_of(seq) - blk * CHUNK
            s01 = jnp.where(lane < jnp.where(row8 < 2, live, 0), s01 * scale, NEG)
            s2 = jnp.where(lane2 < jnp.where(row8 == 2, live, jnp.where(row8 == 3, live - part_rows, 0)), s2 * scale, NEG)
            m_i = jnp.maximum(jnp.max(s01, axis=1, keepdims=True), jnp.max(s2, axis=1, keepdims=True))
            p01 = jnp.where(row8 < 2, jnp.exp(s01 - m_i), 0.0)
            p2 = jnp.where(row8 < 2, 0.0, jnp.exp(s2 - m_i))
            l_i = jnp.sum(p01, axis=1, keepdims=True) + jnp.sum(p2, axis=1, keepdims=True)
            weights.append((m_i, l_i, p01.astype(BF16), p2.astype(BF16)))
        values = []
        for (seq, blk, slot), (m_i, l_i, p01, p2) in zip(items, weights):
            v01 = jnp.concatenate([vbuf[slot, 0], vbuf[slot, 1]], axis=1)
            v2 = jnp.concatenate([vbuf[slot, 2, 0:part_rows, :], vbuf[slot, 2, part_rows:CHUNK, :]], axis=1)
            values.append(dot(p01, v01) + dot(p2, v2))
        for (seq, blk, slot), (m_i, l_i, p01, p2), pv in zip(items, weights, values):
            row = jnp.minimum(seq, batch)
            m_old = m_s[row]
            m_new = jnp.maximum(m_old, m_i)
            keep = jnp.exp(m_old - m_new)
            add = jnp.exp(m_i - m_new)
            m_s[row] = m_new
            l_s[row] = l_s[row] * keep + l_i * add
            acc_s[row] = acc_s[row] * jnp.concatenate([keep] * 2, axis=1) + pv * jnp.concatenate([add] * 2, axis=1)
        ptr = fetch_group(group, ptr, False)
        return (*ptr, *cur)

    lax.fori_loop(0, n_steps, step, (*ptr, jnp.int32(0), jnp.int32(0)))
    for seq in range(batch):
        m, l, acc = m_s[seq], l_s[seq], acc_s[seq]
        top = jnp.maximum(m[2:3], m[3:4])
        w_a, w_b = jnp.exp(m[2:3] - top), jnp.exp(m[3:4] - top)
        o2 = (acc[2:3, 0:dim] * w_a + acc[3:4, dim:pair] * w_b) / (l[2:3] * w_a + l[3:4] * w_b)
        o_s[seq:seq + 1, :] = jnp.concatenate([acc[0:1, 0:dim] / l[0:1], acc[1:2, dim:pair] / l[1:2], o2], axis=1)
    loads[3].wait()
    part_ref[...] = dot(o_s[...].astype(BF16), wo[...]).astype(BF16)


def rest_kernel(batch, heads, dim, tp, part_ref, x_ref, g2, b2, g3, b3, wqc_h, e_own_h, wk_h, wv_h, wkr_h, wvr_h, woc_h, wup_h, wdn_h,
                out_ref,
                wqc, enc, wkv, wkvr, woc, wup, wdn, kv_own, kv_rem, recv, send2, send3, qc_s, qc_r, o_snd, o_rcv,
                lsem, ssem, rsem, xs, xr, ns, nr):
    width = heads * dim
    scale = dim ** -0.5
    me = lax.axis_index('tp')
    far = lax.rem(me + 2, tp)
    near = me + 1 - 2 * lax.rem(me, 2)
    half = enc.shape[0] // 2
    early = wvr_h.shape[1]

    def load(i, src, dst):
        copy = pltpu.make_async_copy(src, dst, lsem.at[i])
        copy.start()
        return copy

    ld_e0 = load(0, e_own_h, enc.at[pl.ds(0, half), :])
    ld_wk = load(1, wk_h, wkv.at[:, pl.ds(0, width)])
    ld_wv = load(2, wv_h, wkv.at[:, pl.ds(width, width)])
    ld_wkr = load(3, wkr_h, wkvr.at[:, pl.ds(0, width)])
    ld_wvr = load(4, wvr_h, wkvr.at[:, pl.ds(width, early)])
    ld_wqc = load(5, wqc_h, wqc)
    ld_woc = load(6, woc_h, woc)
    ld_up = load(7, wup_h, wup)
    ld_dn = load(8, wdn_h, wdn)

    barrier = pltpu.get_barrier_semaphore()
    for d in range(1, tp):
        pl.semaphore_signal(barrier, inc=1, device_id={'tp': lax.rem(me + d, tp)}, device_id_type=pl.DeviceIdType.MESH)
    pl.semaphore_wait(barrier, tp - 1)

    def exchange(n, src):
        for d in range(1, tp):
            pltpu.make_async_remote_copy(src_ref=src, dst_ref=recv.at[n, me], send_sem=ssem.at[n, d - 1], recv_sem=rsem.at[n, me],
                                         device_id={'tp': lax.rem(me + d, tp)}, device_id_type=pl.DeviceIdType.MESH).start()
        recv[n, me] = src[...]

    def collect(n, src):
        for d in range(1, tp):
            other = lax.rem(me + d, tp)
            pltpu.make_async_remote_copy(src_ref=src, dst_ref=recv.at[n, other], send_sem=ssem.at[n, d - 1], recv_sem=rsem.at[n, other],
                                         device_id={'tp': other}, device_id_type=pl.DeviceIdType.MESH).wait()
        total = recv[n, 0].astype(F32)
        for t in range(1, tp):
            total = total + recv[n, t].astype(F32)
        return total

    def to_far(i, src, dst):
        return pltpu.make_async_remote_copy(src_ref=src, dst_ref=dst, send_sem=xs.at[i], recv_sem=xr.at[i],
                                            device_id={'tp': far}, device_id_type=pl.DeviceIdType.MESH)

    def project(first, count, jobs, tile=256):
        def body(i, c):
            rows = pl.ds(pl.multiple_of(i * tile, tile), tile)
            for weights, out, lo, hi in jobs:
                out[rows, lo:hi] = dot(enc[rows, :], weights[:, lo:hi]).astype(BF16)
            return c
        lax.fori_loop(first // tile, (first + count) // tile, body, 0)

    late_rows = (0, 640, wv_h.shape[0])

    def late(i):
        rows, cols = pl.ds(late_rows[i], late_rows[i + 1] - late_rows[i]), width - early
        return to_far(2 + i, wv_h.at[rows, pl.ds(early, cols)], wkvr.at[rows, pl.ds(width + early, cols)])

    exchange(0, part_ref)
    near_e = pltpu.make_async_remote_copy(src_ref=e_own_h, dst_ref=enc.at[pl.ds(half, half), :], send_sem=ns.at[0], recv_sem=nr.at[0],
                                          device_id={'tp': near}, device_id_type=pl.DeviceIdType.MESH)
    near_e.start()
    late(0).start()
    jobs = ((wkv, kv_own, 0, 2 * width), (wkvr, kv_rem, 0, width + early))
    for copy in (ld_e0, ld_wk, ld_wv, ld_wkr, ld_wvr):
        copy.wait()
    project(0, half, jobs)

    h1 = x_ref[...].astype(F32) + collect(0, part_ref)
    c_norm = layer_norm(h1, g2[...].reshape(1, -1), b2[...].reshape(1, -1))
    ld_wqc.wait()
    qc_s[...] = dot(c_norm, wqc[...]).astype(BF16)
    send_q = to_far(0, qc_s, qc_r)
    send_q.start()
    late(1).start()
    near_e.wait()
    project(half, half, jobs[1:])
    for i in range(2):
        late(i).wait()
    project(0, 2 * half, ((wkvr, kv_rem, width + early, 2 * width),))

    rows = heads * batch
    row_b = lax.rem(lax.broadcasted_iota(jnp.int32, (rows, 128), 0), batch)
    lane = lax.broadcasted_iota(jnp.int32, (rows, 128), 1)
    per = half // batch
    pack = 128 // per
    blocks = half // 128
    mine = lax.rem(row_b, pack) == lane // per
    row_blk = row_b // pack
    lane_head = lax.broadcasted_iota(jnp.int32, (batch, width), 1) // dim

    def attend(q, kv):
        qf = q.astype(F32)
        q_rows = jnp.concatenate([jnp.where(lane_head == h, qf, 0.0) for h in range(heads)], axis=0).astype(BF16)
        parts = []
        for part in range(2):
            s_all = dot_t(q_rows, kv[part * half:(part + 1) * half, 0:width])
            s = s_all[:, 0:128]
            for k in range(1, blocks):
                s = jnp.where(row_blk == k, s_all[:, k * 128:(k + 1) * 128], s)
            parts.append(jnp.where(mine, s * scale, NEG))
        m = jnp.maximum(jnp.max(parts[0], axis=1, keepdims=True), jnp.max(parts[1], axis=1, keepdims=True))
        p = [jnp.exp(s - m) for s in parts]
        l = jnp.sum(p[0], axis=1, keepdims=True) + jnp.sum(p[1], axis=1, keepdims=True)
        o = None
        for part in range(2):
            p_wide = jnp.concatenate([jnp.where(row_blk == k, p[part], 0.0) for k in range(blocks)], axis=1).astype(BF16)
            o_part = dot(p_wide, kv[part * half:(part + 1) * half, width:2 * width])
            o = o_part if o is None else o + o_part
        o = jnp.concatenate([o[h * batch:(h + 1) * batch, h * dim:(h + 1) * dim] for h in range(heads)], axis=0)
        return m, l, o

    send_q.wait()
    m_r, l_r, o_r = attend(qc_r[...], kv_rem)
    o_snd[0:rows, :] = o_r
    stats = jnp.zeros((batch, dim), F32)
    st_lane = lax.broadcasted_iota(jnp.int32, (batch, dim), 1)
    for h in range(heads):
        stats = jnp.where(st_lane == 2 * h, m_r[h * batch:(h + 1) * batch], jnp.where(st_lane == 2 * h + 1, l_r[h * batch:(h + 1) * batch], stats))
    o_snd[rows:rows + batch, :] = stats
    send_o = to_far(1, o_snd, o_rcv)
    send_o.start()
    project(half, half, jobs[:1])
    m_a, l_a, o_a = attend(qc_s[...], kv_own)
    send_o.wait()
    stats = o_rcv[rows:rows + batch, :]
    m_b = jnp.concatenate([stats[:, 2 * h:2 * h + 1] for h in range(heads)], axis=0)
    l_b = jnp.concatenate([stats[:, 2 * h + 1:2 * h + 2] for h in range(heads)], axis=0)
    m = jnp.maximum(m_a, m_b)
    w_a, w_b = jnp.exp(m_a - m), jnp.exp(m_b - m)
    o = (o_a * w_a + o_rcv[0:rows, :] * w_b) / (l_a * w_a + l_b * w_b)
    oc = jnp.concatenate([o[h * batch:(h + 1) * batch, :] for h in range(heads)], axis=1).astype(BF16)
    ld_woc.wait()
    send2[...] = dot(oc, woc[...]).astype(BF16)
    exchange(1, send2)
    h2 = h1 + collect(1, send2)
    m_norm = layer_norm(h2, g3[...].reshape(1, -1), b3[...].reshape(1, -1))
    ld_up.wait()
    up = dot(m_norm, wup[...])
    hidden = (0.5 * up * (1.0 + lax.erf(up * (0.5 ** 0.5)))).astype(BF16)
    ld_dn.wait()
    send3[...] = dot(hidden, wdn[...]).astype(BF16)
    exchange(2, send3)
    out_ref[...] = h2 + collect(2, send3)


def local_step(x, k_cache, v_cache, seq_lens, nbr_enc, ln1_gain, ln1_bias, w_q, w_k, w_v, w_o, ln2_gain, ln2_bias, wq_c, wk_c, wv_c, wo_c, ln3_gain, ln3_bias, w_up, w_down):
    batch, d_model = x.shape
    heads, dim = k_cache.shape[2:]
    width = heads * dim
    tp = lax.axis_size('tp')
    far = [(i, (i + 2) % tp) for i in range(tp)]
    enc = nbr_enc.reshape(-1, nbr_enc.shape[-1])
    wk_far = lax.ppermute(wk_c, 'tp', far)
    wv_far = lax.ppermute(wv_c[:, :2 * dim], 'tp', far)

    any_spec = pl.BlockSpec(memory_space=pl.ANY)
    hbm = pl.BlockSpec(memory_space=pltpu.HBM)
    vmem = pl.BlockSpec(memory_space=pltpu.VMEM)
    smem = pl.BlockSpec(memory_space=pltpu.SMEM)
    slots = GROUPS * UNROLL
    part, k_new, v_new = pl.pallas_call(
        functools.partial(self_kernel, batch, heads, dim),
        out_shape=(jax.ShapeDtypeStruct((batch, d_model), BF16), jax.ShapeDtypeStruct((heads, batch, dim), BF16), jax.ShapeDtypeStruct((heads, batch, dim), BF16)),
        in_specs=[smem, vmem, vmem, vmem] + [hbm] * 6,
        out_specs=(vmem, vmem, vmem),
        scratch_shapes=[
            pltpu.VMEM((d_model, width), BF16), pltpu.VMEM((d_model, width), BF16), pltpu.VMEM((d_model, width), BF16), pltpu.VMEM((width, d_model), BF16),
            pltpu.VMEM((slots, heads, CHUNK, dim), BF16), pltpu.VMEM((slots, heads, CHUNK, dim), BF16),
            pltpu.VMEM((batch + 8, width), F32), pltpu.VMEM((batch, width), F32),
            pltpu.VMEM((batch + 1, 8, dim), F32), pltpu.VMEM((batch + 1, 8, dim), F32), pltpu.VMEM((batch + 1, 8, 2 * dim), F32),
            pltpu.SemaphoreType.DMA((4,)), pltpu.SemaphoreType.DMA((slots,)), pltpu.SemaphoreType.DMA((slots,)),
        ],
        compiler_params=pltpu.CompilerParams(vmem_limit_bytes=46000000),
        cost_estimate=pl.CostEstimate(flops=40_000_000_000, bytes_accessed=60_000_000, transcendentals=0),
        name='self_attention',
    )(*in_hbm(seq_lens, x, ln1_gain, ln1_bias, jnp.transpose(k_cache, (0, 2, 1, 3)), jnp.transpose(v_cache, (0, 2, 1, 3)), w_q, w_k, w_v, w_o))

    n_enc, enc_dim = enc.shape
    ff = w_up.shape[1]
    out = pl.pallas_call(
        functools.partial(rest_kernel, batch, heads, dim, tp),
        out_shape=jax.ShapeDtypeStruct((batch, d_model), F32),
        in_specs=[vmem] * 6 + [hbm] * 4 + [any_spec] * 2 + [hbm] * 3,
        out_specs=vmem,
        scratch_shapes=[
            pltpu.VMEM((d_model, width), BF16), pltpu.VMEM((2 * n_enc, enc_dim), BF16),
            pltpu.VMEM((enc_dim, 2 * width), BF16), pltpu.VMEM((enc_dim, 2 * width), BF16),
            pltpu.VMEM((width, d_model), BF16), pltpu.VMEM((d_model, ff), BF16), pltpu.VMEM((ff, d_model), BF16),
            pltpu.VMEM((2 * n_enc, 2 * width), BF16), pltpu.VMEM((2 * n_enc, 2 * width), BF16),
            pltpu.VMEM((3, tp, batch, d_model), BF16), pltpu.VMEM((batch, d_model), BF16), pltpu.VMEM((batch, d_model), BF16),
            pltpu.VMEM((batch, width), BF16), pltpu.VMEM((batch, width), BF16),
            pltpu.VMEM((heads * batch + batch, dim), F32), pltpu.VMEM((heads * batch + batch, dim), F32),
            pltpu.SemaphoreType.DMA((9,)), pltpu.SemaphoreType.DMA((3, tp - 1)), pltpu.SemaphoreType.DMA((3, tp)),
            pltpu.SemaphoreType.DMA((4,)), pltpu.SemaphoreType.DMA((4,)), pltpu.SemaphoreType.DMA((1,)), pltpu.SemaphoreType.DMA((1,)),
        ],
        compiler_params=pltpu.CompilerParams(collective_id=0, has_side_effects=True, vmem_limit_bytes=46000000),
        cost_estimate=pl.CostEstimate(flops=20_000_000_000, bytes_accessed=30_000_000, transcendentals=0),
        name='rest_of_layer',
    )(part, x, ln2_gain, ln2_bias, ln3_gain, ln3_bias, *in_hbm(wq_c, enc, wk_c, wv_c), wk_far, wv_far, *in_hbm(wo_c, w_up, w_down))
    return out.astype(BF16), jnp.transpose(k_new, (1, 0, 2)), jnp.transpose(v_new, (1, 0, 2))


def solution(mesh):
    row_spec = P('dp', None)
    cache_spec = P('dp', None, 'tp', None)
    head_spec = P('dp', 'tp', None)
    vec_spec = P(None)
    col_split = P(None, 'tp')
    row_split = P('tp', None)
    in_specs = (row_spec, cache_spec, cache_spec, P('dp'), P('dp', 'tp', None), vec_spec, vec_spec, col_split, col_split, col_split, row_split, vec_spec, vec_spec, col_split, col_split, col_split, row_split, vec_spec, vec_spec, col_split, row_split)
    out_specs = (row_spec, head_spec, head_spec)
    return jax.shard_map(local_step, mesh=mesh, in_specs=in_specs, out_specs=out_specs, check_vma=False)
```

```python
import functools

import jax
import jax.numpy as jnp
from jax import lax
from jax.experimental import pallas as pl
from jax.experimental.pallas import tpu as pltpu
from jax.sharding import PartitionSpec as P


LN_EPS = 1e-5
NEG = -1e30
F32 = jnp.float32
BF16 = jnp.bfloat16
CHUNK = 512
UNROLL = 4
GRAIN = 64
GROUPS = 6


def layer_norm(values, ln_gain, ln_bias):
    row_mean = jnp.mean(values, axis=-1, keepdims=True)
    centred = values - row_mean
    row_var = jnp.mean(jnp.square(centred), axis=-1, keepdims=True)
    return (centred * lax.rsqrt(row_var + LN_EPS) * ln_gain + ln_bias).astype(BF16)


def dot(lhs, rhs):
    return jnp.dot(lhs, rhs, preferred_element_type=F32)


def dot_t(lhs, rhs):
    return lax.dot_general(lhs, rhs, (((1,), (1,)), ((), ())), preferred_element_type=F32)


def in_hbm(*arrays):
    return [pltpu.with_memory_space_constraint(a, pltpu.HBM) for a in arrays]


def self_kernel(batch, heads, dim, lens_h, x_h, g_h, b_h, kc, vc, wq_h, wk_h, wv_h, wo_h,
                part_ref, knew_ref, vnew_ref,
                lens, x_v, g_v, b_v, wq, wk, wv, wo, kbuf, vbuf, q_s, v_s, o_s, m_s, l_s, acc_s, new_s, wsem, ksem, vsem):
    width = heads * dim
    scale = dim ** -0.5
    pairs = ((x_h, x_v), (g_h, g_v), (b_h, b_v), (wq_h, wq), (lens_h, lens), (wk_h, wk), (wv_h, wv), (wo_h, wo))
    ld_x, ld_g, ld_b, ld_q, ld_len, ld_k, ld_v, ld_o = [pltpu.make_async_copy(src, dst, wsem.at[i]) for i, (src, dst) in enumerate(pairs)]
    for copy in (ld_len, ld_x, ld_g, ld_b, ld_q, ld_k, ld_v):
        copy.start()

    def len_of(seq):
        return jnp.where(seq < batch, lens[jnp.minimum(seq, batch - 1)], 0)

    def following(seq, blk):
        more = (blk + 1) * CHUNK < len_of(seq)
        return jnp.where(more, seq, seq + 1), jnp.where(more, blk + 1, 0)

    def copies(seq, blk, slot, whole):
        live = pl.multiple_of(jnp.minimum(len_of(seq) - blk * CHUNK, CHUNK), GRAIN)
        first = pl.multiple_of(blk * CHUNK, CHUNK)
        count = CHUNK if whole else live
        src, dst = pl.ds(first, count), pl.ds(0, count)
        return (pltpu.make_async_copy(kc.at[seq, :, src, :], kbuf.at[slot, :, dst, :], ksem.at[slot]),
                pltpu.make_async_copy(vc.at[seq, :, src, :], vbuf.at[slot, :, dst, :], vsem.at[slot]))

    def fetch_group(group, ptr, whole):
        for u in range(UNROLL):
            seq, blk = ptr

            @pl.when(seq < batch)
            def _():
                for copy in copies(seq, blk, group * UNROLL + u, whole):
                    copy.start()

            ptr = following(seq, blk)
        return ptr

    ld_len.wait()
    ptr = (jnp.int32(0), jnp.int32(0))
    for group in range(GROUPS):
        ptr = fetch_group(group, ptr, True)
    ld_o.start()

    n_items = jnp.int32(0)
    for seq in range(batch):
        n_items = n_items + lax.div(lens[seq] + (CHUNK - 1), CHUNK)
    n_steps = lax.div(n_items + (UNROLL - 1), UNROLL)

    for copy in (ld_x, ld_g, ld_b):
        copy.wait()
    a_norm = layer_norm(x_v[...].astype(F32), g_v[...].reshape(1, -1), b_v[...].reshape(1, -1))
    ld_q.wait()
    q_s[0:batch, :] = dot(a_norm, wq[...]).astype(BF16).astype(F32)
    q_s[batch:, :] = jnp.zeros((q_s.shape[0] - batch, width), F32)
    m_s[...] = jnp.full(m_s.shape, NEG, F32)
    l_s[...] = jnp.zeros_like(l_s)
    acc_s[...] = jnp.zeros_like(acc_s)

    pair = 2 * dim
    part_rows = CHUNK // 2
    row8 = lax.broadcasted_iota(jnp.int32, (8, 1), 0)
    pair_row = lax.broadcasted_iota(jnp.int32, (8, pair), 0)
    pair_side = lax.broadcasted_iota(jnp.int32, (8, pair), 1) // dim
    sel01 = (pair_row == pair_side).astype(F32)
    sel2 = (pair_row == pair_side + 2).astype(F32)
    lane = lax.broadcasted_iota(jnp.int32, (8, CHUNK), 1)
    lane2 = lax.broadcasted_iota(jnp.int32, (8, part_rows), 1)

    def new_token():
        ld_k.wait()
        k_new = dot(a_norm, wk[...]).astype(BF16)
        ld_v.wait()
        v_new = dot(a_norm, wv[...]).astype(BF16)
        for h in range(heads):
            knew_ref[h] = k_new[:, h * dim:(h + 1) * dim]
            vnew_ref[h] = v_new[:, h * dim:(h + 1) * dim]
        qk = q_s[0:batch, :] * k_new.astype(F32)
        v_s[...] = v_new.astype(F32)
        for seq in range(batch):
            prod = qk[seq:seq + 1, :]
            tail = jnp.concatenate([prod[:, pair:width], jnp.zeros((1, pair - dim), F32)], axis=1)
            s_new = jnp.sum(prod[:, 0:pair] * sel01 + tail * sel2, axis=1, keepdims=True) * scale
            new_s[seq] = jnp.broadcast_to(jnp.where(row8 == 3, NEG, s_new), (8, dim))

    def step(i, carry):
        ptr, cur = carry[:2], carry[2:]
        group = lax.rem(i, GROUPS)

        @pl.when(i == 1)
        def _():
            new_token()

        items = []
        for u in range(UNROLL):
            items.append((*cur, group * UNROLL + u))
            cur = following(*cur)
        for seq, blk, slot in items:

            @pl.when((seq < batch) & (i < GROUPS))
            def _():
                for copy in copies(seq, blk, slot, True):
                    copy.wait()

            @pl.when((seq < batch) & (i >= GROUPS))
            def _():
                for copy in copies(seq, blk, slot, False):
                    copy.wait()
        scores = []
        for seq, blk, slot in items:
            q_row = q_s[pl.ds(jnp.minimum(seq, batch), 1), :]
            q01 = (q_row[:, 0:pair] * sel01).astype(BF16)
            q2 = (jnp.concatenate([q_row[:, pair:width]] * 2, axis=1) * sel2).astype(BF16)
            k01 = jnp.concatenate([kbuf[slot, 0], kbuf[slot, 1]], axis=1)
            k2 = jnp.concatenate([kbuf[slot, 2, 0:part_rows, :], kbuf[slot, 2, part_rows:CHUNK, :]], axis=1)
            scores.append((dot_t(q01, k01), dot_t(q2, k2)))
        weights = []
        for (seq, blk, slot), (s01, s2) in zip(items, scores):
            live = len_of(seq) - blk * CHUNK
            s01 = jnp.where(lane < jnp.where(row8 < 2, live, 0), s01 * scale, NEG)
            s2 = jnp.where(lane2 < jnp.where(row8 == 2, live, jnp.where(row8 == 3, live - part_rows, 0)), s2 * scale, NEG)
            m_i = jnp.maximum(jnp.max(s01, axis=1, keepdims=True), jnp.max(s2, axis=1, keepdims=True))
            p01 = jnp.where(row8 < 2, jnp.exp(s01 - m_i), 0.0)
            p2 = jnp.where(row8 < 2, 0.0, jnp.exp(s2 - m_i))
            l_i = jnp.sum(p01, axis=1, keepdims=True) + jnp.sum(p2, axis=1, keepdims=True)
            weights.append((m_i, l_i, p01.astype(BF16), p2.astype(BF16)))
        values = []
        for (seq, blk, slot), (m_i, l_i, p01, p2) in zip(items, weights):
            v01 = jnp.concatenate([vbuf[slot, 0], vbuf[slot, 1]], axis=1)
            v2 = jnp.concatenate([vbuf[slot, 2, 0:part_rows, :], vbuf[slot, 2, part_rows:CHUNK, :]], axis=1)
            values.append(dot(p01, v01) + dot(p2, v2))
        for (seq, blk, slot), (m_i, l_i, p01, p2), pv in zip(items, weights, values):
            row = jnp.minimum(seq, batch)
            m_old = m_s[row]
            m_new = jnp.maximum(m_old, m_i)
            keep = jnp.exp(m_old - m_new)
            add = jnp.exp(m_i - m_new)
            m_s[row] = m_new
            l_s[row] = l_s[row] * keep + l_i * add
            acc_s[row] = acc_s[row] * jnp.concatenate([keep] * 2, axis=1) + pv * jnp.concatenate([add] * 2, axis=1)
        ptr = fetch_group(group, ptr, False)
        return (*ptr, *cur)

    lax.fori_loop(0, n_steps, step, (*ptr, jnp.int32(0), jnp.int32(0)))
    for seq in range(batch):
        m_old, s_new = m_s[seq], new_s[seq]
        m = jnp.maximum(m_old, s_new)
        keep, add = jnp.exp(m_old - m), jnp.exp(s_new - m)
        v_row = v_s[seq:seq + 1, :]
        v_pair = jnp.where(pair_row < 2, v_row[:, 0:pair], jnp.concatenate([v_row[:, pair:width]] * 2, axis=1))
        l = l_s[seq] * keep + add
        acc = acc_s[seq] * jnp.concatenate([keep] * 2, axis=1) + v_pair * jnp.concatenate([add] * 2, axis=1)
        top = jnp.maximum(m[2:3], m[3:4])
        w_a, w_b = jnp.exp(m[2:3] - top), jnp.exp(m[3:4] - top)
        o2 = (acc[2:3, 0:dim] * w_a + acc[3:4, dim:pair] * w_b) / (l[2:3] * w_a + l[3:4] * w_b)
        o_s[seq:seq + 1, :] = jnp.concatenate([acc[0:1, 0:dim] / l[0:1], acc[1:2, dim:pair] / l[1:2], o2], axis=1)
    ld_o.wait()
    part_ref[...] = dot(o_s[...].astype(BF16), wo[...]).astype(BF16)


def rest_kernel(batch, heads, dim, tp, part_ref, x_ref, g2, b2, g3, b3, wqc_h, e_own_h, wk_h, wv_h, wkr_h, wvr_h, woc_h, wup_h, wdn_h,
                out_ref,
                wqc, enc, wkv, wkvr, woc, wup, wdn, kv_own, kv_rem, recv, send2, send3, qc_s, qc_r, o_snd, o_rcv,
                lsem, ssem, rsem, xs, xr, ns, nr):
    width = heads * dim
    scale = dim ** -0.5
    me = lax.axis_index('tp')
    far = lax.rem(me + 2, tp)
    near = me + 1 - 2 * lax.rem(me, 2)
    half = enc.shape[0] // 2
    early = wvr_h.shape[1]

    def load(i, src, dst):
        copy = pltpu.make_async_copy(src, dst, lsem.at[i])
        copy.start()
        return copy

    ld_e0 = load(0, e_own_h, enc.at[pl.ds(0, half), :])
    ld_wk = load(1, wk_h, wkv.at[:, pl.ds(0, width)])
    ld_wv = load(2, wv_h, wkv.at[:, pl.ds(width, width)])
    ld_wkr = load(3, wkr_h, wkvr.at[:, pl.ds(0, width)])
    ld_wvr = load(4, wvr_h, wkvr.at[:, pl.ds(width, early)])
    ld_wqc = load(5, wqc_h, wqc)
    ld_woc = load(6, woc_h, woc)
    ld_up = load(7, wup_h, wup)
    ld_dn = load(8, wdn_h, wdn)

    barrier = pltpu.get_barrier_semaphore()
    for d in range(1, tp):
        pl.semaphore_signal(barrier, inc=1, device_id={'tp': lax.rem(me + d, tp)}, device_id_type=pl.DeviceIdType.MESH)
    pl.semaphore_wait(barrier, tp - 1)

    def exchange(n, src):
        for d in range(1, tp):
            pltpu.make_async_remote_copy(src_ref=src, dst_ref=recv.at[n, me], send_sem=ssem.at[n, d - 1], recv_sem=rsem.at[n, me],
                                         device_id={'tp': lax.rem(me + d, tp)}, device_id_type=pl.DeviceIdType.MESH).start()
        recv[n, me] = src[...]

    def collect(n, src):
        for d in range(1, tp):
            other = lax.rem(me + d, tp)
            pltpu.make_async_remote_copy(src_ref=src, dst_ref=recv.at[n, other], send_sem=ssem.at[n, d - 1], recv_sem=rsem.at[n, other],
                                         device_id={'tp': other}, device_id_type=pl.DeviceIdType.MESH).wait()
        total = recv[n, 0].astype(F32)
        for t in range(1, tp):
            total = total + recv[n, t].astype(F32)
        return total

    def to_far(i, src, dst):
        return pltpu.make_async_remote_copy(src_ref=src, dst_ref=dst, send_sem=xs.at[i], recv_sem=xr.at[i],
                                            device_id={'tp': far}, device_id_type=pl.DeviceIdType.MESH)

    def project(first, count, jobs, tile=256):
        def body(i, c):
            rows = pl.ds(pl.multiple_of(i * tile, tile), tile)
            for weights, out, lo, hi in jobs:
                out[rows, lo:hi] = dot(enc[rows, :], weights[:, lo:hi]).astype(BF16)
            return c

        lax.fori_loop(first // tile, (first + count) // tile, body, 0)

    late_rows = (0, 640, wv_h.shape[0])

    def late(i):
        rows, cols = pl.ds(late_rows[i], late_rows[i + 1] - late_rows[i]), width - early
        return to_far(2 + i, wv_h.at[rows, pl.ds(early, cols)], wkvr.at[rows, pl.ds(width + early, cols)])

    exchange(0, part_ref)
    near_e = pltpu.make_async_remote_copy(src_ref=e_own_h, dst_ref=enc.at[pl.ds(half, half), :], send_sem=ns.at[0], recv_sem=nr.at[0],
                                          device_id={'tp': near}, device_id_type=pl.DeviceIdType.MESH)
    near_e.start()
    late(0).start()
    jobs = ((wkv, kv_own, 0, 2 * width), (wkvr, kv_rem, 0, width + early))
    for copy in (ld_e0, ld_wk, ld_wv, ld_wkr, ld_wvr):
        copy.wait()
    project(0, half, jobs)

    h1 = x_ref[...].astype(F32) + collect(0, part_ref)
    c_norm = layer_norm(h1, g2[...].reshape(1, -1), b2[...].reshape(1, -1))
    ld_wqc.wait()
    qc_s[...] = dot(c_norm, wqc[...]).astype(BF16)
    send_q = to_far(0, qc_s, qc_r)
    send_q.start()
    late(1).start()
    near_e.wait()
    project(half, half, jobs[1:])
    for i in range(2):
        late(i).wait()
    project(0, 2 * half, ((wkvr, kv_rem, width + early, 2 * width),))

    rows = heads * batch
    row_b = lax.rem(lax.broadcasted_iota(jnp.int32, (rows, 128), 0), batch)
    lane = lax.broadcasted_iota(jnp.int32, (rows, 128), 1)
    per = half // batch
    pack = 128 // per
    blocks = half // 128
    mine = lax.rem(row_b, pack) == lane // per
    row_blk = row_b // pack
    lane_head = lax.broadcasted_iota(jnp.int32, (batch, width), 1) // dim

    def attend(q, kv):
        qf = q.astype(F32)
        q_rows = jnp.concatenate([jnp.where(lane_head == h, qf, 0.0) for h in range(heads)], axis=0).astype(BF16)
        parts = []
        for part in range(2):
            s_all = dot_t(q_rows, kv[part * half:(part + 1) * half, 0:width])
            s = s_all[:, 0:128]
            for k in range(1, blocks):
                s = jnp.where(row_blk == k, s_all[:, k * 128:(k + 1) * 128], s)
            parts.append(jnp.where(mine, s * scale, NEG))
        m = jnp.maximum(jnp.max(parts[0], axis=1, keepdims=True), jnp.max(parts[1], axis=1, keepdims=True))
        p = [jnp.exp(s - m) for s in parts]
        l = jnp.sum(p[0], axis=1, keepdims=True) + jnp.sum(p[1], axis=1, keepdims=True)
        o = None
        for part in range(2):
            p_wide = jnp.concatenate([jnp.where(row_blk == k, p[part], 0.0) for k in range(blocks)], axis=1).astype(BF16)
            o_part = dot(p_wide, kv[part * half:(part + 1) * half, width:2 * width])
            o = o_part if o is None else o + o_part
        o = jnp.concatenate([o[h * batch:(h + 1) * batch, h * dim:(h + 1) * dim] for h in range(heads)], axis=0)
        return m, l, o

    send_q.wait()
    m_r, l_r, o_r = attend(qc_r[...], kv_rem)
    o_snd[0:rows, :] = o_r
    stats = jnp.zeros((batch, dim), F32)
    st_lane = lax.broadcasted_iota(jnp.int32, (batch, dim), 1)
    for h in range(heads):
        stats = jnp.where(st_lane == 2 * h, m_r[h * batch:(h + 1) * batch], jnp.where(st_lane == 2 * h + 1, l_r[h * batch:(h + 1) * batch], stats))
    o_snd[rows:rows + batch, :] = stats
    send_o = to_far(1, o_snd, o_rcv)
    send_o.start()
    project(half, half, jobs[:1])
    m_a, l_a, o_a = attend(qc_s[...], kv_own)
    send_o.wait()
    stats = o_rcv[rows:rows + batch, :]
    m_b = jnp.concatenate([stats[:, 2 * h:2 * h + 1] for h in range(heads)], axis=0)
    l_b = jnp.concatenate([stats[:, 2 * h + 1:2 * h + 2] for h in range(heads)], axis=0)
    m = jnp.maximum(m_a, m_b)
    w_a, w_b = jnp.exp(m_a - m), jnp.exp(m_b - m)
    o = (o_a * w_a + o_rcv[0:rows, :] * w_b) / (l_a * w_a + l_b * w_b)
    oc = jnp.concatenate([o[h * batch:(h + 1) * batch, :] for h in range(heads)], axis=1).astype(BF16)
    ld_woc.wait()
    send2[...] = dot(oc, woc[...]).astype(BF16)
    exchange(1, send2)
    h2 = h1 + collect(1, send2)
    m_norm = layer_norm(h2, g3[...].reshape(1, -1), b3[...].reshape(1, -1))
    ld_up.wait()
    up = dot(m_norm, wup[...])
    hidden = (0.5 * up * (1.0 + lax.erf(up * (0.5 ** 0.5)))).astype(BF16)
    ld_dn.wait()
    send3[...] = dot(hidden, wdn[...]).astype(BF16)
    exchange(2, send3)
    out_ref[...] = h2 + collect(2, send3)


def local_step(x, k_cache, v_cache, seq_lens, nbr_enc, ln1_gain, ln1_bias, w_q, w_k, w_v, w_o, ln2_gain, ln2_bias, wq_c, wk_c, wv_c, wo_c, ln3_gain, ln3_bias, w_up, w_down):
    batch, d_model = x.shape
    heads, dim = k_cache.shape[2:]
    width = heads * dim
    tp = lax.axis_size('tp')
    far = [(i, (i + 2) % tp) for i in range(tp)]
    enc = nbr_enc.reshape(-1, nbr_enc.shape[-1])
    wk_far = lax.ppermute(wk_c, 'tp', far)
    wv_cut = wv_c[:, :2 * dim]
    wv_far = lax.ppermute(wv_cut, 'tp', far)

    any_spec = pl.BlockSpec(memory_space=pl.ANY)
    hbm = pl.BlockSpec(memory_space=pltpu.HBM)
    vmem = pl.BlockSpec(memory_space=pltpu.VMEM)
    slots = GROUPS * UNROLL
    part, k_new, v_new = pl.pallas_call(
        functools.partial(self_kernel, batch, heads, dim),
        out_shape=(jax.ShapeDtypeStruct((batch, d_model), BF16), jax.ShapeDtypeStruct((heads, batch, dim), BF16), jax.ShapeDtypeStruct((heads, batch, dim), BF16)),
        in_specs=[hbm] * 10,
        out_specs=(vmem, vmem, vmem),
        scratch_shapes=[
            pltpu.SMEM((batch,), jnp.int32), pltpu.VMEM((batch, d_model), BF16), pltpu.VMEM((d_model,), F32), pltpu.VMEM((d_model,), F32),
            pltpu.VMEM((d_model, width), BF16), pltpu.VMEM((d_model, width), BF16), pltpu.VMEM((d_model, width), BF16), pltpu.VMEM((width, d_model), BF16),
            pltpu.VMEM((slots, heads, CHUNK, dim), BF16), pltpu.VMEM((slots, heads, CHUNK, dim), BF16),
            pltpu.VMEM((batch + 8, width), F32), pltpu.VMEM((batch, width), F32), pltpu.VMEM((batch, width), F32),
            pltpu.VMEM((batch + 1, 8, dim), F32), pltpu.VMEM((batch + 1, 8, dim), F32), pltpu.VMEM((batch + 1, 8, 2 * dim), F32), pltpu.VMEM((batch, 8, dim), F32),
            pltpu.SemaphoreType.DMA((8,)), pltpu.SemaphoreType.DMA((slots,)), pltpu.SemaphoreType.DMA((slots,)),
        ],
        compiler_params=pltpu.CompilerParams(vmem_limit_bytes=46000000),
        cost_estimate=pl.CostEstimate(flops=40_000_000_000, bytes_accessed=60_000_000, transcendentals=0),
        name='self_attention',
    )(*in_hbm(seq_lens, x, ln1_gain, ln1_bias, jnp.transpose(k_cache, (0, 2, 1, 3)), jnp.transpose(v_cache, (0, 2, 1, 3)), w_q, w_k, w_v, w_o))

    n_enc, enc_dim = enc.shape
    ff = w_up.shape[1]
    out = pl.pallas_call(
        functools.partial(rest_kernel, batch, heads, dim, tp),
        out_shape=jax.ShapeDtypeStruct((batch, d_model), F32),
        in_specs=[vmem] * 6 + [hbm] * 4 + [any_spec] * 2 + [hbm] * 3,
        out_specs=vmem,
        scratch_shapes=[
            pltpu.VMEM((d_model, width), BF16), pltpu.VMEM((2 * n_enc, enc_dim), BF16),
            pltpu.VMEM((enc_dim, 2 * width), BF16), pltpu.VMEM((enc_dim, 2 * width), BF16),
            pltpu.VMEM((width, d_model), BF16), pltpu.VMEM((d_model, ff), BF16), pltpu.VMEM((ff, d_model), BF16),
            pltpu.VMEM((2 * n_enc, 2 * width), BF16), pltpu.VMEM((2 * n_enc, 2 * width), BF16),
            pltpu.VMEM((3, tp, batch, d_model), BF16), pltpu.VMEM((batch, d_model), BF16), pltpu.VMEM((batch, d_model), BF16),
            pltpu.VMEM((batch, width), BF16), pltpu.VMEM((batch, width), BF16),
            pltpu.VMEM((heads * batch + batch, dim), F32), pltpu.VMEM((heads * batch + batch, dim), F32),
            pltpu.SemaphoreType.DMA((9,)), pltpu.SemaphoreType.DMA((3, tp - 1)), pltpu.SemaphoreType.DMA((3, tp)),
            pltpu.SemaphoreType.DMA((4,)), pltpu.SemaphoreType.DMA((4,)), pltpu.SemaphoreType.DMA((1,)), pltpu.SemaphoreType.DMA((1,)),
        ],
        compiler_params=pltpu.CompilerParams(collective_id=0, has_side_effects=True, vmem_limit_bytes=46000000),
        cost_estimate=pl.CostEstimate(flops=20_000_000_000, bytes_accessed=30_000_000, transcendentals=0),
        name='rest_of_layer',
    )(part, x, ln2_gain, ln2_bias, ln3_gain, ln3_bias, *in_hbm(wq_c, enc, wk_c, wv_c), wk_far, wv_far, *in_hbm(wo_c, w_up, w_down))
    return out.astype(BF16), jnp.transpose(k_new, (1, 0, 2)), jnp.transpose(v_new, (1, 0, 2))


def solution(mesh):
    row_spec = P('dp', None)
    cache_spec = P('dp', None, 'tp', None)
    head_spec = P('dp', 'tp', None)
    vec_spec = P(None)
    col_split = P(None, 'tp')
    row_split = P('tp', None)
    in_specs = (row_spec, cache_spec, cache_spec, P('dp'), P('dp', 'tp', None), vec_spec, vec_spec, col_split, col_split, col_split, row_split, vec_spec, vec_spec, col_split, col_split, col_split, row_split, vec_spec, vec_spec, col_split, row_split)
    out_specs = (row_spec, head_spec, head_spec)
    return jax.shard_map(local_step, mesh=mesh, in_specs=in_specs, out_specs=out_specs, check_vma=False)
```

```python
import functools

import jax
import jax.numpy as jnp
from jax import lax
from jax.experimental import pallas as pl
from jax.experimental.pallas import tpu as pltpu
from jax.sharding import PartitionSpec as P


LN_EPS = 1e-5
NEG = -1e30
F32 = jnp.float32
BF16 = jnp.bfloat16
CHUNK = 512
UNROLL = 4
GRAIN = 64
GROUPS = 6


def layer_norm(values, ln_gain, ln_bias):
    row_mean = jnp.mean(values, axis=-1, keepdims=True)
    centred = values - row_mean
    row_var = jnp.mean(jnp.square(centred), axis=-1, keepdims=True)
    return (centred * lax.rsqrt(row_var + LN_EPS) * ln_gain + ln_bias).astype(BF16)


def dot(lhs, rhs):
    return jnp.dot(lhs, rhs, preferred_element_type=F32)


def dot_t(lhs, rhs):
    return lax.dot_general(lhs, rhs, (((1,), (1,)), ((), ())), preferred_element_type=F32)


def in_hbm(*arrays):
    return [pltpu.with_memory_space_constraint(a, pltpu.HBM) for a in arrays]


def self_kernel(batch, heads, dim, lens_h, x_h, g_h, b_h, kc, vc, wq_h, wk_h, wv_h, wo_h,
                part_ref, knew_ref, vnew_ref,
                lens, x_v, g_v, b_v, wq, wk, wv, wo, kbuf, vbuf, q_s, v_s, o_s, m_s, l_s, acc_s, new_s, wsem, ksem, vsem):
    width = heads * dim
    scale = dim ** -0.5
    pairs = ((x_h, x_v), (g_h, g_v), (b_h, b_v), (wq_h, wq), (lens_h, lens), (wk_h, wk), (wv_h, wv), (wo_h, wo))
    ld_x, ld_g, ld_b, ld_q, ld_len, ld_k, ld_v, ld_o = [pltpu.make_async_copy(src, dst, wsem.at[i]) for i, (src, dst) in enumerate(pairs)]
    for copy in (ld_len, ld_x, ld_g, ld_b, ld_q, ld_k, ld_v):
        copy.start()

    def len_of(seq):
        return jnp.where(seq < batch, lens[jnp.minimum(seq, batch - 1)], 0)

    def following(seq, blk):
        more = (blk + 1) * CHUNK < len_of(seq)
        return jnp.where(more, seq, seq + 1), jnp.where(more, blk + 1, 0)

    def copies(seq, blk, slot, whole):
        live = pl.multiple_of(jnp.minimum(len_of(seq) - blk * CHUNK, CHUNK), GRAIN)
        first = pl.multiple_of(blk * CHUNK, CHUNK)
        count = CHUNK if whole else live
        src, dst = pl.ds(first, count), pl.ds(0, count)
        return (pltpu.make_async_copy(kc.at[seq, :, src, :], kbuf.at[slot, :, dst, :], ksem.at[slot]),
                pltpu.make_async_copy(vc.at[seq, :, src, :], vbuf.at[slot, :, dst, :], vsem.at[slot]))

    def fetch_group(group, ptr, whole):
        for u in range(UNROLL):
            seq, blk = ptr

            @pl.when(seq < batch)
            def _():
                for copy in copies(seq, blk, group * UNROLL + u, whole):
                    copy.start()

            ptr = following(seq, blk)
        return ptr

    ld_len.wait()
    ptr = (jnp.int32(0), jnp.int32(0))
    for group in range(GROUPS):
        ptr = fetch_group(group, ptr, True)
    ld_o.start()

    n_items = jnp.int32(0)
    for seq in range(batch):
        n_items = n_items + lax.div(lens[seq] + (CHUNK - 1), CHUNK)
    n_steps = lax.div(n_items + (UNROLL - 1), UNROLL)

    for copy in (ld_x, ld_g, ld_b):
        copy.wait()
    a_norm = layer_norm(x_v[...].astype(F32), g_v[...].reshape(1, -1), b_v[...].reshape(1, -1))
    ld_q.wait()
    q_s[0:batch, :] = dot(a_norm, wq[...]).astype(BF16).astype(F32)
    q_s[batch:, :] = jnp.zeros((q_s.shape[0] - batch, width), F32)
    m_s[...] = jnp.full(m_s.shape, NEG, F32)
    l_s[...] = jnp.zeros_like(l_s)
    acc_s[...] = jnp.zeros_like(acc_s)

    pair = 2 * dim
    part_rows = CHUNK // 2
    row8 = lax.broadcasted_iota(jnp.int32, (8, 1), 0)
    pair_row = lax.broadcasted_iota(jnp.int32, (8, pair), 0)
    pair_side = lax.broadcasted_iota(jnp.int32, (8, pair), 1) // dim
    sel01 = (pair_row == pair_side).astype(F32)
    sel2 = (pair_row == pair_side + 2).astype(F32)
    lane = lax.broadcasted_iota(jnp.int32, (8, CHUNK), 1)
    lane2 = lax.broadcasted_iota(jnp.int32, (8, part_rows), 1)

    def new_token():
        ld_k.wait()
        k_new = dot(a_norm, wk[...]).astype(BF16)
        ld_v.wait()
        v_new = dot(a_norm, wv[...]).astype(BF16)
        for h in range(heads):
            knew_ref[h] = k_new[:, h * dim:(h + 1) * dim]
            vnew_ref[h] = v_new[:, h * dim:(h + 1) * dim]
        qk = q_s[0:batch, :] * k_new.astype(F32)
        v_s[...] = v_new.astype(F32)
        for seq in range(batch):
            prod = qk[seq:seq + 1, :]
            tail = jnp.concatenate([prod[:, pair:width], jnp.zeros((1, pair - dim), F32)], axis=1)
            s_new = jnp.sum(prod[:, 0:pair] * sel01 + tail * sel2, axis=1, keepdims=True) * scale
            new_s[seq] = jnp.broadcast_to(jnp.where(row8 == 3, NEG, s_new), (8, dim))

    def step(i, carry):
        ptr, cur = carry[:2], carry[2:]
        group = lax.rem(i, GROUPS)

        @pl.when(i == 1)
        def _():
            new_token()

        items = []
        for u in range(UNROLL):
            items.append((*cur, group * UNROLL + u))
            cur = following(*cur)
        for seq, blk, slot in items:

            @pl.when((seq < batch) & (i < GROUPS))
            def _():
                for copy in copies(seq, blk, slot, True):
                    copy.wait()

            @pl.when((seq < batch) & (i >= GROUPS))
            def _():
                for copy in copies(seq, blk, slot, False):
                    copy.wait()
        scores = []
        for seq, blk, slot in items:
            q_row = q_s[pl.ds(jnp.minimum(seq, batch), 1), :]
            q01 = (q_row[:, 0:pair] * sel01).astype(BF16)
            q2 = (jnp.concatenate([q_row[:, pair:width]] * 2, axis=1) * sel2).astype(BF16)
            k01 = jnp.concatenate([kbuf[slot, 0], kbuf[slot, 1]], axis=1)
            k2 = jnp.concatenate([kbuf[slot, 2, 0:part_rows, :], kbuf[slot, 2, part_rows:CHUNK, :]], axis=1)
            scores.append((dot_t(q01, k01), dot_t(q2, k2)))
        weights = []
        for (seq, blk, slot), (s01, s2) in zip(items, scores):
            live = len_of(seq) - blk * CHUNK
            s01 = jnp.where(lane < jnp.where(row8 < 2, live, 0), s01 * scale, NEG)
            s2 = jnp.where(lane2 < jnp.where(row8 == 2, live, jnp.where(row8 == 3, live - part_rows, 0)), s2 * scale, NEG)
            m_i = jnp.maximum(jnp.max(s01, axis=1, keepdims=True), jnp.max(s2, axis=1, keepdims=True))
            p01 = jnp.where(row8 < 2, jnp.exp(s01 - m_i), 0.0)
            p2 = jnp.where(row8 < 2, 0.0, jnp.exp(s2 - m_i))
            l_i = jnp.sum(p01, axis=1, keepdims=True) + jnp.sum(p2, axis=1, keepdims=True)
            weights.append((m_i, l_i, p01.astype(BF16), p2.astype(BF16)))
        values = []
        for (seq, blk, slot), (m_i, l_i, p01, p2) in zip(items, weights):
            v01 = jnp.concatenate([vbuf[slot, 0], vbuf[slot, 1]], axis=1)
            v2 = jnp.concatenate([vbuf[slot, 2, 0:part_rows, :], vbuf[slot, 2, part_rows:CHUNK, :]], axis=1)
            values.append(dot(p01, v01) + dot(p2, v2))
        for (seq, blk, slot), (m_i, l_i, p01, p2), pv in zip(items, weights, values):
            row = jnp.minimum(seq, batch)
            m_old = m_s[row]
            m_new = jnp.maximum(m_old, m_i)
            keep = jnp.exp(m_old - m_new)
            add = jnp.exp(m_i - m_new)
            m_s[row] = m_new
            l_s[row] = l_s[row] * keep + l_i * add
            acc_s[row] = acc_s[row] * jnp.concatenate([keep] * 2, axis=1) + pv * jnp.concatenate([add] * 2, axis=1)
        ptr = fetch_group(group, ptr, False)
        return (*ptr, *cur)

    lax.fori_loop(0, n_steps, step, (*ptr, jnp.int32(0), jnp.int32(0)))
    for seq in range(batch):
        m_old, s_new = m_s[seq], new_s[seq]
        m = jnp.maximum(m_old, s_new)
        keep, add = jnp.exp(m_old - m), jnp.exp(s_new - m)
        v_row = v_s[seq:seq + 1, :]
        v_pair = jnp.where(pair_row < 2, v_row[:, 0:pair], jnp.concatenate([v_row[:, pair:width]] * 2, axis=1))
        l = l_s[seq] * keep + add
        acc = acc_s[seq] * jnp.concatenate([keep] * 2, axis=1) + v_pair * jnp.concatenate([add] * 2, axis=1)
        top = jnp.maximum(m[2:3], m[3:4])
        w_a, w_b = jnp.exp(m[2:3] - top), jnp.exp(m[3:4] - top)
        o2 = (acc[2:3, 0:dim] * w_a + acc[3:4, dim:pair] * w_b) / (l[2:3] * w_a + l[3:4] * w_b)
        o_s[seq:seq + 1, :] = jnp.concatenate([acc[0:1, 0:dim] / l[0:1], acc[1:2, dim:pair] / l[1:2], o2], axis=1)
    ld_o.wait()
    part_ref[...] = dot(o_s[...].astype(BF16), wo[...]).astype(BF16)


def rest_kernel(batch, heads, dim, tp, part_ref, x_ref, g2, b2, g3, b3, wqc_h, e_own_h, wk_h, wv_h, wkr_h, wvr_h, woc_h, wup_h, wdn_h,
                out_ref,
                wqc, enc, wkv, wkvr, woc, wup, wdn, kv_own, kv_rem, v_late, near_1, far_2, sum_1, got_1, sum_2, got_2, send2, send3,
                qc_s, qc_r, o_snd, o_rcv, o2_snd, o2_rcv, lsem, ssem, rsem, xs, xr, ns, nr):
    width = heads * dim
    scale = dim ** -0.5
    d_model = part_ref.shape[1]
    cut, quarter = d_model // 2, d_model // 4
    me = lax.axis_index('tp')
    core = lax.rem(me, 2)
    far = lax.rem(me + 2, tp)
    near = me + 1 - 2 * core
    diag = lax.rem(near + 2, tp)
    half = enc.shape[0] // 2
    early = wvr_h.shape[1]

    def load(i, src, dst):
        copy = pltpu.make_async_copy(src, dst, lsem.at[i])
        copy.start()
        return copy

    ld_e0 = load(0, e_own_h, enc.at[pl.ds(0, half), :])
    ld_wk = load(1, wk_h, wkv.at[:, pl.ds(0, width)])
    ld_wv = load(2, wv_h, wkv.at[:, pl.ds(width, width)])
    ld_wkr = load(3, wkr_h, wkvr.at[:, pl.ds(0, width)])
    ld_wvr = load(4, wvr_h, wkvr.at[:, pl.ds(width, early)])
    ld_wqc = load(5, wqc_h, wqc)
    ld_woc = load(6, woc_h, woc)
    ld_up = load(7, wup_h, wup)
    ld_dn = load(8, wdn_h, wdn)

    barrier = pltpu.get_barrier_semaphore()
    for d in range(1, tp):
        pl.semaphore_signal(barrier, inc=1, device_id={'tp': lax.rem(me + d, tp)}, device_id_type=pl.DeviceIdType.MESH)
    pl.semaphore_wait(barrier, tp - 1)

    def remote(src, dst, send_sem, recv_sem, device):
        return pltpu.make_async_remote_copy(src_ref=src, dst_ref=dst, send_sem=send_sem, recv_sem=recv_sem,
                                            device_id={'tp': device}, device_id_type=pl.DeviceIdType.MESH)

    def far_copy(n, src):
        return remote(src.at[:, pl.ds(cut, cut)], far_2.at[n], ssem.at[n, 1], rsem.at[n, 1], far)

    def near_copy(n, src):
        return remote(src.at[:, pl.ds(0, cut)], near_1.at[n], ssem.at[n, 0], rsem.at[n, 0], near)

    def quarter_copies(n):
        return [remote(sum_1.at[n, core], got_1.at[n, core], ssem.at[n, 2 + k], rsem.at[n, 2 + core], device) for k, device in enumerate((far, diag))]

    def across_copy(n):
        return remote(sum_2.at[n], got_2.at[n], ssem.at[n, 4], rsem.at[n, 4], near)

    def pass_near(n, src):
        near_copy(n, src).wait()
        pair = (src[:, 0:cut].astype(F32) + near_1[n].astype(F32)).astype(BF16)
        for k in range(2):
            sum_1[n, k] = pair[:, k * quarter:(k + 1) * quarter]
        for copy in quarter_copies(n):
            copy.start()

    def pass_far(n, src):
        far_copy(n, src).wait()
        sum_2[n] = (src[:, cut:].astype(F32) + far_2[n].astype(F32)).astype(BF16)
        across_copy(n).start()

    def total(n):
        for copy in quarter_copies(n):
            copy.wait_send()
        for k in range(2):
            remote(sum_1.at[n, k], got_1.at[n, k], ssem.at[n, 2], rsem.at[n, 2 + k], far).wait_recv()
        across_copy(n).wait()
        return jnp.concatenate([sum_1[n, k].astype(F32) + got_1[n, k].astype(F32) for k in range(2)] + [sum_2[n].astype(F32) + got_2[n].astype(F32)], axis=1)

    def project(first, count, jobs, tile=256):
        def body(i, c):
            rows = pl.ds(pl.multiple_of(i * tile, tile), tile)
            for weights, out, lo, hi in jobs:
                out[rows, lo:hi] = dot(enc[rows, :], weights[:, lo:hi]).astype(BF16)
            return c

        lax.fori_loop(first // tile, (first + count) // tile, body, 0)

    late_rows = (0, 512, wv_h.shape[0])

    def late(i):
        rows, cols = pl.ds(late_rows[i], late_rows[i + 1] - late_rows[i]), width - early
        return remote(wv_h.at[rows, pl.ds(early, cols)], wkvr.at[rows, pl.ds(width + early, cols)], xs.at[3 + i], xr.at[3 + i], far)

    def late_product(i, tile=256):
        lo, hi = late_rows[i], late_rows[i + 1]

        def body(t, c):
            rows = pl.ds(pl.multiple_of(t * tile, tile), tile)
            product = dot(enc[rows, lo:hi], wkvr[lo:hi, width + early:2 * width])
            if i == 0:
                v_late[rows, :] = product
            else:
                kv_rem[rows, width + early:2 * width] = (v_late[rows, :] + product).astype(BF16)
            return c

        lax.fori_loop(0, 2 * half // tile, body, 0)

    def near_tokens(i):
        rows = half // 2
        return remote(e_own_h.at[pl.ds(i * rows, rows), :], enc.at[pl.ds(half + i * rows, rows), :], ns.at[i], nr.at[i], near)

    own_job = (wkv, kv_own, 0, 2 * width)
    far_job = (wkvr, kv_rem, 0, width + early)

    far_copy(0, part_ref).start()
    near_copy(0, part_ref).start()
    near_tokens(0).start()
    pass_near(0, part_ref)
    late(0).start()
    for copy in (ld_e0, ld_wk, ld_wv, ld_wkr, ld_wvr):
        copy.wait()
    project(0, half // 2, (own_job, far_job))
    pass_far(0, part_ref)
    near_tokens(1).start()
    project(half // 2, half // 2, (far_job,))
    h1 = x_ref[...].astype(F32) + total(0)
    c_norm = layer_norm(h1, g2[...].reshape(1, -1), b2[...].reshape(1, -1))
    ld_wqc.wait()
    qc_s[...] = dot(c_norm, wqc[...]).astype(BF16)
    send_q = remote(qc_s, qc_r, xs.at[0], xr.at[0], far)
    send_q.start()
    late(1).start()
    near_tokens(0).wait()
    near_tokens(1).wait()
    project(half, half, (far_job,))
    late(0).wait()
    late_product(0)

    rows = heads * batch
    row_b = lax.rem(lax.broadcasted_iota(jnp.int32, (rows, 128), 0), batch)
    lane = lax.broadcasted_iota(jnp.int32, (rows, 128), 1)
    per = half // batch
    pack = 128 // per
    blocks = half // 128
    mine = lax.rem(row_b, pack) == lane // per
    row_blk = row_b // pack
    lane_head = lax.broadcasted_iota(jnp.int32, (batch, width), 1) // dim

    def weigh(q, kv):
        qf = q.astype(F32)
        q_rows = jnp.concatenate([jnp.where(lane_head == h, qf, 0.0) for h in range(heads)], axis=0).astype(BF16)
        parts = []
        for part in range(2):
            s_all = dot_t(q_rows, kv[part * half:(part + 1) * half, 0:width])
            s = s_all[:, 0:128]
            for k in range(1, blocks):
                s = jnp.where(row_blk == k, s_all[:, k * 128:(k + 1) * 128], s)
            parts.append(jnp.where(mine, s * scale, NEG))
        m = jnp.maximum(jnp.max(parts[0], axis=1, keepdims=True), jnp.max(parts[1], axis=1, keepdims=True))
        p = [jnp.exp(s - m) for s in parts]
        l = jnp.sum(p[0], axis=1, keepdims=True) + jnp.sum(p[1], axis=1, keepdims=True)
        wide = [jnp.concatenate([jnp.where(row_blk == k, p[part], 0.0) for k in range(blocks)], axis=1).astype(BF16) for part in range(2)]
        return m, l, wide

    def mix(wide, kv, first, last):
        lo, hi = first * batch, last * batch
        o = sum(dot(wide[part][lo:hi], kv[part * half:(part + 1) * half, width + first * dim:width + last * dim]) for part in range(2))
        return jnp.concatenate([o[(h - first) * batch:(h - first + 1) * batch, (h - first) * dim:(h - first + 1) * dim] for h in range(first, last)], axis=0)

    n_early = early // dim
    send_q.wait()
    m_r, l_r, wide_r = weigh(qc_r[...], kv_rem)
    o_snd[0:n_early * batch, :] = mix(wide_r, kv_rem, 0, n_early)
    stats = jnp.zeros((batch, dim), F32)
    st_lane = lax.broadcasted_iota(jnp.int32, (batch, dim), 1)
    for h in range(heads):
        stats = jnp.where(st_lane == 2 * h, m_r[h * batch:(h + 1) * batch], jnp.where(st_lane == 2 * h + 1, l_r[h * batch:(h + 1) * batch], stats))
    o_snd[n_early * batch:(n_early + 1) * batch, :] = stats
    send_o = remote(o_snd, o_rcv, xs.at[1], xr.at[1], far)
    send_o.start()
    late(1).wait()
    late_product(1)
    o2_snd[...] = mix(wide_r, kv_rem, n_early, heads)
    send_o2 = remote(o2_snd, o2_rcv, xs.at[2], xr.at[2], far)
    send_o2.start()
    project(half // 2, half // 2 + half, (own_job,))
    m_a, l_a, wide_a = weigh(qc_s[...], kv_own)
    o_a = mix(wide_a, kv_own, 0, heads)
    send_o.wait()
    stats = o_rcv[n_early * batch:(n_early + 1) * batch, :]
    m_b = jnp.concatenate([stats[:, 2 * h:2 * h + 1] for h in range(heads)], axis=0)
    l_b = jnp.concatenate([stats[:, 2 * h + 1:2 * h + 2] for h in range(heads)], axis=0)
    m = jnp.maximum(m_a, m_b)
    w_a, w_b = jnp.exp(m_a - m), jnp.exp(m_b - m)
    send_o2.wait()
    o_b = jnp.concatenate([o_rcv[0:n_early * batch, :], o2_rcv[...]], axis=0)
    o = (o_a * w_a + o_b * w_b) / (l_a * w_a + l_b * w_b)
    oc = jnp.concatenate([o[h * batch:(h + 1) * batch, :] for h in range(heads)], axis=1).astype(BF16)

    def matmul_sum(n, lhs, weights, out):
        out[:, cut:] = dot(lhs, weights[:, cut:]).astype(BF16)
        far_copy(n, out).start()
        out[:, 0:cut] = dot(lhs, weights[:, 0:cut]).astype(BF16)
        near_copy(n, out).start()
        pass_near(n, out)
        pass_far(n, out)
        return total(n)

    ld_woc.wait()
    h2 = h1 + matmul_sum(1, oc, woc, send2)
    m_norm = layer_norm(h2, g3[...].reshape(1, -1), b3[...].reshape(1, -1))
    ld_up.wait()
    up = dot(m_norm, wup[...])
    hidden = (0.5 * up * (1.0 + lax.erf(up * (0.5 ** 0.5)))).astype(BF16)
    ld_dn.wait()
    out_ref[...] = h2 + matmul_sum(2, hidden, wdn, send3)


def local_step(x, k_cache, v_cache, seq_lens, nbr_enc, ln1_gain, ln1_bias, w_q, w_k, w_v, w_o, ln2_gain, ln2_bias, wq_c, wk_c, wv_c, wo_c, ln3_gain, ln3_bias, w_up, w_down):
    batch, d_model = x.shape
    heads, dim = k_cache.shape[2:]
    width = heads * dim
    tp = lax.axis_size('tp')
    far = [(i, (i + 2) % tp) for i in range(tp)]
    enc = nbr_enc.reshape(-1, nbr_enc.shape[-1])
    wk_far = lax.ppermute(wk_c, 'tp', far)
    wv_cut = wv_c[:, :2 * dim]
    wv_far = lax.ppermute(wv_cut, 'tp', far)

    any_spec = pl.BlockSpec(memory_space=pl.ANY)
    hbm = pl.BlockSpec(memory_space=pltpu.HBM)
    vmem = pl.BlockSpec(memory_space=pltpu.VMEM)
    slots = GROUPS * UNROLL
    part, k_new, v_new = pl.pallas_call(
        functools.partial(self_kernel, batch, heads, dim),
        out_shape=(jax.ShapeDtypeStruct((batch, d_model), BF16), jax.ShapeDtypeStruct((heads, batch, dim), BF16), jax.ShapeDtypeStruct((heads, batch, dim), BF16)),
        in_specs=[hbm] * 10,
        out_specs=(vmem, vmem, vmem),
        scratch_shapes=[
            pltpu.SMEM((batch,), jnp.int32), pltpu.VMEM((batch, d_model), BF16), pltpu.VMEM((d_model,), F32), pltpu.VMEM((d_model,), F32),
            pltpu.VMEM((d_model, width), BF16), pltpu.VMEM((d_model, width), BF16), pltpu.VMEM((d_model, width), BF16), pltpu.VMEM((width, d_model), BF16),
            pltpu.VMEM((slots, heads, CHUNK, dim), BF16), pltpu.VMEM((slots, heads, CHUNK, dim), BF16),
            pltpu.VMEM((batch + 8, width), F32), pltpu.VMEM((batch, width), F32), pltpu.VMEM((batch, width), F32),
            pltpu.VMEM((batch + 1, 8, dim), F32), pltpu.VMEM((batch + 1, 8, dim), F32), pltpu.VMEM((batch + 1, 8, 2 * dim), F32), pltpu.VMEM((batch, 8, dim), F32),
            pltpu.SemaphoreType.DMA((8,)), pltpu.SemaphoreType.DMA((slots,)), pltpu.SemaphoreType.DMA((slots,)),
        ],
        compiler_params=pltpu.CompilerParams(vmem_limit_bytes=46000000),
        cost_estimate=pl.CostEstimate(flops=40_000_000_000, bytes_accessed=60_000_000, transcendentals=0),
        name='self_attention',
    )(*in_hbm(seq_lens, x, ln1_gain, ln1_bias, jnp.transpose(k_cache, (0, 2, 1, 3)), jnp.transpose(v_cache, (0, 2, 1, 3)), w_q, w_k, w_v, w_o))

    n_enc, enc_dim = enc.shape
    ff = w_up.shape[1]
    out = pl.pallas_call(
        functools.partial(rest_kernel, batch, heads, dim, tp),
        out_shape=jax.ShapeDtypeStruct((batch, d_model), F32),
        in_specs=[vmem] * 6 + [hbm] * 4 + [any_spec] * 2 + [hbm] * 3,
        out_specs=vmem,
        scratch_shapes=[
            pltpu.VMEM((d_model, width), BF16), pltpu.VMEM((2 * n_enc, enc_dim), BF16),
            pltpu.VMEM((enc_dim, 2 * width), BF16), pltpu.VMEM((enc_dim, 2 * width), BF16),
            pltpu.VMEM((width, d_model), BF16), pltpu.VMEM((d_model, ff), BF16), pltpu.VMEM((ff, d_model), BF16),
            pltpu.VMEM((2 * n_enc, 2 * width), BF16), pltpu.VMEM((2 * n_enc, 2 * width), BF16), pltpu.VMEM((2 * n_enc, dim), F32),
            pltpu.VMEM((3, batch, d_model // 2), BF16), pltpu.VMEM((3, batch, d_model // 2), BF16),
            pltpu.VMEM((3, 2, batch, d_model // 4), BF16), pltpu.VMEM((3, 2, batch, d_model // 4), BF16),
            pltpu.VMEM((3, batch, d_model // 2), BF16), pltpu.VMEM((3, batch, d_model // 2), BF16),
            pltpu.VMEM((batch, d_model), BF16), pltpu.VMEM((batch, d_model), BF16),
            pltpu.VMEM((batch, width), BF16), pltpu.VMEM((batch, width), BF16),
            pltpu.VMEM((heads * batch, dim), F32), pltpu.VMEM((heads * batch, dim), F32), pltpu.VMEM((batch, dim), F32), pltpu.VMEM((batch, dim), F32),
            pltpu.SemaphoreType.DMA((9,)), pltpu.SemaphoreType.DMA((3, 5)), pltpu.SemaphoreType.DMA((3, 5)),
            pltpu.SemaphoreType.DMA((5,)), pltpu.SemaphoreType.DMA((5,)), pltpu.SemaphoreType.DMA((2,)), pltpu.SemaphoreType.DMA((2,)),
        ],
        compiler_params=pltpu.CompilerParams(collective_id=0, has_side_effects=True, vmem_limit_bytes=46000000),
        cost_estimate=pl.CostEstimate(flops=20_000_000_000, bytes_accessed=30_000_000, transcendentals=0),
        name='rest_of_layer',
    )(part, x, ln2_gain, ln2_bias, ln3_gain, ln3_bias, *in_hbm(wq_c, enc, wk_c, wv_c), wk_far, wv_far, *in_hbm(wo_c, w_up, w_down))
    return out.astype(BF16), jnp.transpose(k_new, (1, 0, 2)), jnp.transpose(v_new, (1, 0, 2))


def solution(mesh):
    row_spec = P('dp', None)
    cache_spec = P('dp', None, 'tp', None)
    head_spec = P('dp', 'tp', None)
    vec_spec = P(None)
    col_split = P(None, 'tp')
    row_split = P('tp', None)
    in_specs = (row_spec, cache_spec, cache_spec, P('dp'), P('dp', 'tp', None), vec_spec, vec_spec, col_split, col_split, col_split, row_split, vec_spec, vec_spec, col_split, col_split, col_split, row_split, vec_spec, vec_spec, col_split, row_split)
    out_specs = (row_spec, head_spec, head_spec)
    return jax.shard_map(local_step, mesh=mesh, in_specs=in_specs, out_specs=out_specs, check_vma=False)
```

```python
import functools

import jax
import jax.numpy as jnp
from jax import lax
from jax.experimental import pallas as pl
from jax.experimental.pallas import tpu as pltpu
from jax.sharding import PartitionSpec as P


LN_EPS = 1e-5
NEG = -1e30
F32 = jnp.float32
BF16 = jnp.bfloat16
CHUNK = 512
UNROLL = 4
GRAIN = 64
GROUPS = 6


def layer_norm(values, ln_gain, ln_bias):
    row_mean = jnp.mean(values, axis=-1, keepdims=True)
    centred = values - row_mean
    row_var = jnp.mean(jnp.square(centred), axis=-1, keepdims=True)
    return (centred * lax.rsqrt(row_var + LN_EPS) * ln_gain + ln_bias).astype(BF16)


def dot(lhs, rhs):
    return jnp.dot(lhs, rhs, preferred_element_type=F32)


def dot_t(lhs, rhs):
    return lax.dot_general(lhs, rhs, (((1,), (1,)), ((), ())), preferred_element_type=F32)


def in_hbm(*arrays):
    return [pltpu.with_memory_space_constraint(a, pltpu.HBM) for a in arrays]


def self_kernel(batch, heads, dim, lens_h, x_h, g_h, b_h, kc, vc, wq_h, wk_h, wv_h, wo_h,
                part_ref, knew_ref, vnew_ref,
                lens, x_v, g_v, b_v, wq, wk, wv, wo, kbuf, vbuf, q_s, v_s, o_s, m_s, l_s, acc_s, new_s, wsem, ksem, vsem):
    width = heads * dim
    scale = dim ** -0.5
    pairs = ((x_h, x_v), (g_h, g_v), (b_h, b_v), (wq_h, wq), (lens_h, lens), (wk_h, wk), (wv_h, wv), (wo_h, wo))
    ld_x, ld_g, ld_b, ld_q, ld_len, ld_k, ld_v, ld_o = [pltpu.make_async_copy(src, dst, wsem.at[i]) for i, (src, dst) in enumerate(pairs)]
    for copy in (ld_len, ld_x, ld_g, ld_b, ld_q, ld_k, ld_v):
        copy.start()

    def len_of(seq):
        return jnp.where(seq < batch, lens[jnp.minimum(seq, batch - 1)], 0)

    def following(seq, blk):
        more = (blk + 1) * CHUNK < len_of(seq)
        return jnp.where(more, seq, seq + 1), jnp.where(more, blk + 1, 0)

    def copies(seq, blk, slot, whole):
        live = pl.multiple_of(jnp.minimum(len_of(seq) - blk * CHUNK, CHUNK), GRAIN)
        first = pl.multiple_of(blk * CHUNK, CHUNK)
        count = CHUNK if whole else live
        src, dst = pl.ds(first, count), pl.ds(0, count)
        return (pltpu.make_async_copy(kc.at[seq, :, src, :], kbuf.at[slot, :, dst, :], ksem.at[slot]),
                pltpu.make_async_copy(vc.at[seq, :, src, :], vbuf.at[slot, :, dst, :], vsem.at[slot]))

    def fetch_group(group, ptr, whole):
        for u in range(UNROLL):
            seq, blk = ptr

            @pl.when(seq < batch)
            def _():
                for copy in copies(seq, blk, group * UNROLL + u, whole):
                    copy.start()

            ptr = following(seq, blk)
        return ptr

    ld_len.wait()
    ptr = (jnp.int32(0), jnp.int32(0))
    for group in range(GROUPS):
        ptr = fetch_group(group, ptr, True)
    ld_o.start()

    n_items = jnp.int32(0)
    for seq in range(batch):
        n_items = n_items + lax.div(lens[seq] + (CHUNK - 1), CHUNK)
    n_steps = lax.div(n_items + (UNROLL - 1), UNROLL)

    for copy in (ld_x, ld_g, ld_b):
        copy.wait()
    a_norm = layer_norm(x_v[...].astype(F32), g_v[...].reshape(1, -1), b_v[...].reshape(1, -1))
    ld_q.wait()
    q_s[0:batch, :] = dot(a_norm, wq[...]).astype(BF16).astype(F32)
    q_s[batch:, :] = jnp.zeros((q_s.shape[0] - batch, width), F32)
    m_s[...] = jnp.full(m_s.shape, NEG, F32)
    l_s[...] = jnp.zeros_like(l_s)
    acc_s[...] = jnp.zeros_like(acc_s)

    pair = 2 * dim
    part_rows = CHUNK // 2
    row8 = lax.broadcasted_iota(jnp.int32, (8, 1), 0)
    pair_row = lax.broadcasted_iota(jnp.int32, (8, pair), 0)
    pair_side = lax.broadcasted_iota(jnp.int32, (8, pair), 1) // dim
    sel01 = (pair_row == pair_side).astype(F32)
    sel2 = (pair_row == pair_side + 2).astype(F32)
    lane = lax.broadcasted_iota(jnp.int32, (8, CHUNK), 1)
    lane2 = lax.broadcasted_iota(jnp.int32, (8, part_rows), 1)

    def new_token():
        ld_k.wait()
        k_new = dot(a_norm, wk[...]).astype(BF16)
        ld_v.wait()
        v_new = dot(a_norm, wv[...]).astype(BF16)
        for h in range(heads):
            knew_ref[h] = k_new[:, h * dim:(h + 1) * dim]
            vnew_ref[h] = v_new[:, h * dim:(h + 1) * dim]
        qk = q_s[0:batch, :] * k_new.astype(F32)
        v_s[...] = v_new.astype(F32)
        for seq in range(batch):
            prod = qk[seq:seq + 1, :]
            tail = jnp.concatenate([prod[:, pair:width], jnp.zeros((1, pair - dim), F32)], axis=1)
            s_new = jnp.sum(prod[:, 0:pair] * sel01 + tail * sel2, axis=1, keepdims=True) * scale
            new_s[seq] = jnp.broadcast_to(jnp.where(row8 == 3, NEG, s_new), (8, dim))

    def step(i, carry):
        ptr, cur = carry[:2], carry[2:]
        group = lax.rem(i, GROUPS)

        @pl.when(i == 1)
        def _():
            new_token()

        items = []
        for u in range(UNROLL):
            items.append((*cur, group * UNROLL + u))
            cur = following(*cur)
        for seq, blk, slot in items:

            @pl.when((seq < batch) & (i < GROUPS))
            def _():
                for copy in copies(seq, blk, slot, True):
                    copy.wait()

            @pl.when((seq < batch) & (i >= GROUPS))
            def _():
                for copy in copies(seq, blk, slot, False):
                    copy.wait()
        scores = []
        for seq, blk, slot in items:
            q_row = q_s[pl.ds(jnp.minimum(seq, batch), 1), :]
            q01 = (q_row[:, 0:pair] * sel01).astype(BF16)
            q2 = (jnp.concatenate([q_row[:, pair:width]] * 2, axis=1) * sel2).astype(BF16)
            k01 = jnp.concatenate([kbuf[slot, 0], kbuf[slot, 1]], axis=1)
            k2 = jnp.concatenate([kbuf[slot, 2, 0:part_rows, :], kbuf[slot, 2, part_rows:CHUNK, :]], axis=1)
            scores.append((dot_t(q01, k01), dot_t(q2, k2)))
        weights = []
        for (seq, blk, slot), (s01, s2) in zip(items, scores):
            live = len_of(seq) - blk * CHUNK
            s01 = jnp.where(lane < jnp.where(row8 < 2, live, 0), s01 * scale, NEG)
            s2 = jnp.where(lane2 < jnp.where(row8 == 2, live, jnp.where(row8 == 3, live - part_rows, 0)), s2 * scale, NEG)
            m_i = jnp.maximum(jnp.max(s01, axis=1, keepdims=True), jnp.max(s2, axis=1, keepdims=True))
            p01 = jnp.where(row8 < 2, jnp.exp(s01 - m_i), 0.0)
            p2 = jnp.where(row8 < 2, 0.0, jnp.exp(s2 - m_i))
            l_i = jnp.sum(p01, axis=1, keepdims=True) + jnp.sum(p2, axis=1, keepdims=True)
            weights.append((m_i, l_i, p01.astype(BF16), p2.astype(BF16)))
        values = []
        for (seq, blk, slot), (m_i, l_i, p01, p2) in zip(items, weights):
            v01 = jnp.concatenate([vbuf[slot, 0], vbuf[slot, 1]], axis=1)
            v2 = jnp.concatenate([vbuf[slot, 2, 0:part_rows, :], vbuf[slot, 2, part_rows:CHUNK, :]], axis=1)
            values.append(dot(p01, v01) + dot(p2, v2))
        for (seq, blk, slot), (m_i, l_i, p01, p2), pv in zip(items, weights, values):
            row = jnp.minimum(seq, batch)
            m_old = m_s[row]
            m_new = jnp.maximum(m_old, m_i)
            keep = jnp.exp(m_old - m_new)
            add = jnp.exp(m_i - m_new)
            m_s[row] = m_new
            l_s[row] = l_s[row] * keep + l_i * add
            acc_s[row] = acc_s[row] * jnp.concatenate([keep] * 2, axis=1) + pv * jnp.concatenate([add] * 2, axis=1)
        ptr = fetch_group(group, ptr, False)
        return (*ptr, *cur)

    lax.fori_loop(0, n_steps, step, (*ptr, jnp.int32(0), jnp.int32(0)))
    for seq in range(batch):
        m_old, s_new = m_s[seq], new_s[seq]
        m = jnp.maximum(m_old, s_new)
        keep, add = jnp.exp(m_old - m), jnp.exp(s_new - m)
        v_row = v_s[seq:seq + 1, :]
        v_pair = jnp.where(pair_row < 2, v_row[:, 0:pair], jnp.concatenate([v_row[:, pair:width]] * 2, axis=1))
        l = l_s[seq] * keep + add
        acc = acc_s[seq] * jnp.concatenate([keep] * 2, axis=1) + v_pair * jnp.concatenate([add] * 2, axis=1)
        top = jnp.maximum(m[2:3], m[3:4])
        w_a, w_b = jnp.exp(m[2:3] - top), jnp.exp(m[3:4] - top)
        o2 = (acc[2:3, 0:dim] * w_a + acc[3:4, dim:pair] * w_b) / (l[2:3] * w_a + l[3:4] * w_b)
        o_s[seq:seq + 1, :] = jnp.concatenate([acc[0:1, 0:dim] / l[0:1], acc[1:2, dim:pair] / l[1:2], o2], axis=1)
    ld_o.wait()
    part_ref[...] = dot(o_s[...].astype(BF16), wo[...]).astype(BF16)


def rest_kernel(batch, heads, dim, tp, part_ref, x_ref, g2, b2, g3, b3, wqc_h, e_own_h, wk_h, wv_h, wkr_h, wvr_h, woc_h, wup_h, wdn_h,
                out_ref,
                wqc, enc, wkv, wkvr, woc, wup, wdn, kv_own, kv_rem, v_late, recv, send2, send3,
                qc_s, qc_r, o_snd, o_rcv, o2_snd, o2_rcv, lsem, ssem, rsem, xs, xr, ns, nr):
    width = heads * dim
    scale = dim ** -0.5
    me = lax.axis_index('tp')
    far = lax.rem(me + 2, tp)
    near = me + 1 - 2 * lax.rem(me, 2)
    half = enc.shape[0] // 2
    early = wvr_h.shape[1]

    def load(i, src, dst):
        copy = pltpu.make_async_copy(src, dst, lsem.at[i])
        copy.start()
        return copy

    ld_e0 = load(0, e_own_h, enc.at[pl.ds(0, half), :])
    ld_wk = load(1, wk_h, wkv.at[:, pl.ds(0, width)])
    ld_wv = load(2, wv_h, wkv.at[:, pl.ds(width, width)])
    ld_wkr = load(3, wkr_h, wkvr.at[:, pl.ds(0, width)])
    ld_wvr = load(4, wvr_h, wkvr.at[:, pl.ds(width, early)])
    ld_wqc = load(5, wqc_h, wqc)
    ld_woc = load(6, woc_h, woc)
    ld_up = load(7, wup_h, wup)
    ld_dn = load(8, wdn_h, wdn)

    barrier = pltpu.get_barrier_semaphore()
    for d in range(1, tp):
        pl.semaphore_signal(barrier, inc=1, device_id={'tp': lax.rem(me + d, tp)}, device_id_type=pl.DeviceIdType.MESH)
    pl.semaphore_wait(barrier, tp - 1)

    def remote(src, dst, send_sem, recv_sem, device):
        return pltpu.make_async_remote_copy(src_ref=src, dst_ref=dst, send_sem=send_sem, recv_sem=recv_sem,
                                            device_id={'tp': device}, device_id_type=pl.DeviceIdType.MESH)

    def sum_copies(n, src):
        return [remote(src, recv.at[n, me], ssem.at[n, d - 1], rsem.at[n, me], lax.rem(me + d, tp)) for d in range(1, tp)]

    def exchange(n, src):
        for copy in sum_copies(n, src):
            copy.start()
        recv[n, me] = src[...]

    def collect(n, src):
        for copy in sum_copies(n, src):
            copy.wait_send()
        for d in range(1, tp):
            other = lax.rem(me + d, tp)
            remote(src, recv.at[n, other], ssem.at[n, d - 1], rsem.at[n, other], other).wait_recv()
        total = recv[n, 0].astype(F32)
        for t in range(1, tp):
            total = total + recv[n, t].astype(F32)
        return total

    def project(first, count, jobs, tile=256):
        def body(i, c):
            rows = pl.ds(pl.multiple_of(i * tile, tile), tile)
            for weights, out, lo, hi in jobs:
                out[rows, lo:hi] = dot(enc[rows, :], weights[:, lo:hi]).astype(BF16)
            return c

        lax.fori_loop(first // tile, (first + count) // tile, body, 0)

    late_rows = (0, 512, wv_h.shape[0])

    def late(i):
        rows, cols = pl.ds(late_rows[i], late_rows[i + 1] - late_rows[i]), width - early
        return remote(wv_h.at[rows, pl.ds(early, cols)], wkvr.at[rows, pl.ds(width + early, cols)], xs.at[3 + i], xr.at[3 + i], far)

    def late_product(i, tile=256):
        lo, hi = late_rows[i], late_rows[i + 1]

        def body(t, c):
            rows = pl.ds(pl.multiple_of(t * tile, tile), tile)
            product = dot(enc[rows, lo:hi], wkvr[lo:hi, width + early:2 * width])
            if i == 0:
                v_late[rows, :] = product
            else:
                kv_rem[rows, width + early:2 * width] = (v_late[rows, :] + product).astype(BF16)
            return c

        lax.fori_loop(0, 2 * half // tile, body, 0)

    def near_tokens(i):
        rows = half // 2
        return remote(e_own_h.at[pl.ds(i * rows, rows), :], enc.at[pl.ds(half + i * rows, rows), :], ns.at[i], nr.at[i], near)

    own_job = (wkv, kv_own, 0, 2 * width)
    far_job = (wkvr, kv_rem, 0, width + early)

    exchange(0, part_ref)
    near_tokens(0).start()
    near_tokens(1).start()
    late(0).start()
    for copy in (ld_e0, ld_wk, ld_wv, ld_wkr, ld_wvr):
        copy.wait()
    project(0, half, (own_job, far_job))
    h1 = x_ref[...].astype(F32) + collect(0, part_ref)
    c_norm = layer_norm(h1, g2[...].reshape(1, -1), b2[...].reshape(1, -1))
    ld_wqc.wait()
    qc_s[...] = dot(c_norm, wqc[...]).astype(BF16)
    send_q = remote(qc_s, qc_r, xs.at[0], xr.at[0], far)
    send_q.start()
    late(1).start()
    near_tokens(0).wait()
    near_tokens(1).wait()
    project(half, half, (far_job,))
    late(0).wait()
    late_product(0)

    rows = heads * batch
    row_b = lax.rem(lax.broadcasted_iota(jnp.int32, (rows, 128), 0), batch)
    lane = lax.broadcasted_iota(jnp.int32, (rows, 128), 1)
    per = half // batch
    pack = 128 // per
    blocks = half // 128
    mine = lax.rem(row_b, pack) == lane // per
    row_blk = row_b // pack
    lane_head = lax.broadcasted_iota(jnp.int32, (batch, width), 1) // dim

    def weigh(q, kv):
        qf = q.astype(F32)
        q_rows = jnp.concatenate([jnp.where(lane_head == h, qf, 0.0) for h in range(heads)], axis=0).astype(BF16)
        parts = []
        for part in range(2):
            s_all = dot_t(q_rows, kv[part * half:(part + 1) * half, 0:width])
            s = s_all[:, 0:128]
            for k in range(1, blocks):
                s = jnp.where(row_blk == k, s_all[:, k * 128:(k + 1) * 128], s)
            parts.append(jnp.where(mine, s * scale, NEG))
        m = jnp.maximum(jnp.max(parts[0], axis=1, keepdims=True), jnp.max(parts[1], axis=1, keepdims=True))
        p = [jnp.exp(s - m) for s in parts]
        l = jnp.sum(p[0], axis=1, keepdims=True) + jnp.sum(p[1], axis=1, keepdims=True)
        wide = [jnp.concatenate([jnp.where(row_blk == k, p[part], 0.0) for k in range(blocks)], axis=1).astype(BF16) for part in range(2)]
        return m, l, wide

    def mix(wide, kv, first, last):
        lo, hi = first * batch, last * batch
        o = sum(dot(wide[part][lo:hi], kv[part * half:(part + 1) * half, width + first * dim:width + last * dim]) for part in range(2))
        return jnp.concatenate([o[(h - first) * batch:(h - first + 1) * batch, (h - first) * dim:(h - first + 1) * dim] for h in range(first, last)], axis=0)

    n_early = early // dim
    send_q.wait()
    m_r, l_r, wide_r = weigh(qc_r[...], kv_rem)
    o_snd[0:n_early * batch, :] = mix(wide_r, kv_rem, 0, n_early)
    stats = jnp.zeros((batch, dim), F32)
    st_lane = lax.broadcasted_iota(jnp.int32, (batch, dim), 1)
    for h in range(heads):
        stats = jnp.where(st_lane == 2 * h, m_r[h * batch:(h + 1) * batch], jnp.where(st_lane == 2 * h + 1, l_r[h * batch:(h + 1) * batch], stats))
    o_snd[n_early * batch:(n_early + 1) * batch, :] = stats
    send_o = remote(o_snd, o_rcv, xs.at[1], xr.at[1], far)
    send_o.start()
    late(1).wait()
    late_product(1)
    o2_snd[...] = mix(wide_r, kv_rem, n_early, heads)
    send_o2 = remote(o2_snd, o2_rcv, xs.at[2], xr.at[2], far)
    send_o2.start()
    project(half, half, (own_job,))
    m_a, l_a, wide_a = weigh(qc_s[...], kv_own)
    o_a = mix(wide_a, kv_own, 0, heads)
    send_o.wait()
    stats = o_rcv[n_early * batch:(n_early + 1) * batch, :]
    m_b = jnp.concatenate([stats[:, 2 * h:2 * h + 1] for h in range(heads)], axis=0)
    l_b = jnp.concatenate([stats[:, 2 * h + 1:2 * h + 2] for h in range(heads)], axis=0)
    m = jnp.maximum(m_a, m_b)
    w_a, w_b = jnp.exp(m_a - m), jnp.exp(m_b - m)
    send_o2.wait()
    o_b = jnp.concatenate([o_rcv[0:n_early * batch, :], o2_rcv[...]], axis=0)
    o = (o_a * w_a + o_b * w_b) / (l_a * w_a + l_b * w_b)
    oc = jnp.concatenate([o[h * batch:(h + 1) * batch, :] for h in range(heads)], axis=1).astype(BF16)

    def matmul_sum(n, lhs, weights, out):
        out[...] = dot(lhs, weights[...]).astype(BF16)
        exchange(n, out)
        return collect(n, out)

    ld_woc.wait()
    h2 = h1 + matmul_sum(1, oc, woc, send2)
    m_norm = layer_norm(h2, g3[...].reshape(1, -1), b3[...].reshape(1, -1))
    ld_up.wait()
    up = dot(m_norm, wup[...])
    hidden = (0.5 * up * (1.0 + lax.erf(up * (0.5 ** 0.5)))).astype(BF16)
    ld_dn.wait()
    out_ref[...] = h2 + matmul_sum(2, hidden, wdn, send3)


def local_step(x, k_cache, v_cache, seq_lens, nbr_enc, ln1_gain, ln1_bias, w_q, w_k, w_v, w_o, ln2_gain, ln2_bias, wq_c, wk_c, wv_c, wo_c, ln3_gain, ln3_bias, w_up, w_down):
    batch, d_model = x.shape
    heads, dim = k_cache.shape[2:]
    width = heads * dim
    tp = lax.axis_size('tp')
    far = [(i, (i + 2) % tp) for i in range(tp)]
    enc = nbr_enc.reshape(-1, nbr_enc.shape[-1])
    wk_far = lax.ppermute(wk_c, 'tp', far)
    wv_cut = wv_c[:, :2 * dim]
    wv_far = lax.ppermute(wv_cut, 'tp', far)

    any_spec = pl.BlockSpec(memory_space=pl.ANY)
    hbm = pl.BlockSpec(memory_space=pltpu.HBM)
    vmem = pl.BlockSpec(memory_space=pltpu.VMEM)
    slots = GROUPS * UNROLL
    part, k_new, v_new = pl.pallas_call(
        functools.partial(self_kernel, batch, heads, dim),
        out_shape=(jax.ShapeDtypeStruct((batch, d_model), BF16), jax.ShapeDtypeStruct((heads, batch, dim), BF16), jax.ShapeDtypeStruct((heads, batch, dim), BF16)),
        in_specs=[hbm] * 10,
        out_specs=(vmem, vmem, vmem),
        scratch_shapes=[
            pltpu.SMEM((batch,), jnp.int32), pltpu.VMEM((batch, d_model), BF16), pltpu.VMEM((d_model,), F32), pltpu.VMEM((d_model,), F32),
            pltpu.VMEM((d_model, width), BF16), pltpu.VMEM((d_model, width), BF16), pltpu.VMEM((d_model, width), BF16), pltpu.VMEM((width, d_model), BF16),
            pltpu.VMEM((slots, heads, CHUNK, dim), BF16), pltpu.VMEM((slots, heads, CHUNK, dim), BF16),
            pltpu.VMEM((batch + 8, width), F32), pltpu.VMEM((batch, width), F32), pltpu.VMEM((batch, width), F32),
            pltpu.VMEM((batch + 1, 8, dim), F32), pltpu.VMEM((batch + 1, 8, dim), F32), pltpu.VMEM((batch + 1, 8, 2 * dim), F32), pltpu.VMEM((batch, 8, dim), F32),
            pltpu.SemaphoreType.DMA((8,)), pltpu.SemaphoreType.DMA((slots,)), pltpu.SemaphoreType.DMA((slots,)),
        ],
        compiler_params=pltpu.CompilerParams(vmem_limit_bytes=46000000),
        cost_estimate=pl.CostEstimate(flops=40_000_000_000, bytes_accessed=60_000_000, transcendentals=0),
        name='self_attention',
    )(*in_hbm(seq_lens, x, ln1_gain, ln1_bias, jnp.transpose(k_cache, (0, 2, 1, 3)), jnp.transpose(v_cache, (0, 2, 1, 3)), w_q, w_k, w_v, w_o))

    n_enc, enc_dim = enc.shape
    ff = w_up.shape[1]
    out = pl.pallas_call(
        functools.partial(rest_kernel, batch, heads, dim, tp),
        out_shape=jax.ShapeDtypeStruct((batch, d_model), F32),
        in_specs=[vmem] * 6 + [hbm] * 4 + [any_spec] * 2 + [hbm] * 3,
        out_specs=vmem,
        scratch_shapes=[
            pltpu.VMEM((d_model, width), BF16), pltpu.VMEM((2 * n_enc, enc_dim), BF16),
            pltpu.VMEM((enc_dim, 2 * width), BF16), pltpu.VMEM((enc_dim, 2 * width), BF16),
            pltpu.VMEM((width, d_model), BF16), pltpu.VMEM((d_model, ff), BF16), pltpu.VMEM((ff, d_model), BF16),
            pltpu.VMEM((2 * n_enc, 2 * width), BF16), pltpu.VMEM((2 * n_enc, 2 * width), BF16), pltpu.VMEM((2 * n_enc, dim), F32),
            pltpu.VMEM((3, tp, batch, d_model), BF16),
            pltpu.VMEM((batch, d_model), BF16), pltpu.VMEM((batch, d_model), BF16),
            pltpu.VMEM((batch, width), BF16), pltpu.VMEM((batch, width), BF16),
            pltpu.VMEM((heads * batch, dim), F32), pltpu.VMEM((heads * batch, dim), F32), pltpu.VMEM((batch, dim), F32), pltpu.VMEM((batch, dim), F32),
            pltpu.SemaphoreType.DMA((9,)), pltpu.SemaphoreType.DMA((3, tp - 1)), pltpu.SemaphoreType.DMA((3, tp)),
            pltpu.SemaphoreType.DMA((5,)), pltpu.SemaphoreType.DMA((5,)), pltpu.SemaphoreType.DMA((2,)), pltpu.SemaphoreType.DMA((2,)),
        ],
        compiler_params=pltpu.CompilerParams(collective_id=0, has_side_effects=True, vmem_limit_bytes=46000000),
        cost_estimate=pl.CostEstimate(flops=20_000_000_000, bytes_accessed=30_000_000, transcendentals=0),
        name='rest_of_layer',
    )(part, x, ln2_gain, ln2_bias, ln3_gain, ln3_bias, *in_hbm(wq_c, enc, wk_c, wv_c), wk_far, wv_far, *in_hbm(wo_c, w_up, w_down))
    return out.astype(BF16), jnp.transpose(k_new, (1, 0, 2)), jnp.transpose(v_new, (1, 0, 2))


def solution(mesh):
    row_spec = P('dp', None)
    cache_spec = P('dp', None, 'tp', None)
    head_spec = P('dp', 'tp', None)
    vec_spec = P(None)
    col_split = P(None, 'tp')
    row_split = P('tp', None)
    in_specs = (row_spec, cache_spec, cache_spec, P('dp'), P('dp', 'tp', None), vec_spec, vec_spec, col_split, col_split, col_split, row_split, vec_spec, vec_spec, col_split, col_split, col_split, row_split, vec_spec, vec_spec, col_split, row_split)
    out_specs = (row_spec, head_spec, head_spec)
    return jax.shard_map(local_step, mesh=mesh, in_specs=in_specs, out_specs=out_specs, check_vma=False)
```

```python
import functools

import jax
import jax.numpy as jnp
from jax import lax
from jax.experimental import pallas as pl
from jax.experimental.pallas import tpu as pltpu
from jax.sharding import PartitionSpec as P


LN_EPS = 1e-5
NEG = -1e30
F32 = jnp.float32
BF16 = jnp.bfloat16
CHUNK = 512
UNROLL = 4
GRAIN = 64
GROUPS = 6
PIECES = 3


def layer_norm(values, ln_gain, ln_bias):
    row_mean = jnp.mean(values, axis=-1, keepdims=True)
    centred = values - row_mean
    row_var = jnp.mean(jnp.square(centred), axis=-1, keepdims=True)
    return (centred * lax.rsqrt(row_var + LN_EPS) * ln_gain + ln_bias).astype(BF16)


def dot(lhs, rhs):
    return jnp.dot(lhs, rhs, preferred_element_type=F32)


def dot_t(lhs, rhs):
    return lax.dot_general(lhs, rhs, (((1,), (1,)), ((), ())), preferred_element_type=F32)


def in_hbm(*arrays):
    return [pltpu.with_memory_space_constraint(a, pltpu.HBM) for a in arrays]


def self_kernel(batch, heads, dim, lens_h, x_h, g_h, b_h, kc, vc, wq_h, wk_h, wv_h, wo_h,
                part_ref, knew_ref, vnew_ref,
                lens, x_v, g_v, b_v, wq, wk, wv, wo, kbuf, vbuf, q_s, v_s, o_s, m_s, l_s, acc_s, new_s, wsem, ksem, vsem):
    width = heads * dim
    scale = dim ** -0.5
    pairs = ((x_h, x_v), (g_h, g_v), (b_h, b_v), (wq_h, wq), (lens_h, lens), (wk_h, wk), (wv_h, wv), (wo_h, wo))
    ld_x, ld_g, ld_b, ld_q, ld_len, ld_k, ld_v, ld_o = [pltpu.make_async_copy(src, dst, wsem.at[i]) for i, (src, dst) in enumerate(pairs)]
    for copy in (ld_len, ld_x, ld_g, ld_b, ld_q, ld_k, ld_v):
        copy.start()

    def len_of(seq):
        return jnp.where(seq < batch, lens[jnp.minimum(seq, batch - 1)], 0)

    def following(seq, blk):
        more = (blk + 1) * CHUNK < len_of(seq)
        return jnp.where(more, seq, seq + 1), jnp.where(more, blk + 1, 0)

    def copies(seq, blk, slot, whole):
        live = pl.multiple_of(jnp.minimum(len_of(seq) - blk * CHUNK, CHUNK), GRAIN)
        first = pl.multiple_of(blk * CHUNK, CHUNK)
        count = CHUNK if whole else live
        src, dst = pl.ds(first, count), pl.ds(0, count)
        return (pltpu.make_async_copy(kc.at[seq, :, src, :], kbuf.at[slot, :, dst, :], ksem.at[slot]),
                pltpu.make_async_copy(vc.at[seq, :, src, :], vbuf.at[slot, :, dst, :], vsem.at[slot]))

    def fetch_group(group, ptr, whole):
        for u in range(UNROLL):
            seq, blk = ptr

            @pl.when(seq < batch)
            def _():
                for copy in copies(seq, blk, group * UNROLL + u, whole):
                    copy.start()

            ptr = following(seq, blk)
        return ptr

    ld_len.wait()
    ptr = (jnp.int32(0), jnp.int32(0))
    for group in range(GROUPS):
        ptr = fetch_group(group, ptr, True)
    ld_o.start()

    n_items = jnp.int32(0)
    for seq in range(batch):
        n_items = n_items + lax.div(lens[seq] + (CHUNK - 1), CHUNK)
    n_steps = lax.div(n_items + (UNROLL - 1), UNROLL)

    for copy in (ld_x, ld_g, ld_b):
        copy.wait()
    a_norm = layer_norm(x_v[...].astype(F32), g_v[...].reshape(1, -1), b_v[...].reshape(1, -1))
    ld_q.wait()
    q_s[0:batch, :] = dot(a_norm, wq[...]).astype(BF16).astype(F32)
    q_s[batch:, :] = jnp.zeros((q_s.shape[0] - batch, width), F32)
    m_s[...] = jnp.full(m_s.shape, NEG, F32)
    l_s[...] = jnp.zeros_like(l_s)
    acc_s[...] = jnp.zeros_like(acc_s)

    pair = 2 * dim
    part_rows = CHUNK // 2
    row8 = lax.broadcasted_iota(jnp.int32, (8, 1), 0)
    pair_row = lax.broadcasted_iota(jnp.int32, (8, pair), 0)
    pair_side = lax.broadcasted_iota(jnp.int32, (8, pair), 1) // dim
    sel01 = (pair_row == pair_side).astype(F32)
    sel2 = (pair_row == pair_side + 2).astype(F32)
    lane = lax.broadcasted_iota(jnp.int32, (8, CHUNK), 1)
    lane2 = lax.broadcasted_iota(jnp.int32, (8, part_rows), 1)

    def new_token():
        ld_k.wait()
        k_new = dot(a_norm, wk[...]).astype(BF16)
        ld_v.wait()
        v_new = dot(a_norm, wv[...]).astype(BF16)
        for h in range(heads):
            knew_ref[h] = k_new[:, h * dim:(h + 1) * dim]
            vnew_ref[h] = v_new[:, h * dim:(h + 1) * dim]
        qk = q_s[0:batch, :] * k_new.astype(F32)
        v_s[...] = v_new.astype(F32)
        for seq in range(batch):
            prod = qk[seq:seq + 1, :]
            tail = jnp.concatenate([prod[:, pair:width], jnp.zeros((1, pair - dim), F32)], axis=1)
            s_new = jnp.sum(prod[:, 0:pair] * sel01 + tail * sel2, axis=1, keepdims=True) * scale
            new_s[seq] = jnp.broadcast_to(jnp.where(row8 == 3, NEG, s_new), (8, dim))

    def step(i, carry):
        ptr, cur = carry[:2], carry[2:]
        group = lax.rem(i, GROUPS)

        @pl.when(i == 1)
        def _():
            new_token()

        items = []
        for u in range(UNROLL):
            items.append((*cur, group * UNROLL + u))
            cur = following(*cur)
        for seq, blk, slot in items:

            @pl.when((seq < batch) & (i < GROUPS))
            def _():
                for copy in copies(seq, blk, slot, True):
                    copy.wait()

            @pl.when((seq < batch) & (i >= GROUPS))
            def _():
                for copy in copies(seq, blk, slot, False):
                    copy.wait()
        scores = []
        for seq, blk, slot in items:
            q_row = q_s[pl.ds(jnp.minimum(seq, batch), 1), :]
            q01 = (q_row[:, 0:pair] * sel01).astype(BF16)
            q2 = (jnp.concatenate([q_row[:, pair:width]] * 2, axis=1) * sel2).astype(BF16)
            k01 = jnp.concatenate([kbuf[slot, 0], kbuf[slot, 1]], axis=1)
            k2 = jnp.concatenate([kbuf[slot, 2, 0:part_rows, :], kbuf[slot, 2, part_rows:CHUNK, :]], axis=1)
            scores.append((dot_t(q01, k01), dot_t(q2, k2)))
        weights = []
        for (seq, blk, slot), (s01, s2) in zip(items, scores):
            live = len_of(seq) - blk * CHUNK
            s01 = jnp.where(lane < jnp.where(row8 < 2, live, 0), s01 * scale, NEG)
            s2 = jnp.where(lane2 < jnp.where(row8 == 2, live, jnp.where(row8 == 3, live - part_rows, 0)), s2 * scale, NEG)
            m_i = jnp.maximum(jnp.max(s01, axis=1, keepdims=True), jnp.max(s2, axis=1, keepdims=True))
            p01 = jnp.where(row8 < 2, jnp.exp(s01 - m_i), 0.0)
            p2 = jnp.where(row8 < 2, 0.0, jnp.exp(s2 - m_i))
            l_i = jnp.sum(p01, axis=1, keepdims=True) + jnp.sum(p2, axis=1, keepdims=True)
            weights.append((m_i, l_i, p01.astype(BF16), p2.astype(BF16)))
        values = []
        for (seq, blk, slot), (m_i, l_i, p01, p2) in zip(items, weights):
            v01 = jnp.concatenate([vbuf[slot, 0], vbuf[slot, 1]], axis=1)
            v2 = jnp.concatenate([vbuf[slot, 2, 0:part_rows, :], vbuf[slot, 2, part_rows:CHUNK, :]], axis=1)
            values.append(dot(p01, v01) + dot(p2, v2))
        for (seq, blk, slot), (m_i, l_i, p01, p2), pv in zip(items, weights, values):
            row = jnp.minimum(seq, batch)
            m_old = m_s[row]
            m_new = jnp.maximum(m_old, m_i)
            keep = jnp.exp(m_old - m_new)
            add = jnp.exp(m_i - m_new)
            m_s[row] = m_new
            l_s[row] = l_s[row] * keep + l_i * add
            acc_s[row] = acc_s[row] * jnp.concatenate([keep] * 2, axis=1) + pv * jnp.concatenate([add] * 2, axis=1)
        ptr = fetch_group(group, ptr, False)
        return (*ptr, *cur)

    lax.fori_loop(0, n_steps, step, (*ptr, jnp.int32(0), jnp.int32(0)))
    for seq in range(batch):
        m_old, s_new = m_s[seq], new_s[seq]
        m = jnp.maximum(m_old, s_new)
        keep, add = jnp.exp(m_old - m), jnp.exp(s_new - m)
        v_row = v_s[seq:seq + 1, :]
        v_pair = jnp.where(pair_row < 2, v_row[:, 0:pair], jnp.concatenate([v_row[:, pair:width]] * 2, axis=1))
        l = l_s[seq] * keep + add
        acc = acc_s[seq] * jnp.concatenate([keep] * 2, axis=1) + v_pair * jnp.concatenate([add] * 2, axis=1)
        top = jnp.maximum(m[2:3], m[3:4])
        w_a, w_b = jnp.exp(m[2:3] - top), jnp.exp(m[3:4] - top)
        o2 = (acc[2:3, 0:dim] * w_a + acc[3:4, dim:pair] * w_b) / (l[2:3] * w_a + l[3:4] * w_b)
        o_s[seq:seq + 1, :] = jnp.concatenate([acc[0:1, 0:dim] / l[0:1], acc[1:2, dim:pair] / l[1:2], o2], axis=1)
    ld_o.wait()
    part_ref[...] = dot(o_s[...].astype(BF16), wo[...]).astype(BF16)


def rest_kernel(batch, heads, dim, tp, part_ref, x_ref, g2, b2, g3, b3, wqc_h, e_own_h, wk_h, wv_h, wkr_h, wvr_h, woc_h, wup_h, wdn_h,
                out_ref,
                wqc, enc, wkv, wkvr, woc, wup, wdn, kv_own, kv_rem, v_late, recv1, recv, send2, send3,
                qc_s, qc_r, o_snd, o_rcv, o2_snd, o2_rcv, lsem, ssem1, rsem1, ssem, rsem, xs, xr, ns, nr):
    width = heads * dim
    scale = dim ** -0.5
    me = lax.axis_index('tp')
    far = lax.rem(me + 2, tp)
    near = me + 1 - 2 * lax.rem(me, 2)
    half = enc.shape[0] // 2
    early = wvr_h.shape[1]

    def load(i, src, dst):
        copy = pltpu.make_async_copy(src, dst, lsem.at[i])
        copy.start()
        return copy

    ld_e0 = load(0, e_own_h, enc.at[pl.ds(0, half), :])
    ld_wk = load(1, wk_h, wkv.at[:, pl.ds(0, width)])
    ld_wv = load(2, wv_h, wkv.at[:, pl.ds(width, width)])
    ld_wkr = load(3, wkr_h, wkvr.at[:, pl.ds(0, width)])
    ld_wvr = load(4, wvr_h, wkvr.at[:, pl.ds(width, early)])
    ld_wqc = load(5, wqc_h, wqc)
    ld_woc = load(6, woc_h, woc)
    ld_up = load(7, wup_h, wup)
    ld_dn = load(8, wdn_h, wdn)

    barrier = pltpu.get_barrier_semaphore()
    for d in range(1, tp):
        pl.semaphore_signal(barrier, inc=1, device_id={'tp': lax.rem(me + d, tp)}, device_id_type=pl.DeviceIdType.MESH)
    pl.semaphore_wait(barrier, tp - 1)

    def remote(src, dst, send_sem, recv_sem, device):
        return pltpu.make_async_remote_copy(src_ref=src, dst_ref=dst, send_sem=send_sem, recv_sem=recv_sem,
                                            device_id={'tp': device}, device_id_type=pl.DeviceIdType.MESH)

    others = [lax.rem(me + d, tp) for d in (2, 3, 1)]

    def sum_copies(n, src):
        return [remote(src, recv.at[n, me], ssem.at[n, k], rsem.at[n, me], device) for k, device in enumerate(others)]

    def exchange(n, src):
        for copy in sum_copies(n, src):
            copy.start()
        recv[n, me] = src[...]

    def collect(n, src):
        for copy in sum_copies(n, src):
            copy.wait_send()
        for k, device in enumerate(others):
            remote(src, recv.at[n, device], ssem.at[n, k], rsem.at[n, device], device).wait_recv()
        total = recv[n, 0].astype(F32)
        for t in range(1, tp):
            total = total + recv[n, t].astype(F32)
        return total

    def matmul_sum(n, lhs, weights, send):
        size = send.shape[2]
        for k in range(send.shape[0]):
            send[k] = dot(lhs, weights[:, k * size:(k + 1) * size]).astype(BF16)
            exchange(n + k, send.at[k])
        return jnp.concatenate([collect(n + k, send.at[k]) for k in range(send.shape[0])], axis=1)

    def project(first, count, jobs, tile=256):
        def body(i, c):
            rows = pl.ds(pl.multiple_of(i * tile, tile), tile)
            for weights, out, lo, hi in jobs:
                out[rows, lo:hi] = dot(enc[rows, :], weights[:, lo:hi]).astype(BF16)
            return c

        lax.fori_loop(first // tile, (first + count) // tile, body, 0)

    late_rows = (0, 256, 640, wv_h.shape[0])

    def late(i):
        rows, cols = pl.ds(late_rows[i], late_rows[i + 1] - late_rows[i]), width - early
        return remote(wv_h.at[rows, pl.ds(early, cols)], wkvr.at[rows, pl.ds(width + early, cols)], xs.at[3 + i], xr.at[3 + i], far)

    def late_product(i, tile=256):
        lo, hi = late_rows[i], late_rows[i + 1]

        def body(t, c):
            rows = pl.ds(pl.multiple_of(t * tile, tile), tile)
            product = dot(enc[rows, lo:hi], wkvr[lo:hi, width + early:2 * width])
            if i == 0:
                v_late[rows, :] = product
            elif i + 2 < len(late_rows):
                v_late[rows, :] = v_late[rows, :] + product
            else:
                kv_rem[rows, width + early:2 * width] = (v_late[rows, :] + product).astype(BF16)
            return c

        lax.fori_loop(0, 2 * half // tile, body, 0)

    def near_tokens(i):
        rows = half // 2
        return remote(e_own_h.at[pl.ds(i * rows, rows), :], enc.at[pl.ds(half + i * rows, rows), :], ns.at[i], nr.at[i], near)

    own_job = (wkv, kv_own, 0, 2 * width)
    far_job = (wkvr, kv_rem, 0, width + early)

    first_copies = [remote(part_ref, recv1.at[me], ssem1.at[k], rsem1.at[me], device) for k, device in enumerate(others)]
    for copy in first_copies:
        copy.start()
    recv1[me] = part_ref[...]
    near_tokens(0).start()
    near_tokens(1).start()
    late(0).start()
    for copy in (ld_e0, ld_wk, ld_wv, ld_wkr, ld_wvr):
        copy.wait()
    project(0, half, (own_job, far_job))
    for copy in first_copies:
        copy.wait_send()
    for k, device in enumerate(others):
        remote(part_ref, recv1.at[device], ssem1.at[k], rsem1.at[device], device).wait_recv()
    h1 = x_ref[...].astype(F32)
    h1 = h1 + sum((recv1[t].astype(F32) for t in range(1, tp)), recv1[0].astype(F32))
    c_norm = layer_norm(h1, g2[...].reshape(1, -1), b2[...].reshape(1, -1))
    ld_wqc.wait()
    qc_s[...] = dot(c_norm, wqc[...]).astype(BF16)
    send_q = remote(qc_s, qc_r, xs.at[0], xr.at[0], far)
    send_q.start()
    late(1).start()
    late(2).start()
    near_tokens(0).wait()
    near_tokens(1).wait()
    project(half, half, (far_job,))
    late(0).wait()
    late_product(0)

    rows = heads * batch
    row_b = lax.rem(lax.broadcasted_iota(jnp.int32, (rows, 128), 0), batch)
    lane = lax.broadcasted_iota(jnp.int32, (rows, 128), 1)
    per = half // batch
    pack = 128 // per
    blocks = half // 128
    mine = lax.rem(row_b, pack) == lane // per
    row_blk = row_b // pack
    lane_head = lax.broadcasted_iota(jnp.int32, (batch, width), 1) // dim

    def weigh(q, kv):
        qf = q.astype(F32)
        q_rows = jnp.concatenate([jnp.where(lane_head == h, qf, 0.0) for h in range(heads)], axis=0).astype(BF16)
        parts = []
        for part in range(2):
            s_all = dot_t(q_rows, kv[part * half:(part + 1) * half, 0:width])
            s = s_all[:, 0:128]
            for k in range(1, blocks):
                s = jnp.where(row_blk == k, s_all[:, k * 128:(k + 1) * 128], s)
            parts.append(jnp.where(mine, s * scale, NEG))
        m = jnp.maximum(jnp.max(parts[0], axis=1, keepdims=True), jnp.max(parts[1], axis=1, keepdims=True))
        p = [jnp.exp(s - m) for s in parts]
        l = jnp.sum(p[0], axis=1, keepdims=True) + jnp.sum(p[1], axis=1, keepdims=True)
        wide = [jnp.concatenate([jnp.where(row_blk == k, p[part], 0.0) for k in range(blocks)], axis=1).astype(BF16) for part in range(2)]
        return m, l, wide

    def mix(wide, kv, first, last):
        lo, hi = first * batch, last * batch
        o = sum(dot(wide[part][lo:hi], kv[part * half:(part + 1) * half, width + first * dim:width + last * dim]) for part in range(2))
        return jnp.concatenate([o[(h - first) * batch:(h - first + 1) * batch, (h - first) * dim:(h - first + 1) * dim] for h in range(first, last)], axis=0)

    n_early = early // dim
    send_q.wait()
    m_r, l_r, wide_r = weigh(qc_r[...], kv_rem)
    o_snd[0:n_early * batch, :] = mix(wide_r, kv_rem, 0, n_early)
    stats = jnp.zeros((batch, dim), F32)
    st_lane = lax.broadcasted_iota(jnp.int32, (batch, dim), 1)
    for h in range(heads):
        stats = jnp.where(st_lane == 2 * h, m_r[h * batch:(h + 1) * batch], jnp.where(st_lane == 2 * h + 1, l_r[h * batch:(h + 1) * batch], stats))
    o_snd[n_early * batch:(n_early + 1) * batch, :] = stats
    send_o = remote(o_snd, o_rcv, xs.at[1], xr.at[1], far)
    send_o.start()
    for i in (1, 2):
        late(i).wait()
        late_product(i)
    o2_snd[...] = mix(wide_r, kv_rem, n_early, heads)
    send_o2 = remote(o2_snd, o2_rcv, xs.at[2], xr.at[2], far)
    send_o2.start()
    project(half, half, (own_job,))
    m_a, l_a, wide_a = weigh(qc_s[...], kv_own)
    o_a = mix(wide_a, kv_own, 0, heads)
    send_o.wait()
    stats = o_rcv[n_early * batch:(n_early + 1) * batch, :]
    m_b = jnp.concatenate([stats[:, 2 * h:2 * h + 1] for h in range(heads)], axis=0)
    l_b = jnp.concatenate([stats[:, 2 * h + 1:2 * h + 2] for h in range(heads)], axis=0)
    m = jnp.maximum(m_a, m_b)
    w_a, w_b = jnp.exp(m_a - m), jnp.exp(m_b - m)
    send_o2.wait()
    o_b = jnp.concatenate([o_rcv[0:n_early * batch, :], o2_rcv[...]], axis=0)
    o = (o_a * w_a + o_b * w_b) / (l_a * w_a + l_b * w_b)
    oc = jnp.concatenate([o[h * batch:(h + 1) * batch, :] for h in range(heads)], axis=1).astype(BF16)

    ld_woc.wait()
    h2 = h1 + matmul_sum(0, oc, woc, send2)
    m_norm = layer_norm(h2, g3[...].reshape(1, -1), b3[...].reshape(1, -1))
    ld_up.wait()
    up = dot(m_norm, wup[...])
    hidden = (0.5 * up * (1.0 + lax.erf(up * (0.5 ** 0.5)))).astype(BF16)
    ld_dn.wait()
    out_ref[...] = h2 + matmul_sum(send2.shape[0], hidden, wdn, send3)


def local_step(x, k_cache, v_cache, seq_lens, nbr_enc, ln1_gain, ln1_bias, w_q, w_k, w_v, w_o, ln2_gain, ln2_bias, wq_c, wk_c, wv_c, wo_c, ln3_gain, ln3_bias, w_up, w_down):
    batch, d_model = x.shape
    heads, dim = k_cache.shape[2:]
    width = heads * dim
    tp = lax.axis_size('tp')
    far = [(i, (i + 2) % tp) for i in range(tp)]
    enc = nbr_enc.reshape(-1, nbr_enc.shape[-1])
    wk_far = lax.ppermute(wk_c, 'tp', far)
    wv_cut = wv_c[:, :2 * dim]
    wv_far = lax.ppermute(wv_cut, 'tp', far)

    any_spec = pl.BlockSpec(memory_space=pl.ANY)
    hbm = pl.BlockSpec(memory_space=pltpu.HBM)
    vmem = pl.BlockSpec(memory_space=pltpu.VMEM)
    slots = GROUPS * UNROLL
    part, k_new, v_new = pl.pallas_call(
        functools.partial(self_kernel, batch, heads, dim),
        out_shape=(jax.ShapeDtypeStruct((batch, d_model), BF16), jax.ShapeDtypeStruct((heads, batch, dim), BF16), jax.ShapeDtypeStruct((heads, batch, dim), BF16)),
        in_specs=[hbm] * 10,
        out_specs=(vmem, vmem, vmem),
        scratch_shapes=[
            pltpu.SMEM((batch,), jnp.int32), pltpu.VMEM((batch, d_model), BF16), pltpu.VMEM((d_model,), F32), pltpu.VMEM((d_model,), F32),
            pltpu.VMEM((d_model, width), BF16), pltpu.VMEM((d_model, width), BF16), pltpu.VMEM((d_model, width), BF16), pltpu.VMEM((width, d_model), BF16),
            pltpu.VMEM((slots, heads, CHUNK, dim), BF16), pltpu.VMEM((slots, heads, CHUNK, dim), BF16),
            pltpu.VMEM((batch + 8, width), F32), pltpu.VMEM((batch, width), F32), pltpu.VMEM((batch, width), F32),
            pltpu.VMEM((batch + 1, 8, dim), F32), pltpu.VMEM((batch + 1, 8, dim), F32), pltpu.VMEM((batch + 1, 8, 2 * dim), F32), pltpu.VMEM((batch, 8, dim), F32),
            pltpu.SemaphoreType.DMA((8,)), pltpu.SemaphoreType.DMA((slots,)), pltpu.SemaphoreType.DMA((slots,)),
        ],
        compiler_params=pltpu.CompilerParams(vmem_limit_bytes=46000000),
        cost_estimate=pl.CostEstimate(flops=40_000_000_000, bytes_accessed=60_000_000, transcendentals=0),
        name='self_attention',
    )(*in_hbm(seq_lens, x, ln1_gain, ln1_bias, jnp.transpose(k_cache, (0, 2, 1, 3)), jnp.transpose(v_cache, (0, 2, 1, 3)), w_q, w_k, w_v, w_o))

    n_enc, enc_dim = enc.shape
    ff = w_up.shape[1]
    out = pl.pallas_call(
        functools.partial(rest_kernel, batch, heads, dim, tp),
        out_shape=jax.ShapeDtypeStruct((batch, d_model), F32),
        in_specs=[vmem] * 6 + [hbm] * 4 + [any_spec] * 2 + [hbm] * 3,
        out_specs=vmem,
        scratch_shapes=[
            pltpu.VMEM((d_model, width), BF16), pltpu.VMEM((2 * n_enc, enc_dim), BF16),
            pltpu.VMEM((enc_dim, 2 * width), BF16), pltpu.VMEM((enc_dim, 2 * width), BF16),
            pltpu.VMEM((width, d_model), BF16), pltpu.VMEM((d_model, ff), BF16), pltpu.VMEM((ff, d_model), BF16),
            pltpu.VMEM((2 * n_enc, 2 * width), BF16), pltpu.VMEM((2 * n_enc, 2 * width), BF16), pltpu.VMEM((2 * n_enc, dim), F32),
            pltpu.VMEM((tp, batch, d_model), BF16), pltpu.VMEM((2 * PIECES, tp, batch, d_model // PIECES), BF16),
            pltpu.VMEM((PIECES, batch, d_model // PIECES), BF16), pltpu.VMEM((PIECES, batch, d_model // PIECES), BF16),
            pltpu.VMEM((batch, width), BF16), pltpu.VMEM((batch, width), BF16),
            pltpu.VMEM((heads * batch, dim), F32), pltpu.VMEM((heads * batch, dim), F32), pltpu.VMEM((batch, dim), F32), pltpu.VMEM((batch, dim), F32),
            pltpu.SemaphoreType.DMA((9,)), pltpu.SemaphoreType.DMA((tp - 1,)), pltpu.SemaphoreType.DMA((tp,)),
            pltpu.SemaphoreType.DMA((2 * PIECES, tp - 1)), pltpu.SemaphoreType.DMA((2 * PIECES, tp)),
            pltpu.SemaphoreType.DMA((6,)), pltpu.SemaphoreType.DMA((6,)), pltpu.SemaphoreType.DMA((2,)), pltpu.SemaphoreType.DMA((2,)),
        ],
        compiler_params=pltpu.CompilerParams(collective_id=0, has_side_effects=True, vmem_limit_bytes=46000000),
        cost_estimate=pl.CostEstimate(flops=20_000_000_000, bytes_accessed=30_000_000, transcendentals=0),
        name='rest_of_layer',
    )(part, x, ln2_gain, ln2_bias, ln3_gain, ln3_bias, *in_hbm(wq_c, enc, wk_c, wv_c), wk_far, wv_far, *in_hbm(wo_c, w_up, w_down))
    return out.astype(BF16), jnp.transpose(k_new, (1, 0, 2)), jnp.transpose(v_new, (1, 0, 2))


def solution(mesh):
    row_spec = P('dp', None)
    cache_spec = P('dp', None, 'tp', None)
    head_spec = P('dp', 'tp', None)
    vec_spec = P(None)
    col_split = P(None, 'tp')
    row_split = P('tp', None)
    in_specs = (row_spec, cache_spec, cache_spec, P('dp'), P('dp', 'tp', None), vec_spec, vec_spec, col_split, col_split, col_split, row_split, vec_spec, vec_spec, col_split, col_split, col_split, row_split, vec_spec, vec_spec, col_split, row_split)
    out_specs = (row_spec, head_spec, head_spec)
    return jax.shard_map(local_step, mesh=mesh, in_specs=in_specs, out_specs=out_specs, check_vma=False)
```

```python
import functools

import jax
import jax.numpy as jnp
from jax import lax
from jax.experimental import pallas as pl
from jax.experimental.pallas import tpu as pltpu
from jax.sharding import PartitionSpec as P


LN_EPS = 1e-5
NEG = -1e30
F32 = jnp.float32
BF16 = jnp.bfloat16
CHUNK = 512
UNROLL = 4
GRAIN = 64
GROUPS = 6


def layer_norm(values, ln_gain, ln_bias):
    row_mean = jnp.mean(values, axis=-1, keepdims=True)
    centred = values - row_mean
    row_var = jnp.mean(jnp.square(centred), axis=-1, keepdims=True)
    return (centred * lax.rsqrt(row_var + LN_EPS) * ln_gain + ln_bias).astype(BF16)


def dot(lhs, rhs):
    return jnp.dot(lhs, rhs, preferred_element_type=F32)


def dot_t(lhs, rhs):
    return lax.dot_general(lhs, rhs, (((1,), (1,)), ((), ())), preferred_element_type=F32)


def in_hbm(*arrays):
    return [pltpu.with_memory_space_constraint(a, pltpu.HBM) for a in arrays]


def self_kernel(batch, heads, dim, lens_h, x_h, g_h, b_h, kc, vc, wq_h, wk_h, wv_h, wo_h,
                part_ref, knew_ref, vnew_ref,
                lens, x_v, g_v, b_v, wq, wk, wv, wo, kbuf, vbuf, q_s, v_s, o_s, m_s, l_s, acc_s, new_s, wsem, ksem, vsem):
    width = heads * dim
    scale = dim ** -0.5
    pairs = ((x_h, x_v), (g_h, g_v), (b_h, b_v), (wq_h, wq), (lens_h, lens), (wk_h, wk), (wv_h, wv), (wo_h, wo))
    ld_x, ld_g, ld_b, ld_q, ld_len, ld_k, ld_v, ld_o = [pltpu.make_async_copy(src, dst, wsem.at[i]) for i, (src, dst) in enumerate(pairs)]
    for copy in (ld_len, ld_x, ld_g, ld_b, ld_q, ld_k, ld_v):
        copy.start()

    def len_of(seq):
        return jnp.where(seq < batch, lens[jnp.minimum(seq, batch - 1)], 0)

    def following(seq, blk):
        more = (blk + 1) * CHUNK < len_of(seq)
        return jnp.where(more, seq, seq + 1), jnp.where(more, blk + 1, 0)

    def copies(seq, blk, slot, whole):
        live = pl.multiple_of(jnp.minimum(len_of(seq) - blk * CHUNK, CHUNK), GRAIN)
        first = pl.multiple_of(blk * CHUNK, CHUNK)
        count = CHUNK if whole else live
        src, dst = pl.ds(first, count), pl.ds(0, count)
        return (pltpu.make_async_copy(kc.at[seq, :, src, :], kbuf.at[slot, :, dst, :], ksem.at[slot]),
                pltpu.make_async_copy(vc.at[seq, :, src, :], vbuf.at[slot, :, dst, :], vsem.at[slot]))

    def fetch_group(group, ptr, whole):
        for u in range(UNROLL):
            seq, blk = ptr

            @pl.when(seq < batch)
            def _():
                for copy in copies(seq, blk, group * UNROLL + u, whole):
                    copy.start()

            ptr = following(seq, blk)
        return ptr

    ld_len.wait()
    ptr = (jnp.int32(0), jnp.int32(0))
    for group in range(GROUPS):
        ptr = fetch_group(group, ptr, True)
    ld_o.start()

    n_items = jnp.int32(0)
    for seq in range(batch):
        n_items = n_items + lax.div(lens[seq] + (CHUNK - 1), CHUNK)
    n_steps = lax.div(n_items + (UNROLL - 1), UNROLL)

    for copy in (ld_x, ld_g, ld_b):
        copy.wait()
    a_norm = layer_norm(x_v[...].astype(F32), g_v[...].reshape(1, -1), b_v[...].reshape(1, -1))
    ld_q.wait()
    q_s[0:batch, :] = dot(a_norm, wq[...]).astype(BF16).astype(F32)
    q_s[batch:, :] = jnp.zeros((q_s.shape[0] - batch, width), F32)
    m_s[...] = jnp.full(m_s.shape, NEG, F32)
    l_s[...] = jnp.zeros_like(l_s)
    acc_s[...] = jnp.zeros_like(acc_s)

    pair = 2 * dim
    part_rows = CHUNK // 2
    row8 = lax.broadcasted_iota(jnp.int32, (8, 1), 0)
    pair_row = lax.broadcasted_iota(jnp.int32, (8, pair), 0)
    pair_side = lax.broadcasted_iota(jnp.int32, (8, pair), 1) // dim
    sel01 = (pair_row == pair_side).astype(F32)
    sel2 = (pair_row == pair_side + 2).astype(F32)
    lane = lax.broadcasted_iota(jnp.int32, (8, CHUNK), 1)
    lane2 = lax.broadcasted_iota(jnp.int32, (8, part_rows), 1)

    def new_token():
        ld_k.wait()
        k_new = dot(a_norm, wk[...]).astype(BF16)
        ld_v.wait()
        v_new = dot(a_norm, wv[...]).astype(BF16)
        for h in range(heads):
            knew_ref[h] = k_new[:, h * dim:(h + 1) * dim]
            vnew_ref[h] = v_new[:, h * dim:(h + 1) * dim]
        qk = q_s[0:batch, :] * k_new.astype(F32)
        v_s[...] = v_new.astype(F32)
        for seq in range(batch):
            prod = qk[seq:seq + 1, :]
            tail = jnp.concatenate([prod[:, pair:width], jnp.zeros((1, pair - dim), F32)], axis=1)
            s_new = jnp.sum(prod[:, 0:pair] * sel01 + tail * sel2, axis=1, keepdims=True) * scale
            new_s[seq] = jnp.broadcast_to(jnp.where(row8 == 3, NEG, s_new), (8, dim))

    def step(i, carry):
        ptr, cur = carry[:2], carry[2:]
        group = lax.rem(i, GROUPS)

        @pl.when(i == 1)
        def _():
            new_token()

        items = []
        for u in range(UNROLL):
            items.append((*cur, group * UNROLL + u))
            cur = following(*cur)
        for seq, blk, slot in items:

            @pl.when((seq < batch) & (i < GROUPS))
            def _():
                for copy in copies(seq, blk, slot, True):
                    copy.wait()

            @pl.when((seq < batch) & (i >= GROUPS))
            def _():
                for copy in copies(seq, blk, slot, False):
                    copy.wait()
        scores = []
        for seq, blk, slot in items:
            q_row = q_s[pl.ds(jnp.minimum(seq, batch), 1), :]
            q01 = (q_row[:, 0:pair] * sel01).astype(BF16)
            q2 = (jnp.concatenate([q_row[:, pair:width]] * 2, axis=1) * sel2).astype(BF16)
            k01 = jnp.concatenate([kbuf[slot, 0], kbuf[slot, 1]], axis=1)
            k2 = jnp.concatenate([kbuf[slot, 2, 0:part_rows, :], kbuf[slot, 2, part_rows:CHUNK, :]], axis=1)
            scores.append((dot_t(q01, k01), dot_t(q2, k2)))
        weights = []
        for (seq, blk, slot), (s01, s2) in zip(items, scores):
            live = len_of(seq) - blk * CHUNK
            s01 = jnp.where(lane < jnp.where(row8 < 2, live, 0), s01 * scale, NEG)
            s2 = jnp.where(lane2 < jnp.where(row8 == 2, live, jnp.where(row8 == 3, live - part_rows, 0)), s2 * scale, NEG)
            m_i = jnp.maximum(jnp.max(s01, axis=1, keepdims=True), jnp.max(s2, axis=1, keepdims=True))
            p01 = jnp.where(row8 < 2, jnp.exp(s01 - m_i), 0.0)
            p2 = jnp.where(row8 < 2, 0.0, jnp.exp(s2 - m_i))
            l_i = jnp.sum(p01, axis=1, keepdims=True) + jnp.sum(p2, axis=1, keepdims=True)
            weights.append((m_i, l_i, p01.astype(BF16), p2.astype(BF16)))
        values = []
        for (seq, blk, slot), (m_i, l_i, p01, p2) in zip(items, weights):
            v01 = jnp.concatenate([vbuf[slot, 0], vbuf[slot, 1]], axis=1)
            v2 = jnp.concatenate([vbuf[slot, 2, 0:part_rows, :], vbuf[slot, 2, part_rows:CHUNK, :]], axis=1)
            values.append(dot(p01, v01) + dot(p2, v2))
        for (seq, blk, slot), (m_i, l_i, p01, p2), pv in zip(items, weights, values):
            row = jnp.minimum(seq, batch)
            m_old = m_s[row]
            m_new = jnp.maximum(m_old, m_i)
            keep = jnp.exp(m_old - m_new)
            add = jnp.exp(m_i - m_new)
            m_s[row] = m_new
            l_s[row] = l_s[row] * keep + l_i * add
            acc_s[row] = acc_s[row] * jnp.concatenate([keep] * 2, axis=1) + pv * jnp.concatenate([add] * 2, axis=1)
        ptr = fetch_group(group, ptr, False)
        return (*ptr, *cur)

    lax.fori_loop(0, n_steps, step, (*ptr, jnp.int32(0), jnp.int32(0)))
    for seq in range(batch):
        m_old, s_new = m_s[seq], new_s[seq]
        m = jnp.maximum(m_old, s_new)
        keep, add = jnp.exp(m_old - m), jnp.exp(s_new - m)
        v_row = v_s[seq:seq + 1, :]
        v_pair = jnp.where(pair_row < 2, v_row[:, 0:pair], jnp.concatenate([v_row[:, pair:width]] * 2, axis=1))
        l = l_s[seq] * keep + add
        acc = acc_s[seq] * jnp.concatenate([keep] * 2, axis=1) + v_pair * jnp.concatenate([add] * 2, axis=1)
        top = jnp.maximum(m[2:3], m[3:4])
        w_a, w_b = jnp.exp(m[2:3] - top), jnp.exp(m[3:4] - top)
        o2 = (acc[2:3, 0:dim] * w_a + acc[3:4, dim:pair] * w_b) / (l[2:3] * w_a + l[3:4] * w_b)
        o_s[seq:seq + 1, :] = jnp.concatenate([acc[0:1, 0:dim] / l[0:1], acc[1:2, dim:pair] / l[1:2], o2], axis=1)
    ld_o.wait()
    part_ref[...] = dot(o_s[...].astype(BF16), wo[...]).astype(BF16)


def rest_kernel(batch, heads, dim, tp, part_ref, x_ref, g2, b2, g3, b3, wqc_h, e_own_h, wk_h, wv_h, wkr_h, wvr_h, woc_h, wup_h, wdn_h,
                out_ref,
                wqc, enc, wkv, wkvr, woc, wup, wdn, kv_own, kv_rem, v_late, far_in, both, near_in, send2, send3,
                qc_s, qc_r, o_snd, o_rcv, o2_snd, o2_rcv, lsem, ssem, rsem, xs, xr, ns, nr):
    width = heads * dim
    scale = dim ** -0.5
    me = lax.axis_index('tp')
    far = lax.rem(me + 2, tp)
    near = me + 1 - 2 * lax.rem(me, 2)
    half = enc.shape[0] // 2
    early = wvr_h.shape[1]

    def load(i, src, dst):
        copy = pltpu.make_async_copy(src, dst, lsem.at[i])
        copy.start()
        return copy

    ld_e0 = load(0, e_own_h, enc.at[pl.ds(0, half), :])
    ld_wk = load(1, wk_h, wkv.at[:, pl.ds(0, width)])
    ld_wv = load(2, wv_h, wkv.at[:, pl.ds(width, width)])
    ld_wkr = load(3, wkr_h, wkvr.at[:, pl.ds(0, width)])
    ld_wvr = load(4, wvr_h, wkvr.at[:, pl.ds(width, early)])
    ld_wqc = load(5, wqc_h, wqc)
    ld_woc = load(6, woc_h, woc)
    ld_up = load(7, wup_h, wup)
    ld_dn = load(8, wdn_h, wdn)

    barrier = pltpu.get_barrier_semaphore()
    for d in range(1, tp):
        pl.semaphore_signal(barrier, inc=1, device_id={'tp': lax.rem(me + d, tp)}, device_id_type=pl.DeviceIdType.MESH)
    pl.semaphore_wait(barrier, tp - 1)

    def remote(src, dst, send_sem, recv_sem, device):
        return pltpu.make_async_remote_copy(src_ref=src, dst_ref=dst, send_sem=send_sem, recv_sem=recv_sem,
                                            device_id={'tp': device}, device_id_type=pl.DeviceIdType.MESH)

    def far_copy(n, src):
        return remote(src, far_in.at[n], ssem.at[n, 0], rsem.at[n, 0], far)

    def near_copy(n):
        return remote(both.at[n], near_in.at[n], ssem.at[n, 1], rsem.at[n, 1], near)

    def pass_on(n, src):
        far_copy(n, src).wait()
        both[n] = (src[...].astype(F32) + far_in[n].astype(F32)).astype(BF16)
        near_copy(n).start()

    def total(n):
        near_copy(n).wait()
        return both[n].astype(F32) + near_in[n].astype(F32)

    def project(first, count, jobs, tile=256):
        def body(i, c):
            rows = pl.ds(pl.multiple_of(i * tile, tile), tile)
            for weights, out, lo, hi in jobs:
                out[rows, lo:hi] = dot(enc[rows, :], weights[:, lo:hi]).astype(BF16)
            return c

        lax.fori_loop(first // tile, (first + count) // tile, body, 0)

    late_rows = (0, 512, wv_h.shape[0])

    def late(i):
        rows, cols = pl.ds(late_rows[i], late_rows[i + 1] - late_rows[i]), width - early
        return remote(wv_h.at[rows, pl.ds(early, cols)], wkvr.at[rows, pl.ds(width + early, cols)], xs.at[3 + i], xr.at[3 + i], far)

    def late_product(i, tile=256):
        lo, hi = late_rows[i], late_rows[i + 1]

        def body(t, c):
            rows = pl.ds(pl.multiple_of(t * tile, tile), tile)
            product = dot(enc[rows, lo:hi], wkvr[lo:hi, width + early:2 * width])
            if i == 0:
                v_late[rows, :] = product
            else:
                kv_rem[rows, width + early:2 * width] = (v_late[rows, :] + product).astype(BF16)
            return c

        lax.fori_loop(0, 2 * half // tile, body, 0)

    def near_tokens(i):
        rows = half // 2
        return remote(e_own_h.at[pl.ds(i * rows, rows), :], enc.at[pl.ds(half + i * rows, rows), :], ns.at[i], nr.at[i], near)

    own_job = (wkv, kv_own, 0, 2 * width)
    far_job = (wkvr, kv_rem, 0, width + early)

    far_copy(0, part_ref).start()
    near_tokens(0).start()
    near_tokens(1).start()
    late(0).start()
    for copy in (ld_e0, ld_wk, ld_wv, ld_wkr, ld_wvr):
        copy.wait()
    before = half * 3 // 4
    project(0, before, (own_job, far_job))
    pass_on(0, part_ref)
    project(before, half - before, (own_job, far_job))
    h1 = x_ref[...].astype(F32) + total(0)
    c_norm = layer_norm(h1, g2[...].reshape(1, -1), b2[...].reshape(1, -1))
    ld_wqc.wait()
    qc_s[...] = dot(c_norm, wqc[...]).astype(BF16)
    send_q = remote(qc_s, qc_r, xs.at[0], xr.at[0], far)
    send_q.start()
    late(1).start()
    near_tokens(0).wait()
    near_tokens(1).wait()
    project(half, half, (far_job,))
    late(0).wait()
    late_product(0)

    rows = heads * batch
    row_b = lax.rem(lax.broadcasted_iota(jnp.int32, (rows, 128), 0), batch)
    lane = lax.broadcasted_iota(jnp.int32, (rows, 128), 1)
    per = half // batch
    pack = 128 // per
    blocks = half // 128
    mine = lax.rem(row_b, pack) == lane // per
    row_blk = row_b // pack
    lane_head = lax.broadcasted_iota(jnp.int32, (batch, width), 1) // dim

    def weigh(q, kv):
        qf = q.astype(F32)
        q_rows = jnp.concatenate([jnp.where(lane_head == h, qf, 0.0) for h in range(heads)], axis=0).astype(BF16)
        parts = []
        for part in range(2):
            s_all = dot_t(q_rows, kv[part * half:(part + 1) * half, 0:width])
            s = s_all[:, 0:128]
            for k in range(1, blocks):
                s = jnp.where(row_blk == k, s_all[:, k * 128:(k + 1) * 128], s)
            parts.append(jnp.where(mine, s * scale, NEG))
        m = jnp.maximum(jnp.max(parts[0], axis=1, keepdims=True), jnp.max(parts[1], axis=1, keepdims=True))
        p = [jnp.exp(s - m) for s in parts]
        l = jnp.sum(p[0], axis=1, keepdims=True) + jnp.sum(p[1], axis=1, keepdims=True)
        wide = [jnp.concatenate([jnp.where(row_blk == k, p[part], 0.0) for k in range(blocks)], axis=1).astype(BF16) for part in range(2)]
        return m, l, wide

    def mix(wide, kv, first, last):
        lo, hi = first * batch, last * batch
        o = sum(dot(wide[part][lo:hi], kv[part * half:(part + 1) * half, width + first * dim:width + last * dim]) for part in range(2))
        return jnp.concatenate([o[(h - first) * batch:(h - first + 1) * batch, (h - first) * dim:(h - first + 1) * dim] for h in range(first, last)], axis=0)

    n_early = early // dim
    send_q.wait()
    m_r, l_r, wide_r = weigh(qc_r[...], kv_rem)
    o_snd[0:n_early * batch, :] = mix(wide_r, kv_rem, 0, n_early)
    stats = jnp.zeros((batch, dim), F32)
    st_lane = lax.broadcasted_iota(jnp.int32, (batch, dim), 1)
    for h in range(heads):
        stats = jnp.where(st_lane == 2 * h, m_r[h * batch:(h + 1) * batch], jnp.where(st_lane == 2 * h + 1, l_r[h * batch:(h + 1) * batch], stats))
    o_snd[n_early * batch:(n_early + 1) * batch, :] = stats
    send_o = remote(o_snd, o_rcv, xs.at[1], xr.at[1], far)
    send_o.start()
    late(1).wait()
    late_product(1)
    o2_snd[...] = mix(wide_r, kv_rem, n_early, heads)
    send_o2 = remote(o2_snd, o2_rcv, xs.at[2], xr.at[2], far)
    send_o2.start()
    project(half, half, (own_job,))
    m_a, l_a, wide_a = weigh(qc_s[...], kv_own)
    o_a = mix(wide_a, kv_own, 0, heads)
    send_o.wait()
    stats = o_rcv[n_early * batch:(n_early + 1) * batch, :]
    m_b = jnp.concatenate([stats[:, 2 * h:2 * h + 1] for h in range(heads)], axis=0)
    l_b = jnp.concatenate([stats[:, 2 * h + 1:2 * h + 2] for h in range(heads)], axis=0)
    m = jnp.maximum(m_a, m_b)
    w_a, w_b = jnp.exp(m_a - m), jnp.exp(m_b - m)
    send_o2.wait()
    o_b = jnp.concatenate([o_rcv[0:n_early * batch, :], o2_rcv[...]], axis=0)
    o = (o_a * w_a + o_b * w_b) / (l_a * w_a + l_b * w_b)
    oc = jnp.concatenate([o[h * batch:(h + 1) * batch, :] for h in range(heads)], axis=1).astype(BF16)

    def matmul_sum(n, lhs, weights, out):
        out[...] = dot(lhs, weights[...]).astype(BF16)
        far_copy(n, out).start()
        pass_on(n, out)
        return total(n)

    ld_woc.wait()
    h2 = h1 + matmul_sum(1, oc, woc, send2)
    m_norm = layer_norm(h2, g3[...].reshape(1, -1), b3[...].reshape(1, -1))
    ld_up.wait()
    up = dot(m_norm, wup[...])
    hidden = (0.5 * up * (1.0 + lax.erf(up * (0.5 ** 0.5)))).astype(BF16)
    ld_dn.wait()
    out_ref[...] = h2 + matmul_sum(2, hidden, wdn, send3)


def local_step(x, k_cache, v_cache, seq_lens, nbr_enc, ln1_gain, ln1_bias, w_q, w_k, w_v, w_o, ln2_gain, ln2_bias, wq_c, wk_c, wv_c, wo_c, ln3_gain, ln3_bias, w_up, w_down):
    batch, d_model = x.shape
    heads, dim = k_cache.shape[2:]
    width = heads * dim
    tp = lax.axis_size('tp')
    far = [(i, (i + 2) % tp) for i in range(tp)]
    enc = nbr_enc.reshape(-1, nbr_enc.shape[-1])
    wk_far = lax.ppermute(wk_c, 'tp', far)
    wv_cut = wv_c[:, :2 * dim]
    wv_far = lax.ppermute(wv_cut, 'tp', far)

    any_spec = pl.BlockSpec(memory_space=pl.ANY)
    hbm = pl.BlockSpec(memory_space=pltpu.HBM)
    vmem = pl.BlockSpec(memory_space=pltpu.VMEM)
    slots = GROUPS * UNROLL
    part, k_new, v_new = pl.pallas_call(
        functools.partial(self_kernel, batch, heads, dim),
        out_shape=(jax.ShapeDtypeStruct((batch, d_model), BF16), jax.ShapeDtypeStruct((heads, batch, dim), BF16), jax.ShapeDtypeStruct((heads, batch, dim), BF16)),
        in_specs=[hbm] * 10,
        out_specs=(vmem, vmem, vmem),
        scratch_shapes=[
            pltpu.SMEM((batch,), jnp.int32), pltpu.VMEM((batch, d_model), BF16), pltpu.VMEM((d_model,), F32), pltpu.VMEM((d_model,), F32),
            pltpu.VMEM((d_model, width), BF16), pltpu.VMEM((d_model, width), BF16), pltpu.VMEM((d_model, width), BF16), pltpu.VMEM((width, d_model), BF16),
            pltpu.VMEM((slots, heads, CHUNK, dim), BF16), pltpu.VMEM((slots, heads, CHUNK, dim), BF16),
            pltpu.VMEM((batch + 8, width), F32), pltpu.VMEM((batch, width), F32), pltpu.VMEM((batch, width), F32),
            pltpu.VMEM((batch + 1, 8, dim), F32), pltpu.VMEM((batch + 1, 8, dim), F32), pltpu.VMEM((batch + 1, 8, 2 * dim), F32), pltpu.VMEM((batch, 8, dim), F32),
            pltpu.SemaphoreType.DMA((8,)), pltpu.SemaphoreType.DMA((slots,)), pltpu.SemaphoreType.DMA((slots,)),
        ],
        compiler_params=pltpu.CompilerParams(vmem_limit_bytes=46000000),
        cost_estimate=pl.CostEstimate(flops=40_000_000_000, bytes_accessed=60_000_000, transcendentals=0),
        name='self_attention',
    )(*in_hbm(seq_lens, x, ln1_gain, ln1_bias, jnp.transpose(k_cache, (0, 2, 1, 3)), jnp.transpose(v_cache, (0, 2, 1, 3)), w_q, w_k, w_v, w_o))

    n_enc, enc_dim = enc.shape
    ff = w_up.shape[1]
    out = pl.pallas_call(
        functools.partial(rest_kernel, batch, heads, dim, tp),
        out_shape=jax.ShapeDtypeStruct((batch, d_model), F32),
        in_specs=[vmem] * 6 + [hbm] * 4 + [any_spec] * 2 + [hbm] * 3,
        out_specs=vmem,
        scratch_shapes=[
            pltpu.VMEM((d_model, width), BF16), pltpu.VMEM((2 * n_enc, enc_dim), BF16),
            pltpu.VMEM((enc_dim, 2 * width), BF16), pltpu.VMEM((enc_dim, 2 * width), BF16),
            pltpu.VMEM((width, d_model), BF16), pltpu.VMEM((d_model, ff), BF16), pltpu.VMEM((ff, d_model), BF16),
            pltpu.VMEM((2 * n_enc, 2 * width), BF16), pltpu.VMEM((2 * n_enc, 2 * width), BF16), pltpu.VMEM((2 * n_enc, dim), F32),
            pltpu.VMEM((3, batch, d_model), BF16), pltpu.VMEM((3, batch, d_model), BF16), pltpu.VMEM((3, batch, d_model), BF16),
            pltpu.VMEM((batch, d_model), BF16), pltpu.VMEM((batch, d_model), BF16),
            pltpu.VMEM((batch, width), BF16), pltpu.VMEM((batch, width), BF16),
            pltpu.VMEM((heads * batch, dim), F32), pltpu.VMEM((heads * batch, dim), F32), pltpu.VMEM((batch, dim), F32), pltpu.VMEM((batch, dim), F32),
            pltpu.SemaphoreType.DMA((9,)), pltpu.SemaphoreType.DMA((3, 2)), pltpu.SemaphoreType.DMA((3, 2)),
            pltpu.SemaphoreType.DMA((5,)), pltpu.SemaphoreType.DMA((5,)), pltpu.SemaphoreType.DMA((2,)), pltpu.SemaphoreType.DMA((2,)),
        ],
        compiler_params=pltpu.CompilerParams(collective_id=0, has_side_effects=True, vmem_limit_bytes=46000000),
        cost_estimate=pl.CostEstimate(flops=20_000_000_000, bytes_accessed=30_000_000, transcendentals=0),
        name='rest_of_layer',
    )(part, x, ln2_gain, ln2_bias, ln3_gain, ln3_bias, *in_hbm(wq_c, enc, wk_c, wv_c), wk_far, wv_far, *in_hbm(wo_c, w_up, w_down))
    return out.astype(BF16), jnp.transpose(k_new, (1, 0, 2)), jnp.transpose(v_new, (1, 0, 2))


def solution(mesh):
    row_spec = P('dp', None)
    cache_spec = P('dp', None, 'tp', None)
    head_spec = P('dp', 'tp', None)
    vec_spec = P(None)
    col_split = P(None, 'tp')
    row_split = P('tp', None)
    in_specs = (row_spec, cache_spec, cache_spec, P('dp'), P('dp', 'tp', None), vec_spec, vec_spec, col_split, col_split, col_split, row_split, vec_spec, vec_spec, col_split, col_split, col_split, row_split, vec_spec, vec_spec, col_split, row_split)
    out_specs = (row_spec, head_spec, head_spec)
    return jax.shard_map(local_step, mesh=mesh, in_specs=in_specs, out_specs=out_specs, check_vma=False)
```

```python
import functools

import jax
import jax.numpy as jnp
from jax import lax
from jax.experimental import pallas as pl
from jax.experimental.pallas import tpu as pltpu
from jax.sharding import PartitionSpec as P


LN_EPS = 1e-5
NEG = -1e30
F32 = jnp.float32
BF16 = jnp.bfloat16
CHUNK = 512
UNROLL = 4
GRAIN = 64
GROUPS = 6


def layer_norm(values, ln_gain, ln_bias):
    row_mean = jnp.mean(values, axis=-1, keepdims=True)
    centred = values - row_mean
    row_var = jnp.mean(jnp.square(centred), axis=-1, keepdims=True)
    return (centred * lax.rsqrt(row_var + LN_EPS) * ln_gain + ln_bias).astype(BF16)


def dot(lhs, rhs):
    return jnp.dot(lhs, rhs, preferred_element_type=F32)


def dot_t(lhs, rhs):
    return lax.dot_general(lhs, rhs, (((1,), (1,)), ((), ())), preferred_element_type=F32)


def in_hbm(*arrays):
    return [pltpu.with_memory_space_constraint(a, pltpu.HBM) for a in arrays]


def self_kernel(batch, heads, dim, lens_h, x_h, g_h, b_h, kc, vc, wq_h, wk_h, wv_h, wo_h,
                part_ref, knew_ref, vnew_ref,
                lens, x_v, g_v, b_v, wq, wk, wv, wo, kbuf, vbuf, q_s, v_s, o_s, m_s, l_s, acc_s, new_s, wsem, ksem, vsem):
    width = heads * dim
    scale = dim ** -0.5
    pairs = ((x_h, x_v), (g_h, g_v), (b_h, b_v), (wq_h, wq), (lens_h, lens), (wk_h, wk), (wv_h, wv), (wo_h, wo))
    ld_x, ld_g, ld_b, ld_q, ld_len, ld_k, ld_v, ld_o = [pltpu.make_async_copy(src, dst, wsem.at[i]) for i, (src, dst) in enumerate(pairs)]
    for copy in (ld_len, ld_x, ld_g, ld_b, ld_q, ld_k, ld_v):
        copy.start()

    def len_of(seq):
        return jnp.where(seq < batch, lens[jnp.minimum(seq, batch - 1)], 0)

    def following(seq, blk):
        more = (blk + 1) * CHUNK < len_of(seq)
        return jnp.where(more, seq, seq + 1), jnp.where(more, blk + 1, 0)

    def copies(seq, blk, slot, whole):
        live = pl.multiple_of(jnp.minimum(len_of(seq) - blk * CHUNK, CHUNK), GRAIN)
        first = pl.multiple_of(blk * CHUNK, CHUNK)
        count = CHUNK if whole else live
        src, dst = pl.ds(first, count), pl.ds(0, count)
        return (pltpu.make_async_copy(kc.at[seq, :, src, :], kbuf.at[slot, :, dst, :], ksem.at[slot]),
                pltpu.make_async_copy(vc.at[seq, :, src, :], vbuf.at[slot, :, dst, :], vsem.at[slot]))

    def fetch_group(group, ptr, whole):
        for u in range(UNROLL):
            seq, blk = ptr

            @pl.when(seq < batch)
            def _():
                for copy in copies(seq, blk, group * UNROLL + u, whole):
                    copy.start()

            ptr = following(seq, blk)
        return ptr

    ld_len.wait()
    ptr = (jnp.int32(0), jnp.int32(0))
    for group in range(GROUPS):
        ptr = fetch_group(group, ptr, True)
    ld_o.start()

    n_items = jnp.int32(0)
    for seq in range(batch):
        n_items = n_items + lax.div(lens[seq] + (CHUNK - 1), CHUNK)
    n_steps = lax.div(n_items + (UNROLL - 1), UNROLL)

    for copy in (ld_x, ld_g, ld_b):
        copy.wait()
    a_norm = layer_norm(x_v[...].astype(F32), g_v[...].reshape(1, -1), b_v[...].reshape(1, -1))
    ld_q.wait()
    q_s[0:batch, :] = dot(a_norm, wq[...]).astype(BF16).astype(F32)
    q_s[batch:, :] = jnp.zeros((q_s.shape[0] - batch, width), F32)
    m_s[...] = jnp.full(m_s.shape, NEG, F32)
    l_s[...] = jnp.zeros_like(l_s)
    acc_s[...] = jnp.zeros_like(acc_s)

    pair = 2 * dim
    part_rows = CHUNK // 2
    row8 = lax.broadcasted_iota(jnp.int32, (8, 1), 0)
    pair_row = lax.broadcasted_iota(jnp.int32, (8, pair), 0)
    pair_side = lax.broadcasted_iota(jnp.int32, (8, pair), 1) // dim
    sel01 = (pair_row == pair_side).astype(F32)
    sel2 = (pair_row == pair_side + 2).astype(F32)
    lane = lax.broadcasted_iota(jnp.int32, (8, CHUNK), 1)
    lane2 = lax.broadcasted_iota(jnp.int32, (8, part_rows), 1)

    def new_token():
        ld_k.wait()
        k_new = dot(a_norm, wk[...]).astype(BF16)
        ld_v.wait()
        v_new = dot(a_norm, wv[...]).astype(BF16)
        for h in range(heads):
            knew_ref[h] = k_new[:, h * dim:(h + 1) * dim]
            vnew_ref[h] = v_new[:, h * dim:(h + 1) * dim]
        qk = q_s[0:batch, :] * k_new.astype(F32)
        v_s[...] = v_new.astype(F32)
        for seq in range(batch):
            prod = qk[seq:seq + 1, :]
            tail = jnp.concatenate([prod[:, pair:width], jnp.zeros((1, pair - dim), F32)], axis=1)
            s_new = jnp.sum(prod[:, 0:pair] * sel01 + tail * sel2, axis=1, keepdims=True) * scale
            new_s[seq] = jnp.broadcast_to(jnp.where(row8 == 3, NEG, s_new), (8, dim))

    def step(i, carry):
        ptr, cur = carry[:2], carry[2:]
        group = lax.rem(i, GROUPS)

        @pl.when(i == 1)
        def _():
            new_token()

        items = []
        for u in range(UNROLL):
            items.append((*cur, group * UNROLL + u))
            cur = following(*cur)
        for seq, blk, slot in items:

            @pl.when((seq < batch) & (i < GROUPS))
            def _():
                for copy in copies(seq, blk, slot, True):
                    copy.wait()

            @pl.when((seq < batch) & (i >= GROUPS))
            def _():
                for copy in copies(seq, blk, slot, False):
                    copy.wait()
        scores = []
        for seq, blk, slot in items:
            q_row = q_s[pl.ds(jnp.minimum(seq, batch), 1), :]
            q01 = (q_row[:, 0:pair] * sel01).astype(BF16)
            q2 = (jnp.concatenate([q_row[:, pair:width]] * 2, axis=1) * sel2).astype(BF16)
            k01 = jnp.concatenate([kbuf[slot, 0], kbuf[slot, 1]], axis=1)
            k2 = jnp.concatenate([kbuf[slot, 2, 0:part_rows, :], kbuf[slot, 2, part_rows:CHUNK, :]], axis=1)
            scores.append((dot_t(q01, k01), dot_t(q2, k2)))
        weights = []
        for (seq, blk, slot), (s01, s2) in zip(items, scores):
            live = len_of(seq) - blk * CHUNK
            s01 = jnp.where(lane < jnp.where(row8 < 2, live, 0), s01 * scale, NEG)
            s2 = jnp.where(lane2 < jnp.where(row8 == 2, live, jnp.where(row8 == 3, live - part_rows, 0)), s2 * scale, NEG)
            m_i = jnp.maximum(jnp.max(s01, axis=1, keepdims=True), jnp.max(s2, axis=1, keepdims=True))
            p01 = jnp.where(row8 < 2, jnp.exp(s01 - m_i), 0.0)
            p2 = jnp.where(row8 < 2, 0.0, jnp.exp(s2 - m_i))
            l_i = jnp.sum(p01, axis=1, keepdims=True) + jnp.sum(p2, axis=1, keepdims=True)
            weights.append((m_i, l_i, p01.astype(BF16), p2.astype(BF16)))
        values = []
        for (seq, blk, slot), (m_i, l_i, p01, p2) in zip(items, weights):
            v01 = jnp.concatenate([vbuf[slot, 0], vbuf[slot, 1]], axis=1)
            v2 = jnp.concatenate([vbuf[slot, 2, 0:part_rows, :], vbuf[slot, 2, part_rows:CHUNK, :]], axis=1)
            values.append(dot(p01, v01) + dot(p2, v2))
        for (seq, blk, slot), (m_i, l_i, p01, p2), pv in zip(items, weights, values):
            row = jnp.minimum(seq, batch)
            m_old = m_s[row]
            m_new = jnp.maximum(m_old, m_i)
            keep = jnp.exp(m_old - m_new)
            add = jnp.exp(m_i - m_new)
            m_s[row] = m_new
            l_s[row] = l_s[row] * keep + l_i * add
            acc_s[row] = acc_s[row] * jnp.concatenate([keep] * 2, axis=1) + pv * jnp.concatenate([add] * 2, axis=1)
        ptr = fetch_group(group, ptr, False)
        return (*ptr, *cur)

    lax.fori_loop(0, n_steps, step, (*ptr, jnp.int32(0), jnp.int32(0)))
    for seq in range(batch):
        m_old, s_new = m_s[seq], new_s[seq]
        m = jnp.maximum(m_old, s_new)
        keep, add = jnp.exp(m_old - m), jnp.exp(s_new - m)
        v_row = v_s[seq:seq + 1, :]
        v_pair = jnp.where(pair_row < 2, v_row[:, 0:pair], jnp.concatenate([v_row[:, pair:width]] * 2, axis=1))
        l = l_s[seq] * keep + add
        acc = acc_s[seq] * jnp.concatenate([keep] * 2, axis=1) + v_pair * jnp.concatenate([add] * 2, axis=1)
        top = jnp.maximum(m[2:3], m[3:4])
        w_a, w_b = jnp.exp(m[2:3] - top), jnp.exp(m[3:4] - top)
        o2 = (acc[2:3, 0:dim] * w_a + acc[3:4, dim:pair] * w_b) / (l[2:3] * w_a + l[3:4] * w_b)
        o_s[seq:seq + 1, :] = jnp.concatenate([acc[0:1, 0:dim] / l[0:1], acc[1:2, dim:pair] / l[1:2], o2], axis=1)
    ld_o.wait()
    part_ref[...] = dot(o_s[...].astype(BF16), wo[...]).astype(BF16)


def rest_kernel(batch, heads, dim, tp, part_ref, x_ref, g2, b2, g3, b3, wqc_h, e_own_h, wk_h, wv_h, wkr_h, wvr_h, woc_h, wup_h, wdn_h,
                out_ref,
                wqc, enc, wkv, wkvr, woc, wup, wdn, kv_own, kv_rem, v_late, recv, send2, send3,
                qc_s, qc_r, o_snd, o_rcv, o2_snd, o2_rcv, lsem, ssem, rsem, xs, xr, ns, nr):
    width = heads * dim
    scale = dim ** -0.5
    me = lax.axis_index('tp')
    far = lax.rem(me + 2, tp)
    near = me + 1 - 2 * lax.rem(me, 2)
    half = enc.shape[0] // 2
    early = wvr_h.shape[1]

    def load(i, src, dst):
        copy = pltpu.make_async_copy(src, dst, lsem.at[i])
        copy.start()
        return copy

    ld_wv = load(2, wv_h, wkv.at[:, pl.ds(width, width)])
    ld_e0 = load(0, e_own_h, enc.at[pl.ds(0, half), :])
    ld_wk = load(1, wk_h, wkv.at[:, pl.ds(0, width)])
    ld_wkr = load(3, wkr_h, wkvr.at[:, pl.ds(0, width)])
    ld_wvr = load(4, wvr_h, wkvr.at[:, pl.ds(width, early)])
    ld_wqc = load(5, wqc_h, wqc)
    ld_woc = load(6, woc_h, woc)
    ld_up = load(7, wup_h, wup)
    ld_dn = load(8, wdn_h, wdn)

    barrier = pltpu.get_barrier_semaphore()
    for d in range(1, tp):
        pl.semaphore_signal(barrier, inc=1, device_id={'tp': lax.rem(me + d, tp)}, device_id_type=pl.DeviceIdType.MESH)
    pl.semaphore_wait(barrier, tp - 1)

    def remote(src, dst, send_sem, recv_sem, device):
        return pltpu.make_async_remote_copy(src_ref=src, dst_ref=dst, send_sem=send_sem, recv_sem=recv_sem,
                                            device_id={'tp': device}, device_id_type=pl.DeviceIdType.MESH)

    def sum_copies(n, src):
        return [remote(src, recv.at[n, me], ssem.at[n, d - 1], rsem.at[n, me], lax.rem(me + d, tp)) for d in range(1, tp)]

    def exchange(n, src):
        for copy in sum_copies(n, src):
            copy.start()
        recv[n, me] = src[...]

    def collect(n, src):
        for copy in sum_copies(n, src):
            copy.wait_send()
        for d in range(1, tp):
            other = lax.rem(me + d, tp)
            remote(src, recv.at[n, other], ssem.at[n, d - 1], rsem.at[n, other], other).wait_recv()
        total = recv[n, 0].astype(F32)
        for t in range(1, tp):
            total = total + recv[n, t].astype(F32)
        return total

    def project(first, count, jobs, tile=256):
        def body(i, c):
            rows = pl.ds(pl.multiple_of(i * tile, tile), tile)
            for weights, out, lo, hi in jobs:
                out[rows, lo:hi] = dot(enc[rows, :], weights[:, lo:hi]).astype(BF16)
            return c

        lax.fori_loop(first // tile, (first + count) // tile, body, 0)

    late_rows = (0, 512, wv_h.shape[0])

    def late(i):
        rows, cols = pl.ds(late_rows[i], late_rows[i + 1] - late_rows[i]), width - early
        return remote(wkv.at[rows, pl.ds(width + early, cols)], wkvr.at[rows, pl.ds(width + early, cols)], xs.at[3 + i], xr.at[3 + i], far)

    def late_product(i, tile=256):
        lo, hi = late_rows[i], late_rows[i + 1]

        def body(t, c):
            rows = pl.ds(pl.multiple_of(t * tile, tile), tile)
            product = dot(enc[rows, lo:hi], wkvr[lo:hi, width + early:2 * width])
            if i == 0:
                v_late[rows, :] = product
            else:
                kv_rem[rows, width + early:2 * width] = (v_late[rows, :] + product).astype(BF16)
            return c

        lax.fori_loop(0, 2 * half // tile, body, 0)

    def near_tokens(i):
        rows = half // 2
        return remote(enc.at[pl.ds(i * rows, rows), :], enc.at[pl.ds(half + i * rows, rows), :], ns.at[i], nr.at[i], near)

    own_job = (wkv, kv_own, 0, 2 * width)
    far_job = (wkvr, kv_rem, 0, width + early)

    exchange(0, part_ref)
    ld_wv.wait()
    late(0).start()
    ld_e0.wait()
    near_tokens(0).start()
    near_tokens(1).start()
    for copy in (ld_wk, ld_wkr, ld_wvr):
        copy.wait()
    project(0, half, (own_job, far_job))
    h1 = x_ref[...].astype(F32) + collect(0, part_ref)
    c_norm = layer_norm(h1, g2[...].reshape(1, -1), b2[...].reshape(1, -1))
    ld_wqc.wait()
    qc_s[...] = dot(c_norm, wqc[...]).astype(BF16)
    send_q = remote(qc_s, qc_r, xs.at[0], xr.at[0], far)
    send_q.start()
    late(1).start()
    near_tokens(0).wait()
    near_tokens(1).wait()
    project(half, half, (far_job,))

    rows = heads * batch
    row_b = lax.rem(lax.broadcasted_iota(jnp.int32, (rows, 128), 0), batch)
    lane = lax.broadcasted_iota(jnp.int32, (rows, 128), 1)
    per = half // batch
    pack = 128 // per
    blocks = half // 128
    mine = lax.rem(row_b, pack) == lane // per
    row_blk = row_b // pack
    lane_head = lax.broadcasted_iota(jnp.int32, (batch, width), 1) // dim

    def weigh(q, kv):
        qf = q.astype(F32)
        q_rows = jnp.concatenate([jnp.where(lane_head == h, qf, 0.0) for h in range(heads)], axis=0).astype(BF16)
        parts = []
        for part in range(2):
            s_all = dot_t(q_rows, kv[part * half:(part + 1) * half, 0:width])
            s = s_all[:, 0:128]
            for k in range(1, blocks):
                s = jnp.where(row_blk == k, s_all[:, k * 128:(k + 1) * 128], s)
            parts.append(jnp.where(mine, s * scale, NEG))
        m = jnp.maximum(jnp.max(parts[0], axis=1, keepdims=True), jnp.max(parts[1], axis=1, keepdims=True))
        p = [jnp.exp(s - m) for s in parts]
        l = jnp.sum(p[0], axis=1, keepdims=True) + jnp.sum(p[1], axis=1, keepdims=True)
        wide = [jnp.concatenate([jnp.where(row_blk == k, p[part], 0.0) for k in range(blocks)], axis=1).astype(BF16) for part in range(2)]
        return m, l, wide

    def mix(wide, kv, first, last):
        lo, hi = first * batch, last * batch
        o = sum(dot(wide[part][lo:hi], kv[part * half:(part + 1) * half, width + first * dim:width + last * dim]) for part in range(2))
        return jnp.concatenate([o[(h - first) * batch:(h - first + 1) * batch, (h - first) * dim:(h - first + 1) * dim] for h in range(first, last)], axis=0)

    n_early = early // dim
    send_q.wait()
    m_r, l_r, wide_r = weigh(qc_r[...], kv_rem)
    o_snd[0:n_early * batch, :] = mix(wide_r, kv_rem, 0, n_early)
    stats = jnp.zeros((batch, dim), F32)
    st_lane = lax.broadcasted_iota(jnp.int32, (batch, dim), 1)
    for h in range(heads):
        stats = jnp.where(st_lane == 2 * h, m_r[h * batch:(h + 1) * batch], jnp.where(st_lane == 2 * h + 1, l_r[h * batch:(h + 1) * batch], stats))
    o_snd[n_early * batch:(n_early + 1) * batch, :] = stats
    send_o = remote(o_snd, o_rcv, xs.at[1], xr.at[1], far)
    send_o.start()
    for i in range(2):
        late(i).wait()
        late_product(i)
    o2_snd[...] = mix(wide_r, kv_rem, n_early, heads)
    send_o2 = remote(o2_snd, o2_rcv, xs.at[2], xr.at[2], far)
    send_o2.start()
    project(half, half, (own_job,))
    m_a, l_a, wide_a = weigh(qc_s[...], kv_own)
    o_a = mix(wide_a, kv_own, 0, heads)
    send_o.wait()
    stats = o_rcv[n_early * batch:(n_early + 1) * batch, :]
    m_b = jnp.concatenate([stats[:, 2 * h:2 * h + 1] for h in range(heads)], axis=0)
    l_b = jnp.concatenate([stats[:, 2 * h + 1:2 * h + 2] for h in range(heads)], axis=0)
    m = jnp.maximum(m_a, m_b)
    w_a, w_b = jnp.exp(m_a - m), jnp.exp(m_b - m)
    send_o2.wait()
    o_b = jnp.concatenate([o_rcv[0:n_early * batch, :], o2_rcv[...]], axis=0)
    o = (o_a * w_a + o_b * w_b) / (l_a * w_a + l_b * w_b)
    oc = jnp.concatenate([o[h * batch:(h + 1) * batch, :] for h in range(heads)], axis=1).astype(BF16)

    def matmul_sum(n, lhs, weights, out):
        out[...] = dot(lhs, weights[...]).astype(BF16)
        exchange(n, out)
        return collect(n, out)

    ld_woc.wait()
    h2 = h1 + matmul_sum(1, oc, woc, send2)
    m_norm = layer_norm(h2, g3[...].reshape(1, -1), b3[...].reshape(1, -1))
    ld_up.wait()
    up = dot(m_norm, wup[...])
    hidden = (0.5 * up * (1.0 + lax.erf(up * (0.5 ** 0.5)))).astype(BF16)
    ld_dn.wait()
    out_ref[...] = h2 + matmul_sum(2, hidden, wdn, send3)


def local_step(x, k_cache, v_cache, seq_lens, nbr_enc, ln1_gain, ln1_bias, w_q, w_k, w_v, w_o, ln2_gain, ln2_bias, wq_c, wk_c, wv_c, wo_c, ln3_gain, ln3_bias, w_up, w_down):
    batch, d_model = x.shape
    heads, dim = k_cache.shape[2:]
    width = heads * dim
    tp = lax.axis_size('tp')
    far = [(i, (i + 2) % tp) for i in range(tp)]
    enc = nbr_enc.reshape(-1, nbr_enc.shape[-1])
    wk_far = lax.ppermute(wk_c, 'tp', far)
    wv_cut = wv_c[:, :2 * dim]
    wv_far = lax.ppermute(wv_cut, 'tp', far)

    any_spec = pl.BlockSpec(memory_space=pl.ANY)
    hbm = pl.BlockSpec(memory_space=pltpu.HBM)
    vmem = pl.BlockSpec(memory_space=pltpu.VMEM)
    slots = GROUPS * UNROLL
    part, k_new, v_new = pl.pallas_call(
        functools.partial(self_kernel, batch, heads, dim),
        out_shape=(jax.ShapeDtypeStruct((batch, d_model), BF16), jax.ShapeDtypeStruct((heads, batch, dim), BF16), jax.ShapeDtypeStruct((heads, batch, dim), BF16)),
        in_specs=[hbm] * 10,
        out_specs=(vmem, vmem, vmem),
        scratch_shapes=[
            pltpu.SMEM((batch,), jnp.int32), pltpu.VMEM((batch, d_model), BF16), pltpu.VMEM((d_model,), F32), pltpu.VMEM((d_model,), F32),
            pltpu.VMEM((d_model, width), BF16), pltpu.VMEM((d_model, width), BF16), pltpu.VMEM((d_model, width), BF16), pltpu.VMEM((width, d_model), BF16),
            pltpu.VMEM((slots, heads, CHUNK, dim), BF16), pltpu.VMEM((slots, heads, CHUNK, dim), BF16),
            pltpu.VMEM((batch + 8, width), F32), pltpu.VMEM((batch, width), F32), pltpu.VMEM((batch, width), F32),
            pltpu.VMEM((batch + 1, 8, dim), F32), pltpu.VMEM((batch + 1, 8, dim), F32), pltpu.VMEM((batch + 1, 8, 2 * dim), F32), pltpu.VMEM((batch, 8, dim), F32),
            pltpu.SemaphoreType.DMA((8,)), pltpu.SemaphoreType.DMA((slots,)), pltpu.SemaphoreType.DMA((slots,)),
        ],
        compiler_params=pltpu.CompilerParams(vmem_limit_bytes=46000000),
        cost_estimate=pl.CostEstimate(flops=40_000_000_000, bytes_accessed=60_000_000, transcendentals=0),
        name='self_attention',
    )(*in_hbm(seq_lens, x, ln1_gain, ln1_bias, jnp.transpose(k_cache, (0, 2, 1, 3)), jnp.transpose(v_cache, (0, 2, 1, 3)), w_q, w_k, w_v, w_o))

    n_enc, enc_dim = enc.shape
    ff = w_up.shape[1]
    out = pl.pallas_call(
        functools.partial(rest_kernel, batch, heads, dim, tp),
        out_shape=jax.ShapeDtypeStruct((batch, d_model), F32),
        in_specs=[vmem] * 6 + [hbm] * 4 + [any_spec] * 2 + [hbm] * 3,
        out_specs=vmem,
        scratch_shapes=[
            pltpu.VMEM((d_model, width), BF16), pltpu.VMEM((2 * n_enc, enc_dim), BF16),
            pltpu.VMEM((enc_dim, 2 * width), BF16), pltpu.VMEM((enc_dim, 2 * width), BF16),
            pltpu.VMEM((width, d_model), BF16), pltpu.VMEM((d_model, ff), BF16), pltpu.VMEM((ff, d_model), BF16),
            pltpu.VMEM((2 * n_enc, 2 * width), BF16), pltpu.VMEM((2 * n_enc, 2 * width), BF16), pltpu.VMEM((2 * n_enc, dim), F32),
            pltpu.VMEM((3, tp, batch, d_model), BF16),
            pltpu.VMEM((batch, d_model), BF16), pltpu.VMEM((batch, d_model), BF16),
            pltpu.VMEM((batch, width), BF16), pltpu.VMEM((batch, width), BF16),
            pltpu.VMEM((heads * batch, dim), F32), pltpu.VMEM((heads * batch, dim), F32), pltpu.VMEM((batch, dim), F32), pltpu.VMEM((batch, dim), F32),
            pltpu.SemaphoreType.DMA((9,)), pltpu.SemaphoreType.DMA((3, tp - 1)), pltpu.SemaphoreType.DMA((3, tp)),
            pltpu.SemaphoreType.DMA((5,)), pltpu.SemaphoreType.DMA((5,)), pltpu.SemaphoreType.DMA((2,)), pltpu.SemaphoreType.DMA((2,)),
        ],
        compiler_params=pltpu.CompilerParams(collective_id=0, has_side_effects=True, vmem_limit_bytes=46000000),
        cost_estimate=pl.CostEstimate(flops=20_000_000_000, bytes_accessed=30_000_000, transcendentals=0),
        name='rest_of_layer',
    )(part, x, ln2_gain, ln2_bias, ln3_gain, ln3_bias, *in_hbm(wq_c, enc, wk_c, wv_c), wk_far, wv_far, *in_hbm(wo_c, w_up, w_down))
    return out.astype(BF16), jnp.transpose(k_new, (1, 0, 2)), jnp.transpose(v_new, (1, 0, 2))


def solution(mesh):
    row_spec = P('dp', None)
    cache_spec = P('dp', None, 'tp', None)
    head_spec = P('dp', 'tp', None)
    vec_spec = P(None)
    col_split = P(None, 'tp')
    row_split = P('tp', None)
    in_specs = (row_spec, cache_spec, cache_spec, P('dp'), P('dp', 'tp', None), vec_spec, vec_spec, col_split, col_split, col_split, row_split, vec_spec, vec_spec, col_split, col_split, col_split, row_split, vec_spec, vec_spec, col_split, row_split)
    out_specs = (row_spec, head_spec, head_spec)
    return jax.shard_map(local_step, mesh=mesh, in_specs=in_specs, out_specs=out_specs, check_vma=False)
```

```python
import functools

import jax
import jax.numpy as jnp
from jax import lax
from jax.experimental import pallas as pl
from jax.experimental.pallas import tpu as pltpu
from jax.sharding import PartitionSpec as P


LN_EPS = 1e-5
NEG = -1e30
F32 = jnp.float32
BF16 = jnp.bfloat16
CHUNK = 512
UNROLL = 4
GRAIN = 64
GROUPS = 6
ENC_STEPS = 4


def layer_norm(values, ln_gain, ln_bias):
    row_mean = jnp.mean(values, axis=-1, keepdims=True)
    centred = values - row_mean
    row_var = jnp.mean(jnp.square(centred), axis=-1, keepdims=True)
    return (centred * lax.rsqrt(row_var + LN_EPS) * ln_gain + ln_bias).astype(BF16)


def dot(lhs, rhs):
    return jnp.dot(lhs, rhs, preferred_element_type=F32)


def dot_t(lhs, rhs):
    return lax.dot_general(lhs, rhs, (((1,), (1,)), ((), ())), preferred_element_type=F32)


def in_hbm(*arrays):
    return [pltpu.with_memory_space_constraint(a, pltpu.HBM) for a in arrays]


def self_kernel(batch, heads, dim, lens_h, x_h, g_h, b_h, kc, vc, wq_h, wk_h, wv_h, wo_h, e_h, wkc_h, wvc_h,
                part_ref, knew_ref, vnew_ref, kv_ref,
                lens, x_v, g_v, b_v, wq, wk, wv, wo, kbuf, vbuf, q_s, v_s, o_s, m_s, l_s, acc_s, new_s, enc, wkv, wsem, ksem, vsem, esem):
    width = heads * dim
    scale = dim ** -0.5
    pairs = ((x_h, x_v), (g_h, g_v), (b_h, b_v), (wq_h, wq), (lens_h, lens), (wk_h, wk), (wv_h, wv), (wo_h, wo))
    ld_x, ld_g, ld_b, ld_q, ld_len, ld_k, ld_v, ld_o = [pltpu.make_async_copy(src, dst, wsem.at[i]) for i, (src, dst) in enumerate(pairs)]
    for copy in (ld_len, ld_x, ld_g, ld_b, ld_q, ld_k, ld_v):
        copy.start()

    def len_of(seq):
        return jnp.where(seq < batch, lens[jnp.minimum(seq, batch - 1)], 0)

    def following(seq, blk):
        more = (blk + 1) * CHUNK < len_of(seq)
        return jnp.where(more, seq, seq + 1), jnp.where(more, blk + 1, 0)

    def copies(seq, blk, slot, whole):
        live = pl.multiple_of(jnp.minimum(len_of(seq) - blk * CHUNK, CHUNK), GRAIN)
        first = pl.multiple_of(blk * CHUNK, CHUNK)
        count = CHUNK if whole else live
        src, dst = pl.ds(first, count), pl.ds(0, count)
        return (pltpu.make_async_copy(kc.at[seq, :, src, :], kbuf.at[slot, :, dst, :], ksem.at[slot]),
                pltpu.make_async_copy(vc.at[seq, :, src, :], vbuf.at[slot, :, dst, :], vsem.at[slot]))

    def fetch_group(group, ptr, whole):
        for u in range(UNROLL):
            seq, blk = ptr

            @pl.when(seq < batch)
            def _():
                for copy in copies(seq, blk, group * UNROLL + u, whole):
                    copy.start()

            ptr = following(seq, blk)
        return ptr

    ld_len.wait()
    ptr = (jnp.int32(0), jnp.int32(0))
    for group in range(GROUPS):
        ptr = fetch_group(group, ptr, True)
    ld_o.start()
    enc_loads = [pltpu.make_async_copy(src, dst, esem.at[i]) for i, (src, dst) in enumerate(
        ((e_h, enc), (wkc_h, wkv.at[:, pl.ds(0, width)]), (wvc_h, wkv.at[:, pl.ds(width, width)])))]
    for copy in enc_loads:
        copy.start()
    enc_tile = enc.shape[0] // ENC_STEPS

    n_items = jnp.int32(0)
    for seq in range(batch):
        n_items = n_items + lax.div(lens[seq] + (CHUNK - 1), CHUNK)
    n_steps = lax.div(n_items + (UNROLL - 1), UNROLL)

    for copy in (ld_x, ld_g, ld_b):
        copy.wait()
    a_norm = layer_norm(x_v[...].astype(F32), g_v[...].reshape(1, -1), b_v[...].reshape(1, -1))
    ld_q.wait()
    q_s[0:batch, :] = dot(a_norm, wq[...]).astype(BF16).astype(F32)
    q_s[batch:, :] = jnp.zeros((q_s.shape[0] - batch, width), F32)
    m_s[...] = jnp.full(m_s.shape, NEG, F32)
    l_s[...] = jnp.zeros_like(l_s)
    acc_s[...] = jnp.zeros_like(acc_s)

    pair = 2 * dim
    part_rows = CHUNK // 2
    row8 = lax.broadcasted_iota(jnp.int32, (8, 1), 0)
    pair_row = lax.broadcasted_iota(jnp.int32, (8, pair), 0)
    pair_side = lax.broadcasted_iota(jnp.int32, (8, pair), 1) // dim
    sel01 = (pair_row == pair_side).astype(F32)
    sel2 = (pair_row == pair_side + 2).astype(F32)
    lane = lax.broadcasted_iota(jnp.int32, (8, CHUNK), 1)
    lane2 = lax.broadcasted_iota(jnp.int32, (8, part_rows), 1)

    def new_token():
        ld_k.wait()
        k_new = dot(a_norm, wk[...]).astype(BF16)
        ld_v.wait()
        v_new = dot(a_norm, wv[...]).astype(BF16)
        for h in range(heads):
            knew_ref[h] = k_new[:, h * dim:(h + 1) * dim]
            vnew_ref[h] = v_new[:, h * dim:(h + 1) * dim]
        qk = q_s[0:batch, :] * k_new.astype(F32)
        v_s[...] = v_new.astype(F32)
        for seq in range(batch):
            prod = qk[seq:seq + 1, :]
            tail = jnp.concatenate([prod[:, pair:width], jnp.zeros((1, pair - dim), F32)], axis=1)
            s_new = jnp.sum(prod[:, 0:pair] * sel01 + tail * sel2, axis=1, keepdims=True) * scale
            new_s[seq] = jnp.broadcast_to(jnp.where(row8 == 3, NEG, s_new), (8, dim))

    def step(i, carry):
        ptr, cur = carry[:2], carry[2:]
        group = lax.rem(i, GROUPS)

        @pl.when(i == 1)
        def _():
            new_token()
            for copy in enc_loads:
                copy.wait()

        @pl.when((i >= 1) & (i <= ENC_STEPS))
        def _():
            rows = pl.ds(pl.multiple_of((i - 1) * enc_tile, enc_tile), enc_tile)
            kv_ref[rows, :] = dot(enc[rows, :], wkv[...]).astype(BF16)

        items = []
        for u in range(UNROLL):
            items.append((*cur, group * UNROLL + u))
            cur = following(*cur)
        for seq, blk, slot in items:

            @pl.when((seq < batch) & (i < GROUPS))
            def _():
                for copy in copies(seq, blk, slot, True):
                    copy.wait()

            @pl.when((seq < batch) & (i >= GROUPS))
            def _():
                for copy in copies(seq, blk, slot, False):
                    copy.wait()
        scores = []
        for seq, blk, slot in items:
            q_row = q_s[pl.ds(jnp.minimum(seq, batch), 1), :]
            q01 = (q_row[:, 0:pair] * sel01).astype(BF16)
            q2 = (jnp.concatenate([q_row[:, pair:width]] * 2, axis=1) * sel2).astype(BF16)
            k01 = jnp.concatenate([kbuf[slot, 0], kbuf[slot, 1]], axis=1)
            k2 = jnp.concatenate([kbuf[slot, 2, 0:part_rows, :], kbuf[slot, 2, part_rows:CHUNK, :]], axis=1)
            scores.append((dot_t(q01, k01), dot_t(q2, k2)))
        weights = []
        for (seq, blk, slot), (s01, s2) in zip(items, scores):
            live = len_of(seq) - blk * CHUNK
            s01 = jnp.where(lane < jnp.where(row8 < 2, live, 0), s01 * scale, NEG)
            s2 = jnp.where(lane2 < jnp.where(row8 == 2, live, jnp.where(row8 == 3, live - part_rows, 0)), s2 * scale, NEG)
            m_i = jnp.maximum(jnp.max(s01, axis=1, keepdims=True), jnp.max(s2, axis=1, keepdims=True))
            p01 = jnp.where(row8 < 2, jnp.exp(s01 - m_i), 0.0)
            p2 = jnp.where(row8 < 2, 0.0, jnp.exp(s2 - m_i))
            l_i = jnp.sum(p01, axis=1, keepdims=True) + jnp.sum(p2, axis=1, keepdims=True)
            weights.append((m_i, l_i, p01.astype(BF16), p2.astype(BF16)))
        values = []
        for (seq, blk, slot), (m_i, l_i, p01, p2) in zip(items, weights):
            v01 = jnp.concatenate([vbuf[slot, 0], vbuf[slot, 1]], axis=1)
            v2 = jnp.concatenate([vbuf[slot, 2, 0:part_rows, :], vbuf[slot, 2, part_rows:CHUNK, :]], axis=1)
            values.append(dot(p01, v01) + dot(p2, v2))
        for (seq, blk, slot), (m_i, l_i, p01, p2), pv in zip(items, weights, values):
            row = jnp.minimum(seq, batch)
            m_old = m_s[row]
            m_new = jnp.maximum(m_old, m_i)
            keep = jnp.exp(m_old - m_new)
            add = jnp.exp(m_i - m_new)
            m_s[row] = m_new
            l_s[row] = l_s[row] * keep + l_i * add
            acc_s[row] = acc_s[row] * jnp.concatenate([keep] * 2, axis=1) + pv * jnp.concatenate([add] * 2, axis=1)
        ptr = fetch_group(group, ptr, False)
        return (*ptr, *cur)

    lax.fori_loop(0, n_steps, step, (*ptr, jnp.int32(0), jnp.int32(0)))
    for seq in range(batch):
        m_old, s_new = m_s[seq], new_s[seq]
        m = jnp.maximum(m_old, s_new)
        keep, add = jnp.exp(m_old - m), jnp.exp(s_new - m)
        v_row = v_s[seq:seq + 1, :]
        v_pair = jnp.where(pair_row < 2, v_row[:, 0:pair], jnp.concatenate([v_row[:, pair:width]] * 2, axis=1))
        l = l_s[seq] * keep + add
        acc = acc_s[seq] * jnp.concatenate([keep] * 2, axis=1) + v_pair * jnp.concatenate([add] * 2, axis=1)
        top = jnp.maximum(m[2:3], m[3:4])
        w_a, w_b = jnp.exp(m[2:3] - top), jnp.exp(m[3:4] - top)
        o2 = (acc[2:3, 0:dim] * w_a + acc[3:4, dim:pair] * w_b) / (l[2:3] * w_a + l[3:4] * w_b)
        o_s[seq:seq + 1, :] = jnp.concatenate([acc[0:1, 0:dim] / l[0:1], acc[1:2, dim:pair] / l[1:2], o2], axis=1)
    ld_o.wait()
    part_ref[...] = dot(o_s[...].astype(BF16), wo[...]).astype(BF16)


def rest_kernel(batch, heads, dim, tp, part_ref, x_ref, g2, b2, g3, b3, wqc_h, e_own_h, wk_h, wv_h, wkr_h, wvr_h, kv_h, woc_h, wup_h, wdn_h,
                out_ref,
                wqc, enc, wkv, wkvr, woc, wup, wdn, kv_own, kv_rem, v_late, recv, send2, send3,
                qc_s, qc_r, o_snd, o_rcv, o2_snd, o2_rcv, lsem, ssem, rsem, xs, xr, ns, nr):
    width = heads * dim
    scale = dim ** -0.5
    me = lax.axis_index('tp')
    far = lax.rem(me + 2, tp)
    near = me + 1 - 2 * lax.rem(me, 2)
    half = enc.shape[0] // 2
    early = wvr_h.shape[1]

    def load(i, src, dst):
        copy = pltpu.make_async_copy(src, dst, lsem.at[i])
        copy.start()
        return copy

    ld_wv = load(2, wv_h, wkv.at[:, pl.ds(width, width)])
    ld_e0 = load(0, e_own_h, enc.at[pl.ds(0, half), :])
    ld_wk = load(1, wk_h, wkv.at[:, pl.ds(0, width)])
    ld_wkr = load(3, wkr_h, wkvr.at[:, pl.ds(0, width)])
    ld_wvr = load(4, wvr_h, wkvr.at[:, pl.ds(width, early)])
    ld_wqc = load(5, wqc_h, wqc)
    ld_woc = load(6, woc_h, woc)
    ld_up = load(7, wup_h, wup)
    ld_dn = load(8, wdn_h, wdn)
    ld_kv = load(9, kv_h, kv_own.at[pl.ds(0, half), :])

    barrier = pltpu.get_barrier_semaphore()
    for d in range(1, tp):
        pl.semaphore_signal(barrier, inc=1, device_id={'tp': lax.rem(me + d, tp)}, device_id_type=pl.DeviceIdType.MESH)
    pl.semaphore_wait(barrier, tp - 1)

    def remote(src, dst, send_sem, recv_sem, device):
        return pltpu.make_async_remote_copy(src_ref=src, dst_ref=dst, send_sem=send_sem, recv_sem=recv_sem,
                                            device_id={'tp': device}, device_id_type=pl.DeviceIdType.MESH)

    def sum_copies(n, src):
        return [remote(src, recv.at[n, me], ssem.at[n, d - 1], rsem.at[n, me], lax.rem(me + d, tp)) for d in range(1, tp)]

    def exchange(n, src):
        for copy in sum_copies(n, src):
            copy.start()
        recv[n, me] = src[...]

    def collect(n, src):
        for copy in sum_copies(n, src):
            copy.wait_send()
        for d in range(1, tp):
            other = lax.rem(me + d, tp)
            remote(src, recv.at[n, other], ssem.at[n, d - 1], rsem.at[n, other], other).wait_recv()
        total = recv[n, 0].astype(F32)
        for t in range(1, tp):
            total = total + recv[n, t].astype(F32)
        return total

    def project(first, count, jobs, tile=256):
        def body(i, c):
            rows = pl.ds(pl.multiple_of(i * tile, tile), tile)
            for weights, out, lo, hi in jobs:
                out[rows, lo:hi] = dot(enc[rows, :], weights[:, lo:hi]).astype(BF16)
            return c

        lax.fori_loop(first // tile, (first + count) // tile, body, 0)

    late_rows = (0, 512, wv_h.shape[0])

    def late(i):
        rows, cols = pl.ds(late_rows[i], late_rows[i + 1] - late_rows[i]), width - early
        return remote(wkv.at[rows, pl.ds(width + early, cols)], wkvr.at[rows, pl.ds(width + early, cols)], xs.at[3 + i], xr.at[3 + i], far)

    def late_product(i, tile=256):
        lo, hi = late_rows[i], late_rows[i + 1]

        def body(t, c):
            rows = pl.ds(pl.multiple_of(t * tile, tile), tile)
            product = dot(enc[rows, lo:hi], wkvr[lo:hi, width + early:2 * width])
            if i == 0:
                v_late[rows, :] = product
            else:
                kv_rem[rows, width + early:2 * width] = (v_late[rows, :] + product).astype(BF16)
            return c

        lax.fori_loop(0, 2 * half // tile, body, 0)

    def near_tokens(i):
        rows = half // 2
        return remote(enc.at[pl.ds(i * rows, rows), :], enc.at[pl.ds(half + i * rows, rows), :], ns.at[i], nr.at[i], near)

    own_job = (wkv, kv_own, 0, 2 * width)
    far_job = (wkvr, kv_rem, 0, width + early)

    exchange(0, part_ref)
    ld_wv.wait()
    late(0).start()
    ld_e0.wait()
    near_tokens(0).start()
    near_tokens(1).start()
    for copy in (ld_wkr, ld_wvr):
        copy.wait()
    project(0, half, (far_job,))
    near_tokens(0).wait()
    project(half, half // 2, (far_job,))
    h1 = x_ref[...].astype(F32) + collect(0, part_ref)
    c_norm = layer_norm(h1, g2[...].reshape(1, -1), b2[...].reshape(1, -1))
    ld_wqc.wait()
    qc_s[...] = dot(c_norm, wqc[...]).astype(BF16)
    send_q = remote(qc_s, qc_r, xs.at[0], xr.at[0], far)
    send_q.start()
    late(1).start()
    near_tokens(1).wait()
    project(half + half // 2, half // 2, (far_job,))
    late(0).wait()
    late_product(0)

    rows = heads * batch
    row_b = lax.rem(lax.broadcasted_iota(jnp.int32, (rows, 128), 0), batch)
    lane = lax.broadcasted_iota(jnp.int32, (rows, 128), 1)
    per = half // batch
    pack = 128 // per
    blocks = half // 128
    mine = lax.rem(row_b, pack) == lane // per
    row_blk = row_b // pack
    lane_head = lax.broadcasted_iota(jnp.int32, (batch, width), 1) // dim

    def weigh(q, kv):
        qf = q.astype(F32)
        q_rows = jnp.concatenate([jnp.where(lane_head == h, qf, 0.0) for h in range(heads)], axis=0).astype(BF16)
        parts = []
        for part in range(2):
            s_all = dot_t(q_rows, kv[part * half:(part + 1) * half, 0:width])
            s = s_all[:, 0:128]
            for k in range(1, blocks):
                s = jnp.where(row_blk == k, s_all[:, k * 128:(k + 1) * 128], s)
            parts.append(jnp.where(mine, s * scale, NEG))
        m = jnp.maximum(jnp.max(parts[0], axis=1, keepdims=True), jnp.max(parts[1], axis=1, keepdims=True))
        p = [jnp.exp(s - m) for s in parts]
        l = jnp.sum(p[0], axis=1, keepdims=True) + jnp.sum(p[1], axis=1, keepdims=True)
        wide = [jnp.concatenate([jnp.where(row_blk == k, p[part], 0.0) for k in range(blocks)], axis=1).astype(BF16) for part in range(2)]
        return m, l, wide

    def mix(wide, kv, first, last):
        lo, hi = first * batch, last * batch
        o = sum(dot(wide[part][lo:hi], kv[part * half:(part + 1) * half, width + first * dim:width + last * dim]) for part in range(2))
        return jnp.concatenate([o[(h - first) * batch:(h - first + 1) * batch, (h - first) * dim:(h - first + 1) * dim] for h in range(first, last)], axis=0)

    n_early = early // dim
    send_q.wait()
    m_r, l_r, wide_r = weigh(qc_r[...], kv_rem)
    o_snd[0:n_early * batch, :] = mix(wide_r, kv_rem, 0, n_early)
    stats = jnp.zeros((batch, dim), F32)
    st_lane = lax.broadcasted_iota(jnp.int32, (batch, dim), 1)
    for h in range(heads):
        stats = jnp.where(st_lane == 2 * h, m_r[h * batch:(h + 1) * batch], jnp.where(st_lane == 2 * h + 1, l_r[h * batch:(h + 1) * batch], stats))
    o_snd[n_early * batch:(n_early + 1) * batch, :] = stats
    send_o = remote(o_snd, o_rcv, xs.at[1], xr.at[1], far)
    send_o.start()
    late(1).wait()
    late_product(1)
    o2_snd[...] = mix(wide_r, kv_rem, n_early, heads)
    send_o2 = remote(o2_snd, o2_rcv, xs.at[2], xr.at[2], far)
    send_o2.start()
    ld_wk.wait()
    project(half, half, (own_job,))
    ld_kv.wait()
    m_a, l_a, wide_a = weigh(qc_s[...], kv_own)
    o_a = mix(wide_a, kv_own, 0, heads)
    send_o.wait()
    stats = o_rcv[n_early * batch:(n_early + 1) * batch, :]
    m_b = jnp.concatenate([stats[:, 2 * h:2 * h + 1] for h in range(heads)], axis=0)
    l_b = jnp.concatenate([stats[:, 2 * h + 1:2 * h + 2] for h in range(heads)], axis=0)
    m = jnp.maximum(m_a, m_b)
    w_a, w_b = jnp.exp(m_a - m), jnp.exp(m_b - m)
    send_o2.wait()
    o_b = jnp.concatenate([o_rcv[0:n_early * batch, :], o2_rcv[...]], axis=0)
    o = (o_a * w_a + o_b * w_b) / (l_a * w_a + l_b * w_b)
    oc = jnp.concatenate([o[h * batch:(h + 1) * batch, :] for h in range(heads)], axis=1).astype(BF16)

    def matmul_sum(n, lhs, weights, out):
        out[...] = dot(lhs, weights[...]).astype(BF16)
        exchange(n, out)
        return collect(n, out)

    ld_woc.wait()
    h2 = h1 + matmul_sum(1, oc, woc, send2)
    m_norm = layer_norm(h2, g3[...].reshape(1, -1), b3[...].reshape(1, -1))
    ld_up.wait()
    up = dot(m_norm, wup[...])
    hidden = (0.5 * up * (1.0 + lax.erf(up * (0.5 ** 0.5)))).astype(BF16)
    ld_dn.wait()
    out_ref[...] = h2 + matmul_sum(2, hidden, wdn, send3)


def local_step(x, k_cache, v_cache, seq_lens, nbr_enc, ln1_gain, ln1_bias, w_q, w_k, w_v, w_o, ln2_gain, ln2_bias, wq_c, wk_c, wv_c, wo_c, ln3_gain, ln3_bias, w_up, w_down):
    batch, d_model = x.shape
    heads, dim = k_cache.shape[2:]
    width = heads * dim
    tp = lax.axis_size('tp')
    far = [(i, (i + 2) % tp) for i in range(tp)]
    enc = nbr_enc.reshape(-1, nbr_enc.shape[-1])
    wk_far = lax.ppermute(wk_c, 'tp', far)
    wv_cut = wv_c[:, :2 * dim]
    wv_far = lax.ppermute(wv_cut, 'tp', far)

    any_spec = pl.BlockSpec(memory_space=pl.ANY)
    hbm = pl.BlockSpec(memory_space=pltpu.HBM)
    vmem = pl.BlockSpec(memory_space=pltpu.VMEM)
    slots = GROUPS * UNROLL
    part, k_new, v_new, kv_half = pl.pallas_call(
        functools.partial(self_kernel, batch, heads, dim),
        out_shape=(jax.ShapeDtypeStruct((batch, d_model), BF16), jax.ShapeDtypeStruct((heads, batch, dim), BF16), jax.ShapeDtypeStruct((heads, batch, dim), BF16),
                   jax.ShapeDtypeStruct((enc.shape[0], 2 * width), BF16)),
        in_specs=[hbm] * 13,
        out_specs=(vmem, vmem, vmem, vmem),
        scratch_shapes=[
            pltpu.SMEM((batch,), jnp.int32), pltpu.VMEM((batch, d_model), BF16), pltpu.VMEM((d_model,), F32), pltpu.VMEM((d_model,), F32),
            pltpu.VMEM((d_model, width), BF16), pltpu.VMEM((d_model, width), BF16), pltpu.VMEM((d_model, width), BF16), pltpu.VMEM((width, d_model), BF16),
            pltpu.VMEM((slots, heads, CHUNK, dim), BF16), pltpu.VMEM((slots, heads, CHUNK, dim), BF16),
            pltpu.VMEM((batch + 8, width), F32), pltpu.VMEM((batch, width), F32), pltpu.VMEM((batch, width), F32),
            pltpu.VMEM((batch + 1, 8, dim), F32), pltpu.VMEM((batch + 1, 8, dim), F32), pltpu.VMEM((batch + 1, 8, 2 * dim), F32), pltpu.VMEM((batch, 8, dim), F32),
            pltpu.VMEM(enc.shape, BF16), pltpu.VMEM((enc.shape[1], 2 * width), BF16),
            pltpu.SemaphoreType.DMA((8,)), pltpu.SemaphoreType.DMA((slots,)), pltpu.SemaphoreType.DMA((slots,)), pltpu.SemaphoreType.DMA((3,)),
        ],
        compiler_params=pltpu.CompilerParams(vmem_limit_bytes=46000000),
        cost_estimate=pl.CostEstimate(flops=40_000_000_000, bytes_accessed=60_000_000, transcendentals=0),
        name='self_attention',
    )(*in_hbm(seq_lens, x, ln1_gain, ln1_bias, jnp.transpose(k_cache, (0, 2, 1, 3)), jnp.transpose(v_cache, (0, 2, 1, 3)), w_q, w_k, w_v, w_o, enc, wk_c, wv_c))

    n_enc, enc_dim = enc.shape
    ff = w_up.shape[1]
    out = pl.pallas_call(
        functools.partial(rest_kernel, batch, heads, dim, tp),
        out_shape=jax.ShapeDtypeStruct((batch, d_model), F32),
        in_specs=[vmem] * 6 + [hbm] * 4 + [any_spec] * 3 + [hbm] * 3,
        out_specs=vmem,
        scratch_shapes=[
            pltpu.VMEM((d_model, width), BF16), pltpu.VMEM((2 * n_enc, enc_dim), BF16),
            pltpu.VMEM((enc_dim, 2 * width), BF16), pltpu.VMEM((enc_dim, 2 * width), BF16),
            pltpu.VMEM((width, d_model), BF16), pltpu.VMEM((d_model, ff), BF16), pltpu.VMEM((ff, d_model), BF16),
            pltpu.VMEM((2 * n_enc, 2 * width), BF16), pltpu.VMEM((2 * n_enc, 2 * width), BF16), pltpu.VMEM((2 * n_enc, dim), F32),
            pltpu.VMEM((3, tp, batch, d_model), BF16),
            pltpu.VMEM((batch, d_model), BF16), pltpu.VMEM((batch, d_model), BF16),
            pltpu.VMEM((batch, width), BF16), pltpu.VMEM((batch, width), BF16),
            pltpu.VMEM((heads * batch, dim), F32), pltpu.VMEM((heads * batch, dim), F32), pltpu.VMEM((batch, dim), F32), pltpu.VMEM((batch, dim), F32),
            pltpu.SemaphoreType.DMA((10,)), pltpu.SemaphoreType.DMA((3, tp - 1)), pltpu.SemaphoreType.DMA((3, tp)),
            pltpu.SemaphoreType.DMA((5,)), pltpu.SemaphoreType.DMA((5,)), pltpu.SemaphoreType.DMA((2,)), pltpu.SemaphoreType.DMA((2,)),
        ],
        compiler_params=pltpu.CompilerParams(collective_id=0, has_side_effects=True, vmem_limit_bytes=46000000),
        cost_estimate=pl.CostEstimate(flops=20_000_000_000, bytes_accessed=30_000_000, transcendentals=0),
        name='rest_of_layer',
    )(part, x, ln2_gain, ln2_bias, ln3_gain, ln3_bias, *in_hbm(wq_c, enc, wk_c, wv_c), wk_far, wv_far, kv_half, *in_hbm(wo_c, w_up, w_down))
    return out.astype(BF16), jnp.transpose(k_new, (1, 0, 2)), jnp.transpose(v_new, (1, 0, 2))


def solution(mesh):
    row_spec = P('dp', None)
    cache_spec = P('dp', None, 'tp', None)
    head_spec = P('dp', 'tp', None)
    vec_spec = P(None)
    col_split = P(None, 'tp')
    row_split = P('tp', None)
    in_specs = (row_spec, cache_spec, cache_spec, P('dp'), P('dp', 'tp', None), vec_spec, vec_spec, col_split, col_split, col_split, row_split, vec_spec, vec_spec, col_split, col_split, col_split, row_split, vec_spec, vec_spec, col_split, row_split)
    out_specs = (row_spec, head_spec, head_spec)
    return jax.shard_map(local_step, mesh=mesh, in_specs=in_specs, out_specs=out_specs, check_vma=False)
```

```python
import functools

import jax
import jax.numpy as jnp
from jax import lax
from jax.experimental import pallas as pl
from jax.experimental.pallas import tpu as pltpu
from jax.sharding import PartitionSpec as P


LN_EPS = 1e-5
NEG = -1e30
F32 = jnp.float32
BF16 = jnp.bfloat16
CHUNK = 512
UNROLL = 4
GRAIN = 64
GROUPS = 6


def layer_norm(values, ln_gain, ln_bias):
    row_mean = jnp.mean(values, axis=-1, keepdims=True)
    centred = values - row_mean
    row_var = jnp.mean(jnp.square(centred), axis=-1, keepdims=True)
    return (centred * lax.rsqrt(row_var + LN_EPS) * ln_gain + ln_bias).astype(BF16)


def dot(lhs, rhs):
    return jnp.dot(lhs, rhs, preferred_element_type=F32)


def dot_t(lhs, rhs):
    return lax.dot_general(lhs, rhs, (((1,), (1,)), ((), ())), preferred_element_type=F32)


def in_hbm(*arrays):
    return [pltpu.with_memory_space_constraint(a, pltpu.HBM) for a in arrays]


def self_kernel(batch, heads, dim, lens_h, x_h, g_h, b_h, kc, vc, wq_h, wk_h, wv_h, wo_h,
                part_ref, knew_ref, vnew_ref,
                lens, x_v, g_v, b_v, wq, wk, wv, wo, kbuf, vbuf, q_s, v_s, o_s, m_s, l_s, acc_s, new_s, wsem, ksem, vsem):
    width = heads * dim
    scale = dim ** -0.5
    pairs = ((x_h, x_v), (g_h, g_v), (b_h, b_v), (wq_h, wq), (lens_h, lens), (wk_h, wk), (wv_h, wv), (wo_h, wo))
    ld_x, ld_g, ld_b, ld_q, ld_len, ld_k, ld_v, ld_o = [pltpu.make_async_copy(src, dst, wsem.at[i]) for i, (src, dst) in enumerate(pairs)]
    for copy in (ld_len, ld_x, ld_g, ld_b, ld_q, ld_k, ld_v):
        copy.start()

    def len_of(seq):
        return jnp.where(seq < batch, lens[jnp.minimum(seq, batch - 1)], 0)

    def following(seq, blk):
        more = (blk + 1) * CHUNK < len_of(seq)
        return jnp.where(more, seq, seq + 1), jnp.where(more, blk + 1, 0)

    def copies(seq, blk, slot, whole):
        live = pl.multiple_of(jnp.minimum(len_of(seq) - blk * CHUNK, CHUNK), GRAIN)
        first = pl.multiple_of(blk * CHUNK, CHUNK)
        count = CHUNK if whole else live
        src, dst = pl.ds(first, count), pl.ds(0, count)
        return (pltpu.make_async_copy(kc.at[seq, :, src, :], kbuf.at[slot, :, dst, :], ksem.at[slot]),
                pltpu.make_async_copy(vc.at[seq, :, src, :], vbuf.at[slot, :, dst, :], vsem.at[slot]))

    def fetch_group(group, ptr, whole):
        for u in range(UNROLL):
            seq, blk = ptr

            @pl.when(seq < batch)
            def _():
                for copy in copies(seq, blk, group * UNROLL + u, whole):
                    copy.start()

            ptr = following(seq, blk)
        return ptr

    ld_len.wait()
    ptr = (jnp.int32(0), jnp.int32(0))
    for group in range(GROUPS):
        ptr = fetch_group(group, ptr, True)
    ld_o.start()

    n_items = jnp.int32(0)
    for seq in range(batch):
        n_items = n_items + lax.div(lens[seq] + (CHUNK - 1), CHUNK)
    n_steps = lax.div(n_items + (UNROLL - 1), UNROLL)

    for copy in (ld_x, ld_g, ld_b):
        copy.wait()
    a_norm = layer_norm(x_v[...].astype(F32), g_v[...].reshape(1, -1), b_v[...].reshape(1, -1))
    ld_q.wait()
    q_s[0:batch, :] = dot(a_norm, wq[...]).astype(BF16).astype(F32)
    q_s[batch:, :] = jnp.zeros((q_s.shape[0] - batch, width), F32)
    m_s[...] = jnp.full(m_s.shape, NEG, F32)
    l_s[...] = jnp.zeros_like(l_s)
    acc_s[...] = jnp.zeros_like(acc_s)

    pair = 2 * dim
    part_rows = CHUNK // 2
    row8 = lax.broadcasted_iota(jnp.int32, (8, 1), 0)
    pair_row = lax.broadcasted_iota(jnp.int32, (8, pair), 0)
    pair_side = lax.broadcasted_iota(jnp.int32, (8, pair), 1) // dim
    sel01 = (pair_row == pair_side).astype(F32)
    sel2 = (pair_row == pair_side + 2).astype(F32)
    lane = lax.broadcasted_iota(jnp.int32, (8, CHUNK), 1)
    lane2 = lax.broadcasted_iota(jnp.int32, (8, part_rows), 1)

    def new_token():
        ld_k.wait()
        k_new = dot(a_norm, wk[...]).astype(BF16)
        ld_v.wait()
        v_new = dot(a_norm, wv[...]).astype(BF16)
        for h in range(heads):
            knew_ref[h] = k_new[:, h * dim:(h + 1) * dim]
            vnew_ref[h] = v_new[:, h * dim:(h + 1) * dim]
        qk = q_s[0:batch, :] * k_new.astype(F32)
        v_s[...] = v_new.astype(F32)
        for seq in range(batch):
            prod = qk[seq:seq + 1, :]
            tail = jnp.concatenate([prod[:, pair:width], jnp.zeros((1, pair - dim), F32)], axis=1)
            s_new = jnp.sum(prod[:, 0:pair] * sel01 + tail * sel2, axis=1, keepdims=True) * scale
            new_s[seq] = jnp.broadcast_to(jnp.where(row8 == 3, NEG, s_new), (8, dim))

    def step(i, carry):
        ptr, cur = carry[:2], carry[2:]
        group = lax.rem(i, GROUPS)

        @pl.when(i == 1)
        def _():
            new_token()

        items = []
        for u in range(UNROLL):
            items.append((*cur, group * UNROLL + u))
            cur = following(*cur)
        for seq, blk, slot in items:

            @pl.when((seq < batch) & (i < GROUPS))
            def _():
                for copy in copies(seq, blk, slot, True):
                    copy.wait()

            @pl.when((seq < batch) & (i >= GROUPS))
            def _():
                for copy in copies(seq, blk, slot, False):
                    copy.wait()
        scores = []
        for seq, blk, slot in items:
            q_row = q_s[pl.ds(jnp.minimum(seq, batch), 1), :]
            q01 = (q_row[:, 0:pair] * sel01).astype(BF16)
            q2 = (jnp.concatenate([q_row[:, pair:width]] * 2, axis=1) * sel2).astype(BF16)
            k01 = jnp.concatenate([kbuf[slot, 0], kbuf[slot, 1]], axis=1)
            k2 = jnp.concatenate([kbuf[slot, 2, 0:part_rows, :], kbuf[slot, 2, part_rows:CHUNK, :]], axis=1)
            scores.append((dot_t(q01, k01), dot_t(q2, k2)))
        weights = []
        for (seq, blk, slot), (s01, s2) in zip(items, scores):
            live = len_of(seq) - blk * CHUNK
            s01 = jnp.where(lane < jnp.where(row8 < 2, live, 0), s01 * scale, NEG)
            s2 = jnp.where(lane2 < jnp.where(row8 == 2, live, jnp.where(row8 == 3, live - part_rows, 0)), s2 * scale, NEG)
            m_i = jnp.maximum(jnp.max(s01, axis=1, keepdims=True), jnp.max(s2, axis=1, keepdims=True))
            p01 = jnp.where(row8 < 2, jnp.exp(s01 - m_i), 0.0)
            p2 = jnp.where(row8 < 2, 0.0, jnp.exp(s2 - m_i))
            l_i = jnp.sum(p01, axis=1, keepdims=True) + jnp.sum(p2, axis=1, keepdims=True)
            weights.append((m_i, l_i, p01.astype(BF16), p2.astype(BF16)))
        values = []
        for (seq, blk, slot), (m_i, l_i, p01, p2) in zip(items, weights):
            v01 = jnp.concatenate([vbuf[slot, 0], vbuf[slot, 1]], axis=1)
            v2 = jnp.concatenate([vbuf[slot, 2, 0:part_rows, :], vbuf[slot, 2, part_rows:CHUNK, :]], axis=1)
            values.append(dot(p01, v01) + dot(p2, v2))
        for (seq, blk, slot), (m_i, l_i, p01, p2), pv in zip(items, weights, values):
            row = jnp.minimum(seq, batch)
            m_old = m_s[row]
            m_new = jnp.maximum(m_old, m_i)
            keep = jnp.exp(m_old - m_new)
            add = jnp.exp(m_i - m_new)
            m_s[row] = m_new
            l_s[row] = l_s[row] * keep + l_i * add
            acc_s[row] = acc_s[row] * jnp.concatenate([keep] * 2, axis=1) + pv * jnp.concatenate([add] * 2, axis=1)
        ptr = fetch_group(group, ptr, False)
        return (*ptr, *cur)

    lax.fori_loop(0, n_steps, step, (*ptr, jnp.int32(0), jnp.int32(0)))
    for seq in range(batch):
        m_old, s_new = m_s[seq], new_s[seq]
        m = jnp.maximum(m_old, s_new)
        keep, add = jnp.exp(m_old - m), jnp.exp(s_new - m)
        v_row = v_s[seq:seq + 1, :]
        v_pair = jnp.where(pair_row < 2, v_row[:, 0:pair], jnp.concatenate([v_row[:, pair:width]] * 2, axis=1))
        l = l_s[seq] * keep + add
        acc = acc_s[seq] * jnp.concatenate([keep] * 2, axis=1) + v_pair * jnp.concatenate([add] * 2, axis=1)
        top = jnp.maximum(m[2:3], m[3:4])
        w_a, w_b = jnp.exp(m[2:3] - top), jnp.exp(m[3:4] - top)
        o2 = (acc[2:3, 0:dim] * w_a + acc[3:4, dim:pair] * w_b) / (l[2:3] * w_a + l[3:4] * w_b)
        o_s[seq:seq + 1, :] = jnp.concatenate([acc[0:1, 0:dim] / l[0:1], acc[1:2, dim:pair] / l[1:2], o2], axis=1)
    ld_o.wait()
    part_ref[...] = dot(o_s[...].astype(BF16), wo[...]).astype(BF16)


def rest_kernel(batch, heads, dim, tp, part_ref, x_ref, g2, b2, g3, b3, wqc_h, e_own_h, wk_h, wv_h, wkr_h, wvr_h, woc_h, wup_h, wdn_h,
                out_ref,
                wqc, enc, wkv, wkvr, woc, wup, wdn, kv_own, kv_rem, v_late, recv, send2, send3,
                qc_s, qc_r, o_snd, o_rcv, o2_snd, o2_rcv, lsem, ssem, rsem, xs, xr, ns, nr):
    width = heads * dim
    scale = dim ** -0.5
    me = lax.axis_index('tp')
    far = lax.rem(me + 2, tp)
    near = me + 1 - 2 * lax.rem(me, 2)
    half = enc.shape[0] // 2
    early = wvr_h.shape[1]

    def load(i, src, dst):
        copy = pltpu.make_async_copy(src, dst, lsem.at[i])
        copy.start()
        return copy

    ld_wv = load(2, wv_h, wkv.at[:, pl.ds(width, width)])
    ld_e0 = load(0, e_own_h, enc.at[pl.ds(0, half), :])
    ld_wk = load(1, wk_h, wkv.at[:, pl.ds(0, width)])
    ld_wkr = load(3, wkr_h, wkvr.at[:, pl.ds(0, width)])
    ld_wvr = load(4, wvr_h, wkvr.at[:, pl.ds(width, early)])
    ld_wqc = load(5, wqc_h, wqc)
    ld_woc = load(6, woc_h, woc)
    ld_up = load(7, wup_h, wup)
    ld_dn = load(8, wdn_h, wdn)

    barrier = pltpu.get_barrier_semaphore()
    for d in range(1, tp):
        pl.semaphore_signal(barrier, inc=1, device_id={'tp': lax.rem(me + d, tp)}, device_id_type=pl.DeviceIdType.MESH)
    pl.semaphore_wait(barrier, tp - 1)

    def remote(src, dst, send_sem, recv_sem, device):
        return pltpu.make_async_remote_copy(src_ref=src, dst_ref=dst, send_sem=send_sem, recv_sem=recv_sem,
                                            device_id={'tp': device}, device_id_type=pl.DeviceIdType.MESH)

    def sum_copies(n, src):
        return [remote(src, recv.at[n, me], ssem.at[n, d - 1], rsem.at[n, me], lax.rem(me + d, tp)) for d in range(1, tp)]

    def exchange(n, src):
        for copy in sum_copies(n, src):
            copy.start()
        recv[n, me] = src[...]

    def collect(n, src):
        for copy in sum_copies(n, src):
            copy.wait_send()
        for d in range(1, tp):
            other = lax.rem(me + d, tp)
            remote(src, recv.at[n, other], ssem.at[n, d - 1], rsem.at[n, other], other).wait_recv()
        total = recv[n, 0].astype(F32)
        for t in range(1, tp):
            total = total + recv[n, t].astype(F32)
        return total

    def project(first, count, jobs, tile=256):
        def body(i, c):
            rows = pl.ds(pl.multiple_of(i * tile, tile), tile)
            for weights, out, lo, hi in jobs:
                out[rows, lo:hi] = dot(enc[rows, :], weights[:, lo:hi]).astype(BF16)
            return c

        lax.fori_loop(first // tile, (first + count) // tile, body, 0)

    late_rows = (0, 640, wv_h.shape[0])

    def late(i):
        rows, cols = pl.ds(late_rows[i], late_rows[i + 1] - late_rows[i]), width - early
        return remote(wkv.at[rows, pl.ds(width + early, cols)], wkvr.at[rows, pl.ds(width + early, cols)], xs.at[3 + i], xr.at[3 + i], far)

    def late_product(i, tile=256):
        lo, hi = late_rows[i], late_rows[i + 1]

        def body(t, c):
            rows = pl.ds(pl.multiple_of(t * tile, tile), tile)
            product = dot(enc[rows, lo:hi], wkvr[lo:hi, width + early:2 * width])
            if i == 0:
                v_late[rows, :] = product
            else:
                kv_rem[rows, width + early:2 * width] = (v_late[rows, :] + product).astype(BF16)
            return c

        lax.fori_loop(0, 2 * half // tile, body, 0)

    def near_tokens(i):
        rows = half // 2
        return remote(enc.at[pl.ds(i * rows, rows), :], enc.at[pl.ds(half + i * rows, rows), :], ns.at[i], nr.at[i], near)

    own_job = (wkv, kv_own, 0, 2 * width)
    far_job = (wkvr, kv_rem, 0, width + early)

    exchange(0, part_ref)
    ld_wv.wait()
    late(0).start()
    ld_e0.wait()
    near_tokens(0).start()
    near_tokens(1).start()
    for copy in (ld_wk, ld_wkr, ld_wvr):
        copy.wait()
    project(0, half, (own_job, far_job))
    h1 = x_ref[...].astype(F32) + collect(0, part_ref)
    c_norm = layer_norm(h1, g2[...].reshape(1, -1), b2[...].reshape(1, -1))
    ld_wqc.wait()
    qc_s[...] = dot(c_norm, wqc[...]).astype(BF16)
    send_q = remote(qc_s, qc_r, xs.at[0], xr.at[0], far)
    send_q.start()
    late(1).start()
    near_tokens(0).wait()
    near_tokens(1).wait()
    project(half, half, (far_job,))
    late(0).wait()
    late_product(0)

    rows = heads * batch
    row_b = lax.rem(lax.broadcasted_iota(jnp.int32, (rows, 128), 0), batch)
    lane = lax.broadcasted_iota(jnp.int32, (rows, 128), 1)
    per = half // batch
    pack = 128 // per
    blocks = half // 128
    mine = lax.rem(row_b, pack) == lane // per
    row_blk = row_b // pack
    lane_head = lax.broadcasted_iota(jnp.int32, (batch, width), 1) // dim

    def weigh(q, kv):
        qf = q.astype(F32)
        q_rows = jnp.concatenate([jnp.where(lane_head == h, qf, 0.0) for h in range(heads)], axis=0).astype(BF16)
        parts = []
        for part in range(2):
            s_all = dot_t(q_rows, kv[part * half:(part + 1) * half, 0:width])
            s = s_all[:, 0:128]
            for k in range(1, blocks):
                s = jnp.where(row_blk == k, s_all[:, k * 128:(k + 1) * 128], s)
            parts.append(jnp.where(mine, s * scale, NEG))
        m = jnp.maximum(jnp.max(parts[0], axis=1, keepdims=True), jnp.max(parts[1], axis=1, keepdims=True))
        p = [jnp.exp(s - m) for s in parts]
        l = jnp.sum(p[0], axis=1, keepdims=True) + jnp.sum(p[1], axis=1, keepdims=True)
        wide = [jnp.concatenate([jnp.where(row_blk == k, p[part], 0.0) for k in range(blocks)], axis=1).astype(BF16) for part in range(2)]
        return m, l, wide

    def mix(wide, kv, first, last):
        lo, hi = first * batch, last * batch
        o = sum(dot(wide[part][lo:hi], kv[part * half:(part + 1) * half, width + first * dim:width + last * dim]) for part in range(2))
        return jnp.concatenate([o[(h - first) * batch:(h - first + 1) * batch, (h - first) * dim:(h - first + 1) * dim] for h in range(first, last)], axis=0)

    n_early = early // dim
    send_q.wait()
    m_r, l_r, wide_r = weigh(qc_r[...], kv_rem)
    o_snd[0:n_early * batch, :] = mix(wide_r, kv_rem, 0, n_early)
    stats = jnp.zeros((batch, dim), F32)
    st_lane = lax.broadcasted_iota(jnp.int32, (batch, dim), 1)
    for h in range(heads):
        stats = jnp.where(st_lane == 2 * h, m_r[h * batch:(h + 1) * batch], jnp.where(st_lane == 2 * h + 1, l_r[h * batch:(h + 1) * batch], stats))
    o_snd[n_early * batch:(n_early + 1) * batch, :] = stats
    send_o = remote(o_snd, o_rcv, xs.at[1], xr.at[1], far)
    send_o.start()
    late(1).wait()
    late_product(1)
    o2_snd[...] = mix(wide_r, kv_rem, n_early, heads)
    send_o2 = remote(o2_snd, o2_rcv, xs.at[2], xr.at[2], far)
    send_o2.start()
    project(half, half, (own_job,))
    m_a, l_a, wide_a = weigh(qc_s[...], kv_own)
    o_a = mix(wide_a, kv_own, 0, heads)
    send_o.wait()
    stats = o_rcv[n_early * batch:(n_early + 1) * batch, :]
    m_b = jnp.concatenate([stats[:, 2 * h:2 * h + 1] for h in range(heads)], axis=0)
    l_b = jnp.concatenate([stats[:, 2 * h + 1:2 * h + 2] for h in range(heads)], axis=0)
    m = jnp.maximum(m_a, m_b)
    w_a, w_b = jnp.exp(m_a - m), jnp.exp(m_b - m)
    send_o2.wait()
    o_b = jnp.concatenate([o_rcv[0:n_early * batch, :], o2_rcv[...]], axis=0)
    o = (o_a * w_a + o_b * w_b) / (l_a * w_a + l_b * w_b)
    oc = jnp.concatenate([o[h * batch:(h + 1) * batch, :] for h in range(heads)], axis=1).astype(BF16)

    def matmul_sum(n, lhs, weights, out):
        out[...] = dot(lhs, weights[...]).astype(BF16)
        exchange(n, out)
        return collect(n, out)

    ld_woc.wait()
    h2 = h1 + matmul_sum(1, oc, woc, send2)
    m_norm = layer_norm(h2, g3[...].reshape(1, -1), b3[...].reshape(1, -1))
    ld_up.wait()
    up = dot(m_norm, wup[...])
    hidden = (0.5 * up * (1.0 + lax.erf(up * (0.5 ** 0.5)))).astype(BF16)
    ld_dn.wait()
    out_ref[...] = h2 + matmul_sum(2, hidden, wdn, send3)


def local_step(x, k_cache, v_cache, seq_lens, nbr_enc, ln1_gain, ln1_bias, w_q, w_k, w_v, w_o, ln2_gain, ln2_bias, wq_c, wk_c, wv_c, wo_c, ln3_gain, ln3_bias, w_up, w_down):
    batch, d_model = x.shape
    heads, dim = k_cache.shape[2:]
    width = heads * dim
    tp = lax.axis_size('tp')
    far = [(i, (i + 2) % tp) for i in range(tp)]
    enc = nbr_enc.reshape(-1, nbr_enc.shape[-1])
    wk_far = lax.ppermute(wk_c, 'tp', far)
    wv_cut = wv_c[:, :2 * dim]
    wv_far = lax.ppermute(wv_cut, 'tp', far)

    any_spec = pl.BlockSpec(memory_space=pl.ANY)
    hbm = pl.BlockSpec(memory_space=pltpu.HBM)
    vmem = pl.BlockSpec(memory_space=pltpu.VMEM)
    slots = GROUPS * UNROLL
    part, k_new, v_new = pl.pallas_call(
        functools.partial(self_kernel, batch, heads, dim),
        out_shape=(jax.ShapeDtypeStruct((batch, d_model), BF16), jax.ShapeDtypeStruct((heads, batch, dim), BF16), jax.ShapeDtypeStruct((heads, batch, dim), BF16)),
        in_specs=[hbm] * 10,
        out_specs=(vmem, vmem, vmem),
        scratch_shapes=[
            pltpu.SMEM((batch,), jnp.int32), pltpu.VMEM((batch, d_model), BF16), pltpu.VMEM((d_model,), F32), pltpu.VMEM((d_model,), F32),
            pltpu.VMEM((d_model, width), BF16), pltpu.VMEM((d_model, width), BF16), pltpu.VMEM((d_model, width), BF16), pltpu.VMEM((width, d_model), BF16),
            pltpu.VMEM((slots, heads, CHUNK, dim), BF16), pltpu.VMEM((slots, heads, CHUNK, dim), BF16),
            pltpu.VMEM((batch + 8, width), F32), pltpu.VMEM((batch, width), F32), pltpu.VMEM((batch, width), F32),
            pltpu.VMEM((batch + 1, 8, dim), F32), pltpu.VMEM((batch + 1, 8, dim), F32), pltpu.VMEM((batch + 1, 8, 2 * dim), F32), pltpu.VMEM((batch, 8, dim), F32),
            pltpu.SemaphoreType.DMA((8,)), pltpu.SemaphoreType.DMA((slots,)), pltpu.SemaphoreType.DMA((slots,)),
        ],
        compiler_params=pltpu.CompilerParams(vmem_limit_bytes=46000000),
        cost_estimate=pl.CostEstimate(flops=40_000_000_000, bytes_accessed=60_000_000, transcendentals=0),
        name='self_attention',
    )(*in_hbm(seq_lens, x, ln1_gain, ln1_bias, jnp.transpose(k_cache, (0, 2, 1, 3)), jnp.transpose(v_cache, (0, 2, 1, 3)), w_q, w_k, w_v, w_o))

    n_enc, enc_dim = enc.shape
    ff = w_up.shape[1]
    out = pl.pallas_call(
        functools.partial(rest_kernel, batch, heads, dim, tp),
        out_shape=jax.ShapeDtypeStruct((batch, d_model), F32),
        in_specs=[vmem] * 6 + [hbm] * 4 + [any_spec] * 2 + [hbm] * 3,
        out_specs=vmem,
        scratch_shapes=[
            pltpu.VMEM((d_model, width), BF16), pltpu.VMEM((2 * n_enc, enc_dim), BF16),
            pltpu.VMEM((enc_dim, 2 * width), BF16), pltpu.VMEM((enc_dim, 2 * width), BF16),
            pltpu.VMEM((width, d_model), BF16), pltpu.VMEM((d_model, ff), BF16), pltpu.VMEM((ff, d_model), BF16),
            pltpu.VMEM((2 * n_enc, 2 * width), BF16), pltpu.VMEM((2 * n_enc, 2 * width), BF16), pltpu.VMEM((2 * n_enc, dim), F32),
            pltpu.VMEM((3, tp, batch, d_model), BF16),
            pltpu.VMEM((batch, d_model), BF16), pltpu.VMEM((batch, d_model), BF16),
            pltpu.VMEM((batch, width), BF16), pltpu.VMEM((batch, width), BF16),
            pltpu.VMEM((heads * batch, dim), F32), pltpu.VMEM((heads * batch, dim), F32), pltpu.VMEM((batch, dim), F32), pltpu.VMEM((batch, dim), F32),
            pltpu.SemaphoreType.DMA((9,)), pltpu.SemaphoreType.DMA((3, tp - 1)), pltpu.SemaphoreType.DMA((3, tp)),
            pltpu.SemaphoreType.DMA((5,)), pltpu.SemaphoreType.DMA((5,)), pltpu.SemaphoreType.DMA((2,)), pltpu.SemaphoreType.DMA((2,)),
        ],
        compiler_params=pltpu.CompilerParams(collective_id=0, has_side_effects=True, vmem_limit_bytes=46000000),
        cost_estimate=pl.CostEstimate(flops=20_000_000_000, bytes_accessed=30_000_000, transcendentals=0),
        name='rest_of_layer',
    )(part, x, ln2_gain, ln2_bias, ln3_gain, ln3_bias, *in_hbm(wq_c, enc, wk_c, wv_c), wk_far, wv_far, *in_hbm(wo_c, w_up, w_down))
    return out.astype(BF16), jnp.transpose(k_new, (1, 0, 2)), jnp.transpose(v_new, (1, 0, 2))


def solution(mesh):
    row_spec = P('dp', None)
    cache_spec = P('dp', None, 'tp', None)
    head_spec = P('dp', 'tp', None)
    vec_spec = P(None)
    col_split = P(None, 'tp')
    row_split = P('tp', None)
    in_specs = (row_spec, cache_spec, cache_spec, P('dp'), P('dp', 'tp', None), vec_spec, vec_spec, col_split, col_split, col_split, row_split, vec_spec, vec_spec, col_split, col_split, col_split, row_split, vec_spec, vec_spec, col_split, row_split)
    out_specs = (row_spec, head_spec, head_spec)
    return jax.shard_map(local_step, mesh=mesh, in_specs=in_specs, out_specs=out_specs, check_vma=False)
```
